32 devices in a mesh: section: 2 (over core), dp: 4 (over z), tensor: 4 (over y, x).
Axes of the slice: x: 2, y: 2, z: 4, core: 2. Of those that a mesh axis runs over, the one named last changes fastest.
Arguments:
- inputs: bfloat16 [2, 4, 1024, 768], P(None, 'dp', 'tensor'), may hold values from -6 to 6
- segment_ids: int32 [2, 4, 1024], P(None, 'dp'), may hold values from 0 to 7, never falling along the last dimension, each value on 1 to 384 neighbouring positions
- cotangent: float32 [2, 4, 1024, 768], P(None, 'dp', 'tensor'), may hold values from -6 to 6
- qkv_weight: bfloat16 [2, 3, 768, 768], P('section', None, 'dp', 'tensor'), may hold values from -0.21875 to 0.21875
- out_weight: bfloat16 [2, 768, 768], P('section', 'tensor', 'dp'), may hold values from -0.875 to 0.875
- up_weight: bfloat16 [2, 768, 3072], P('section', 'dp', 'tensor'), may hold values from -0.21875 to 0.21875
- down_weight: bfloat16 [2, 3072, 768], P('section', 'tensor', 'dp'), may hold values from -0.109375 to 0.109375
- norm_gain: float32 [2, 2, 768], P('section'), may hold values from 0.5 to 1.5
- norm_bias: float32 [2, 2, 768], P('section'), may hold values from -4 to 4
- qv_bias: float32 [2, 2, 768], P('section'), may hold values from -6 to 6
- up_bias: float32 [2, 3072], P('section'), may hold values from -6 to 6
- resid_bias: float32 [2, 768], P('section'), may hold values from -6 to 6
Outputs:
- outputs: float32 [2, 2, 4, 1024, 768], P('section', None, 'dp', 'tensor')
- input_grads: float32 [2, 2, 4, 1024, 768], P('section', None, 'dp', 'tensor')
- qkv_grad: float32 [2, 3, 768, 768], P('section', None, 'dp', 'tensor')
- out_grad: float32 [2, 768, 768], P('section', 'tensor', 'dp')
- up_grad: float32 [2, 768, 3072], P('section', 'dp', 'tensor')
- down_grad: float32 [2, 3072, 768], P('section', 'tensor', 'dp')
- gain_grad: float32 [2, 2, 768], P('section')
- norm_bias_grad: float32 [2, 2, 768], P('section')
- qv_bias_grad: float32 [2, 2, 768], P('section')
- up_bias_grad: float32 [2, 3072], P('section')
- resid_bias_grad: float32 [2, 768], P('section')
The draws below stay inside these ranges and needn't reach their ends.
Inputs may be any that keep to these rules, and one draw needn't show every extreme that they name: `segment_ids`: along each sequence the ids never fall; every id 0 to 7 holds 1 to 384 tokens, one of them exactly 384.
All inputs are finite; a program needn't handle non-finite values.
Results may differ from the reference program's by a relative error of at most 0.012.
Values may be sent and summed in bfloat16 or wider, within the bound.
A program may use at most 256 MiB of HBM per device.

```python
import math
import jax
import jax.numpy as jnp
import numpy as np
from jax import lax

D = 768
HEADS = 12
HEAD_DIM = 64
ROT = 16
FF = 3072
MICRO = 2
L = 1024
SEGMENTS = 8
HDIM = 768
SEQS = 4
SEG_MOST = 384


def with_spikes(array, rng, source, target, blocks, factor):
    owner, partner = [(jnp.arange(array.shape[position]) // (array.shape[position] // blocks)).reshape([-1 if axis == position else 1 for axis in range(array.ndim)]) for position in (source, target)]
    chosen = jax.random.permutation(rng, blocks)[partner]
    strong = (owner == chosen) | (owner == (partner + blocks // 2) % blocks)
    return jnp.where(strong, factor * array, array)


def level_of(rng, extent, split, low, largest):
    def one(dim, blocks):
        steps = jax.random.uniform(jax.random.fold_in(jax.random.fold_in(rng, 6), dim), (blocks,), jnp.float32, low / len(split), largest / len(split))
        return jnp.repeat(jnp.exp(steps), extent[dim] // blocks).reshape((-1,) + (1,) * (len(extent) - dim - 1))

    gain = one(*split[0])
    for cut in split[1:]:
        gain = gain * one(*cut)
    return gain


def profile(number_of, total, bound, slope):
    weights = [(1 << 20) // math.isqrt(standing ** slope) + 1 for standing in range(2, number_of + 1)]
    rest, given = total - bound - (number_of - 1), [1] * (number_of - 1)
    while rest > 0:
        movable = [i for i in range(number_of - 1) if given[i] < bound]
        mass, remaining = sum([weights[i] for i in movable]), rest
        for i in movable:
            more = min(bound - given[i], max(1, remaining * weights[i] // mass), rest)
            given[i] = given[i] + more
            rest = rest - more
    return np.array([bound] + given)


def uneven(key, number_of, total, bound, skew):
    if number_of == 2:
        one = jax.random.randint(key, (), max(1, total - bound), min(bound, total - 1) + 1)
        return jnp.stack([one, total - one])
    sizes = jnp.asarray(profile(number_of, total, bound, skew), jnp.int32)
    couples = (number_of - 1) // 2
    giver, taker = sizes[1:1 + 2 * couples:2], sizes[2:2 + 2 * couples:2]
    room = jnp.minimum(giver - 1, bound - taker)
    passed = jax.random.randint(jax.random.fold_in(key, 1), (couples,), 0, 1 << 20) % (room + 1)
    sizes = sizes.at[1:1 + 2 * couples:2].set(giver - passed).at[2:2 + 2 * couples:2].set(taker + passed)
    return sizes[jax.random.permutation(jax.random.fold_in(key, 2), number_of)]


def bell_draw(key, extent, spread, bound, split=(), kind=jnp.bfloat16):
    array = jax.random.normal(key, extent, jnp.float32) * spread
    if len(split) > 0:
        array = level_of(key, extent, split, -0.22, 0.18) * array
    return jnp.clip(array, min=-bound, max=bound).astype(kind)


def bell_draw_with(own_key, dims, spread, most, split, heavy, dtype=jnp.bfloat16):
    values = spread * jax.random.normal(own_key, dims, jnp.float32)
    if split:
        values = values * level_of(own_key, dims, split, -0.22, 0.18)
    return jnp.clip(with_spikes(values, jax.random.fold_in(own_key, 3), *heavy), -most, most).astype(dtype)


def setup_inputs(seed: int = 0) -> dict:
    splits = jax.random.split(jax.random.key(seed), 13)
    inputs = bell_draw(splits[0], (MICRO, SEQS, L, D), 1.0, 6.0, ((1, 4), (2, 4)))
    segment_ids = jax.vmap(lambda own: jnp.searchsorted(jnp.cumsum(uneven(own, SEGMENTS, L, SEG_MOST, 1)), jnp.arange(L), side="right"))(jax.random.split(splits[1], MICRO * SEQS)).reshape((MICRO, SEQS, L)).astype(jnp.int32)
    cotangent = bell_draw_with(splits[2], (MICRO, SEQS, L, D), 1.0, 6.0, ((1, 4), (2, 4)), (1, 3, 4, 2.0), jnp.float32)
    qkv_weight = bell_draw(splits[3], (2, 3, D, HDIM), D ** -0.5, 0.21875, ((0, 2), (2, 4), (3, 4)))
    out_weight = bell_draw(splits[4], (2, HDIM, D), (HDIM // 16) ** -0.5, 0.875, ((0, 2), (1, 4), (2, 4)))
    up_weight = bell_draw(splits[5], (2, D, FF), D ** -0.5, 0.21875, ((0, 2), (1, 4), (2, 4)))
    down_weight = bell_draw(splits[6], (2, FF, D), FF ** -0.5, 0.109375, ((0, 2), (1, 4), (2, 4)))
    norm_gain = jnp.clip(1.0 + 0.1 * jax.random.normal(splits[7], (2, 2, D), jnp.float32), 0.5, 1.5)
    norm_bias = bell_draw(splits[8], (2, 2, D), 0.3, 4.0, ((0, 2),), jnp.float32)
    qv_bias = bell_draw(splits[9], (2, 2, HDIM), 0.5, 6.0, ((0, 2),), jnp.float32)
    up_bias = bell_draw(splits[10], (2, FF), 0.5, 6.0, ((0, 2),), jnp.float32)
    resid_bias = bell_draw(splits[11], (2, D), 0.5, 6.0, ((0, 2),), jnp.float32)
    return {"inputs": inputs, "segment_ids": segment_ids, "cotangent": cotangent, "qkv_weight": qkv_weight, "out_weight": out_weight, "up_weight": up_weight, "down_weight": down_weight, "norm_gain": norm_gain, "norm_bias": norm_bias, "qv_bias": qv_bias, "up_bias": up_bias, "resid_bias": resid_bias}


epsilon = 1e-05
root_half = 0.7071067811865476
inv_root_tau = 0.3989422804014327
masked_score = -1e+30

def normalize(values, gain_row, shift_row):
    centre = lax.optimization_barrier(jnp.mean(values, axis=-1, keepdims=True))
    centred = values - centre
    inverse = lax.rsqrt(lax.optimization_barrier(jnp.mean(centred * centred, axis=-1, keepdims=True)) + epsilon)
    unit_rows = centred * inverse
    return (unit_rows, inverse, unit_rows * gain_row + shift_row)

def normalize_back(incoming, unit_rows, inverse, gain_row):
    scaled = incoming * gain_row
    return inverse * (scaled - lax.optimization_barrier(jnp.mean(scaled, axis=-1, keepdims=True)) - unit_rows * lax.optimization_barrier(jnp.mean(scaled * unit_rows, axis=-1, keepdims=True)))

def gelu_value(values):
    return values * 0.5 * (1.0 + lax.erf(values * root_half))

def gelu_slope(values):
    return 0.5 * (1.0 + lax.erf(values * root_half)) + values * inv_root_tau * jnp.exp(-0.5 * values * values)

def rotary_tables(length, rotated):
    positions = lax.broadcasted_iota(jnp.float32, (length, rotated // 2), 0)
    orders = lax.broadcasted_iota(jnp.float32, (length, rotated // 2), 1)
    angles = positions * jnp.exp(orders * (-2.0 * math.log(10000.0) / rotated))
    return (jnp.cos(angles), jnp.sin(angles))

def rotate(head_vals, cosine_table, sine_table, direction):
    half_rot = cosine_table.shape[-1]
    lower_part = head_vals[..., :half_rot]
    upper_part = head_vals[..., half_rot:2 * half_rot]
    turned = direction * sine_table
    return jnp.concatenate([lower_part * cosine_table - upper_part * turned, upper_part * cosine_table + lower_part * turned, head_vals[..., 2 * half_rot:]], axis=-1)

def as_float(values):
    return values.astype(jnp.float32)

def layer_forward(row_in, segments, layer, cosine_table, sine_table):
    query_key_value_matrix, output_matrix, up_matrix, down_matrix, gain_pair, shift_pair, qv_pair, up_bias_row, resid_row = layer
    length = row_in.shape[0]
    widened = row_in.astype(jnp.float32)
    unit_one, inverse_one, normed_one = normalize(widened, gain_pair[0], shift_pair[0])
    unit_two, inverse_two, normed_two = normalize(widened, gain_pair[1], shift_pair[1])
    attention_input = normed_one.astype(jnp.bfloat16)
    feedforward_input = normed_two.astype(jnp.bfloat16)
    projected_rows = jnp.einsum('ld,cde->cle', as_float(attention_input), as_float(query_key_value_matrix))
    cos_b = cosine_table[:, None, :]
    sin_b = sine_table[:, None, :]
    head_shape = (length, HEADS, HEAD_DIM)
    query_b = (rotate((projected_rows[0] + qv_pair[0]).reshape(head_shape), cos_b, sin_b, 1.0) * 0.125).astype(jnp.bfloat16)
    key_b = rotate(projected_rows[1].reshape(head_shape), cos_b, sin_b, 1.0).astype(jnp.bfloat16)
    value_b = (projected_rows[2] + qv_pair[1]).reshape(head_shape).astype(jnp.bfloat16)
    positions = lax.broadcasted_iota(jnp.int32, (length, length), 0)
    key_pos = lax.broadcasted_iota(jnp.int32, (length, length), 1)
    allowed = (segments[:, None] == segments[None, :]) & (key_pos <= positions)
    scores = jnp.einsum('qhd,khd->hqk', as_float(query_b), as_float(key_b))
    scores = jnp.where(allowed[None], scores, masked_score)
    row_top = lax.optimization_barrier(jnp.max(scores, axis=-1, keepdims=True))
    log_total = row_top + jnp.log(lax.optimization_barrier(jnp.sum(jnp.exp(scores - row_top), axis=-1, keepdims=True)))
    probs = jnp.exp(scores - log_total)
    probs_b = probs.astype(jnp.bfloat16)
    context = jnp.einsum('hqk,khd->qhd', as_float(probs_b), as_float(value_b)).astype(jnp.bfloat16)
    flattened_context = context.reshape(length, HDIM)
    up_pre = jnp.dot(feedforward_input, up_matrix, preferred_element_type=jnp.float32) + up_bias_row
    hidden_block = gelu_value(up_pre).astype(jnp.bfloat16)
    branch = jnp.dot(flattened_context, output_matrix, preferred_element_type=jnp.float32) + jnp.dot(hidden_block, down_matrix, preferred_element_type=jnp.float32)
    result = widened + branch + resid_row
    saved = (unit_one, inverse_one, unit_two, inverse_two, attention_input, feedforward_input, query_b, key_b, value_b, probs, probs_b, flattened_context, up_pre, hidden_block)
    return (result, saved)

def layer_backward(row_in, segments, incoming, layer, cosine_table, sine_table):
    query_key_value_matrix, output_matrix, up_matrix, down_matrix, gain_pair, shift_pair, qv_pair, up_bias_row, resid_row = layer
    result, saved = layer_forward(row_in, segments, layer, cosine_table, sine_table)
    unit_one, inverse_one, unit_two, inverse_two, attention_input, feedforward_input, query_b, key_b, value_b, probs, probs_b, flattened_context, up_pre, hidden_block = saved
    length = row_in.shape[0]
    grad_b = incoming.astype(jnp.bfloat16)
    down_weight_gradient = jnp.dot(hidden_block.T, grad_b, preferred_element_type=jnp.float32)
    output_weight_gradient = jnp.dot(flattened_context.T, grad_b, preferred_element_type=jnp.float32)
    resid_g = lax.optimization_barrier(jnp.sum(incoming, axis=0))
    pre_grad = jnp.dot(grad_b, down_matrix.T, preferred_element_type=jnp.float32) * gelu_slope(up_pre)
    up_bias_g = lax.optimization_barrier(jnp.sum(pre_grad, axis=0))
    preactivation_block = pre_grad.astype(jnp.bfloat16)
    up_weight_gradient = jnp.dot(feedforward_input.T, preactivation_block, preferred_element_type=jnp.float32)
    feedforward_input_gradient = jnp.dot(preactivation_block, up_matrix.T, preferred_element_type=jnp.float32)
    context_gradient = jnp.dot(grad_b, output_matrix.T, preferred_element_type=jnp.float32).astype(jnp.bfloat16)
    context_gradient = context_gradient.reshape(length, HEADS, HEAD_DIM)
    value_grad = jnp.einsum('hqk,qhd->khd', as_float(probs_b), as_float(context_gradient))
    prob_grad = jnp.einsum('qhd,khd->hqk', as_float(context_gradient), as_float(value_b))
    score_grad = probs * (prob_grad - lax.optimization_barrier(jnp.sum(probs * prob_grad, axis=-1, keepdims=True)))
    score_b = score_grad.astype(jnp.bfloat16)
    query_grad = jnp.einsum('hqk,khd->qhd', as_float(score_b), as_float(key_b))
    key_grad = jnp.einsum('hqk,qhd->khd', as_float(score_b), as_float(query_b))
    cos_b = cosine_table[:, None, :]
    sin_b = sine_table[:, None, :]
    query_grad = rotate(query_grad, cos_b, sin_b, -1.0) * 0.125
    key_grad = rotate(key_grad, cos_b, sin_b, -1.0)
    stacked = jnp.stack([query_grad.reshape(length, HDIM), key_grad.reshape(length, HDIM), value_grad.reshape(length, HDIM)])
    qv_g = jnp.stack([lax.optimization_barrier(jnp.sum(stacked[0], axis=0)), lax.optimization_barrier(jnp.sum(stacked[2], axis=0))])
    stacked_block = stacked.astype(jnp.bfloat16)
    query_key_value_gradient = jnp.einsum('ld,cle->cde', as_float(attention_input), as_float(stacked_block))
    attn_in_grad = jnp.einsum('cle,cde->ld', as_float(stacked_block), as_float(query_key_value_matrix))
    gain_g = jnp.stack([lax.optimization_barrier(jnp.sum(attn_in_grad * unit_one, axis=0)), lax.optimization_barrier(jnp.sum(feedforward_input_gradient * unit_two, axis=0))])
    shift_g = jnp.stack([lax.optimization_barrier(jnp.sum(attn_in_grad, axis=0)), lax.optimization_barrier(jnp.sum(feedforward_input_gradient, axis=0))])
    input_grad = incoming + normalize_back(attn_in_grad, unit_one, inverse_one, gain_pair[0]) + normalize_back(feedforward_input_gradient, unit_two, inverse_two, gain_pair[1])
    return (input_grad, (query_key_value_gradient, output_weight_gradient, up_weight_gradient, down_weight_gradient, gain_g, shift_g, qv_g, up_bias_g, resid_g))

def reference(inputs, segment_ids, cotangent, qkv_weight, out_weight, up_weight, down_weight, norm_gain, norm_bias, qv_bias, up_bias, resid_bias):
    cosine_table, sine_table = rotary_tables(L, ROT)
    flat_in = inputs.reshape(-1, L, D)
    flat_segs = segment_ids.reshape(-1, L)
    flat_cot = cotangent.reshape(-1, L, D)

    def layer_of(number):
        return (qkv_weight[number], out_weight[number], up_weight[number], down_weight[number], norm_gain[number], norm_bias[number], qv_bias[number], up_bias[number], resid_bias[number])

    def run_layer(layer, row_sets):

        def one_seq(pair):
            made, saved = layer_forward(pair[0], pair[1], layer, cosine_table, sine_table)
            return made
        return lax.map(one_seq, (row_sets, flat_segs))

    def back_layer(layer, row_sets, grad_sets):
        zeros_tree = (jnp.zeros(layer[0].shape, jnp.float32), jnp.zeros(layer[1].shape, jnp.float32), jnp.zeros(layer[2].shape, jnp.float32), jnp.zeros(layer[3].shape, jnp.float32), jnp.zeros(layer[4].shape, jnp.float32), jnp.zeros(layer[5].shape, jnp.float32), jnp.zeros(layer[6].shape, jnp.float32), jnp.zeros(layer[7].shape, jnp.float32), jnp.zeros(layer[8].shape, jnp.float32))

        def step_fn(running, item):
            input_grad, parts = layer_backward(item[0], item[1], item[2], layer, cosine_table, sine_table)
            return (jax.tree.map(lambda left, right: left + right, running, parts), input_grad)
        return lax.scan(step_fn, zeros_tree, (row_sets, flat_segs, grad_sets))
    layer_zero = layer_of(0)
    layer_one = layer_of(1)
    wide_one = run_layer(layer_zero, flat_in)
    hidden_one = wide_one.astype(jnp.bfloat16)
    wide_two = run_layer(layer_one, hidden_one)
    totals_one, grad_mid = back_layer(layer_one, hidden_one, flat_cot)
    totals_zero, grad_first = back_layer(layer_zero, flat_in, grad_mid)
    out_shape = inputs.shape
    outputs = jnp.stack([wide_one.reshape(out_shape), wide_two.reshape(out_shape)])
    input_grads = jnp.stack([grad_first.reshape(out_shape), grad_mid.reshape(out_shape)])
    stacked = [jnp.stack([totals_zero[number], totals_one[number]]) for number in range(9)]
    return (outputs, input_grads, stacked[0], stacked[1], stacked[2], stacked[3], stacked[4], stacked[5], stacked[6], stacked[7], stacked[8])
```

```python
import functools
import math

import jax
import jax.numpy as jnp
import numpy as np
from jax import lax
from jax.experimental import pallas as pl
from jax.experimental.pallas import tpu as pltpu
from jax.sharding import PartitionSpec as P

HEAD_DIM = 64
ROT = 16
SEG_MOST = 384
EPS = 1e-05
MASKED = -1e30
ROOT_HALF = 0.7071067811865476
INV_ROOT_TAU = 0.3989422804014327

BF = jnp.bfloat16
F32 = jnp.float32
MESH = pl.DeviceIdType.MESH

NN = (((1,), (0,)), ((), ()))
NT = (((1,), (1,)), ((), ()))
TN = (((0,), (0,)), ((), ()))

BQ = 128
BK = BQ + SEG_MOST
HL = 256
QO, KO, VO, OO = 0, 192, 384, 576


def mm(a, b, dims):
    return lax.dot_general(a, b, dims, preferred_element_type=F32)


def lane_iota(rows, cols=HL):
    return lax.broadcasted_iota(jnp.int32, (rows, cols), 1)


def remote(src, dst, send, recv, dev):
    return pltpu.make_async_remote_copy(
        src_ref=src, dst_ref=dst, send_sem=send, recv_sem=recv, device_id=dev, device_id_type=MESH
    )


def kernel(
    n,
    heads,
    x_in,
    cot_in,
    segc_in,
    segr_in,
    w_in,
    par_in,
    taba,
    tabb,
    out_y,
    out_g,
    out_w,
    out_s,
    w,
    x,
    an,
    mn,
    mu,
    rstd,
    qb,
    kb,
    vb,
    cb,
    lse,
    slope,
    hid,
    gb,
    du,
    dqkv,
    dc,
    dq,
    dk,
    dv,
    bias,
    pscr,
    dpscr,
    sendb,
    recvb,
    ownp,
    gw,
    gsr,
    zrecv,
    wacc,
    cotv,
    yst,
    gst,
    segc,
    par,
    sm,
    smr,
    smt,
    smz,
    tall,
    lsem,
    psem,
    xs,
    xr,
    gs,
    gr,
    ws,
    wr,
    fs,
    fr,
    rss,
    rsr,
    osend,
    orecv,
    ghs,
    ghr,
    zs,
    zr,
    sms,
    smrs,
):
    s = lax.axis_index("section")
    z = lax.axis_index("dp")
    t = lax.axis_index("tensor")
    sib = (1 - s, z, t)
    width = x.shape[2]
    length = x.shape[1]
    chunk = length // 4
    rows_z = w_in.shape[1]
    nblk = length // BQ
    own = pl.ds(t * chunk, chunk)
    zrows = pl.ds(z * rows_z, rows_z)

    def plane(k):
        return (s, z, t ^ k)

    def other_z(j):
        return lax.rem(z + j, n)

    lx = pltpu.make_async_copy(x_in.at[s], x.at[0, own], lsem.at[0])
    lc = pltpu.make_async_copy(cot_in.at[s], cotv, lsem.at[1])
    lw = [
        pltpu.make_async_copy(w_in.at[p], w.at[s, p, zrows], lsem.at[2 + p]) for p in range(3)
    ]
    lseg = pltpu.make_async_copy(segc_in.at[s], segc, lsem.at[5])
    lpar = pltpu.make_async_copy(par_in, par.at[s], lsem.at[6])
    lx.start()
    for p in range(3):
        lw[p].start()
    lpar.start()
    lc.start()
    lseg.start()

    barrier = pltpu.get_barrier_semaphore()
    pl.semaphore_signal(barrier, inc=1, device_id=sib, device_id_type=MESH)
    for k in range(1, 4):
        pl.semaphore_signal(barrier, inc=1, device_id=plane(k), device_id_type=MESH)
    for j in range(1, n):
        pl.semaphore_signal(barrier, inc=1, device_id=(s, other_z(j), t), device_id_type=MESH)
    pl.semaphore_wait(barrier, 4 + n - 1)

    def w_copy(p, j):
        return remote(
            w.at[s, p, zrows],
            w.at[s, p, zrows],
            ws.at[p, j - 1],
            wr.at[p, j - 1],
            (s, other_z(j), t),
        )

    def w_arrival(p, j):
        rows = pl.ds(other_z(n - j) * rows_z, rows_z)
        return remote(
            w.at[s, p, rows], w.at[s, p, rows], ws.at[p, j - 1], wr.at[p, j - 1], (s, z, t ^ 1)
        )

    def forward(layer, p):
        return remote(w.at[layer, p], w.at[layer, p], fs.at[p], fr.at[p], sib)

    def x_copy(layer, k):
        return remote(
            x.at[layer, own], x.at[layer, own], xs.at[layer, k - 1], xr.at[layer, k - 1], plane(k)
        )

    def x_arrival(layer, k):
        rows = pl.ds((t ^ k) * chunk, chunk)
        return remote(
            x.at[layer, rows],
            x.at[layer, rows],
            xs.at[layer, k - 1],
            xr.at[layer, k - 1],
            plane(k),
        )

    def g_copy(layer, k):
        return remote(
            gb.at[layer, own], gb.at[layer, own], gs.at[layer, k - 1], gr.at[layer, k - 1], plane(k)
        )

    def g_arrival(layer, k):
        rows = pl.ds((t ^ k) * chunk, chunk)
        return remote(
            gb.at[layer, rows],
            gb.at[layer, rows],
            gs.at[layer, k - 1],
            gr.at[layer, k - 1],
            plane(k),
        )

    def part_copy(phase, k):
        return remote(
            sendb.at[k - 1],
            recvb.at[phase % 2, k - 1],
            rss.at[phase, k - 1],
            rsr.at[phase, k - 1],
            plane(k),
        )

    lx.wait()
    for k in range(1, 4):
        x_copy(0, k).start()
    lpar.wait()
    par_copy = remote(par.at[s], par.at[s], psem.at[0], psem.at[1], sib)
    par_copy.start()
    for p in range(3):
        lw[p].wait()

    @pl.when(s == 0)
    def _():
        for p in range(3):
            for j in range(1, n):
                w_copy(p, j).start()

    lc.wait()
    gb[1, own, :] = cotv[...].astype(BF)
    for k in range(1, 4):
        g_copy(1, k).start()

    lseg.wait()

    @pl.loop(0, nblk)
    def _(b):
        q0 = pl.multiple_of(b * BQ, BQ)
        k0 = pl.multiple_of(jnp.maximum(b * BQ - SEG_MOST, 0), BQ)
        seg_k = segc[pl.ds(k0, BK), :]
        seg_q = jnp.where(
            s == 0, segr_in[0:1, pl.ds(q0, BQ)], segr_in[1:2, pl.ds(q0, BQ)]
        )
        kpos = lax.broadcasted_iota(jnp.int32, (BK, BQ), 0) + k0
        qpos = lax.broadcasted_iota(jnp.int32, (BK, BQ), 1) + q0
        allowed = (seg_k == seg_q) & (kpos <= qpos)
        bias[b] = jnp.where(allowed, 0.0, MASKED).astype(BF)

    par_wait = remote(par.at[1 - s], par.at[1 - s], psem.at[0], psem.at[1], sib)
    par_copy.wait_send()
    par_wait.wait_recv()

    @pl.loop(0, 2)
    def _(i):
        sm[i] = jnp.zeros((8, width), F32)

    def need_w(layer, p):
        @pl.when(s == layer)
        def _():
            for j in range(1, n):
                w_arrival(p, j).wait_recv()
            forward(layer, p).start()

        @pl.when(s != layer)
        def _():
            forward(layer, p).wait_recv()
            if layer == 0:
                for j in range(1, n):
                    w_copy(p, j).start()

    def prow(layer, r, cols=None):
        if cols is None:
            return par[layer, r : r + 1, :]
        return par[layer, r : r + 1, cols]

    def rope_tables(b, sign):
        ca = taba[0, b]
        sa = taba[1, b]
        c0 = tabb[0]
        s0 = tabb[1]
        cos = ca * c0 - sa * s0
        sin = sa * c0 + ca * s0
        lane = lane_iota(BQ) & (HEAD_DIM - 1)
        return cos, jnp.where(lane < ROT // 2, -sign, sign) * sin

    def rope(u, b, sign):
        halves = []
        lane = lane_iota(BQ) & (HEAD_DIM - 1)
        for i in range(u.shape[0] // BQ):
            part = u[i * BQ : (i + 1) * BQ]
            cos, sin = rope_tables(b + i, sign)
            partner = jnp.where(
                lane < ROT // 2,
                pltpu.roll(part, HL - ROT // 2, 1),
                pltpu.roll(part, ROT // 2, 1),
            )
            halves.append(part * cos + partner * sin)
        return jnp.concatenate(halves, axis=0)

    def stack_heads(block):
        lane = lane_iota(BQ) >> 6
        return jnp.concatenate(
            [jnp.where(lane == h, block, jnp.zeros_like(block)) for h in range(heads)], axis=0
        )

    sub = 64

    def norm_chunk(layer, c):
        @pl.loop(0, chunk // sub)
        def _(i):
            rows = pl.ds(pl.multiple_of(c * chunk + i * sub, sub), sub)
            v = x[layer, rows, :].astype(F32)
            m = jnp.mean(v, axis=-1, keepdims=True)
            v = v - m
            r = lax.rsqrt(jnp.mean(v * v, axis=-1, keepdims=True) + EPS)
            mu[layer, rows, :] = m
            rstd[layer, rows, :] = r
            v = v * r
            an[rows, :] = (v * prow(layer, 0) + prow(layer, 2)).astype(BF)
            mn[rows, :] = (v * prow(layer, 1) + prow(layer, 3)).astype(BF)

    def renorm_all(layer):
        @pl.loop(0, length // sub)
        def _(i):
            rows = pl.ds(pl.multiple_of(i * sub, sub), sub)
            v = (x[layer, rows, :].astype(F32) - mu[layer, rows, :]) * rstd[layer, rows, :]
            an[rows, :] = (v * prow(layer, 0) + prow(layer, 2)).astype(BF)
            mn[rows, :] = (v * prow(layer, 1) + prow(layer, 3)).astype(BF)

    def forward_layer(layer):
        phase = layer
        norm_chunk(layer, t)
        for k in range(1, 4):
            x_arrival(layer, k).wait_recv()
            norm_chunk(layer, t ^ k)
        need_w(layer, 0)

        @pl.loop(0, 4)
        def _(c):
            rows = pl.ds(pl.multiple_of(c * chunk, chunk), chunk)
            a = an[rows, :]
            b0 = c * (chunk // BQ)
            lane = lane_iota(chunk)
            u = mm(a, w[layer, 0, :, QO : QO + HL], NN) + prow(layer, 4, slice(0, HL))
            qb[layer, rows, :] = (rope(u, b0, 1.0) * 0.125).astype(BF)
            u = mm(a, w[layer, 0, :, KO - 64 : KO - 64 + HL], NN)
            kb[layer, rows, :] = rope(pltpu.roll(u, HL - 64, 1), b0, 1.0).astype(BF)
            u = mm(a, w[layer, 0, :, VO : VO + HL], NN) + prow(layer, 5, slice(0, HL))
            vb[layer, rows, :] = jnp.where(lane < heads * HEAD_DIM, u, 0.0).astype(BF)

        @pl.loop(0, nblk)
        def _(b):
            q0 = pl.multiple_of(b * BQ, BQ)
            k0 = pl.multiple_of(jnp.maximum(b * BQ - SEG_MOST, 0), BQ)
            qm = stack_heads(qb[layer, pl.ds(q0, BQ), :])
            top = None
            for i in range(BK // BQ):
                keys = kb[layer, pl.ds(k0 + i * BQ, BQ), :]
                blk = bias[b, i * BQ : (i + 1) * BQ, :].astype(F32)
                sc = mm(keys, qm, NT) + jnp.concatenate([blk] * heads, axis=1)
                pscr[i * BQ : (i + 1) * BQ, :] = sc
                peak = jnp.max(sc, axis=0, keepdims=True)
                top = peak if top is None else jnp.maximum(top, peak)
            total = None
            for i in range(BK // BQ):
                e = jnp.exp(pscr[i * BQ : (i + 1) * BQ, :] - top)
                pscr[i * BQ : (i + 1) * BQ, :] = e
                part = jnp.sum(e, axis=0, keepdims=True)
                total = part if total is None else total + part
            lse[layer, b] = top + jnp.log(total)
            inv = 1.0 / total
            lane = lane_iota(BQ) >> 6
            ctx = jnp.zeros((BQ, HL), F32)
            vals = vb[layer, pl.ds(k0, BK), :]
            for h in range(heads):
                cols = slice(h * BQ, (h + 1) * BQ)
                ph = (pscr[:, cols] * inv[:, cols]).astype(BF)
                ctx = jnp.where(lane == h, mm(ph, vals, TN), ctx)
            cb[layer, pl.ds(q0, BQ), :] = pltpu.roll(ctx, HL - heads * HEAD_DIM, 1).astype(BF)

        need_w(layer, 1)

        @pl.loop(0, 4)
        def _(c):
            rows = pl.ds(pl.multiple_of(c * chunk, chunk), chunk)
            a = mn[rows, :]
            for j in range(width // 256):
                cols = slice(j * 256, (j + 1) * 256)
                u = mm(a, w[layer, 1, :, cols], NN) + prow(layer, 6, cols)
                phi = 0.5 * (1.0 + lax.erf(u * ROOT_HALF))
                hid[layer, rows, cols] = (u * phi).astype(BF)
                slope[layer, rows, cols] = (
                    phi + u * INV_ROOT_TAU * jnp.exp(-0.5 * u * u)
                ).astype(BF)

        need_w(layer, 2)
        if layer == 1:
            for k in range(1, 4):
                part_copy(0, k).wait_send()
        for k in (1, 2, 3, 0):
            rows = pl.ds(pl.multiple_of((t ^ k) * chunk, chunk), chunk)
            c = cb[layer, rows, :]
            h = hid[layer, rows, :]
            for j in range(width // 256):
                cols = slice(j * 256, (j + 1) * 256)
                y = mm(c, w[layer, 0, cols, 512:768], NT) + mm(h, w[layer, 2, cols, :], NT)
                if k:
                    sendb[k - 1, :, cols] = y.astype(BF)
                else:
                    ownp[phase % 2, :, cols] = y
            if k:
                part_copy(phase, k).start()

    def place(layer, stage, out, idx):
        @pl.when(s == layer)
        def _():
            pltpu.make_async_copy(stage, out.at[s], osend.at[idx]).start()

        @pl.when(s != layer)
        def _():
            remote(stage, out.at[s], osend.at[idx], orecv.at[idx // 2], sib).start()

    def placed(layer, stage, out, idx):
        @pl.when(s == layer)
        def _():
            pltpu.make_async_copy(stage, out.at[s], osend.at[idx]).wait()

        @pl.when(s != layer)
        def _():
            remote(stage, out.at[s], osend.at[idx], orecv.at[idx // 2], sib).wait_send()

    def finish_y(layer):
        phase = layer
        for k in range(1, 4):
            part_copy(phase, k).wait_recv()
        if layer == 1:
            placed(0, yst, out_y, 0)

        @pl.loop(0, chunk // sub)
        def _(i):
            r = pl.ds(pl.multiple_of(i * sub, sub), sub)
            rows = pl.ds(pl.multiple_of(t * chunk + i * sub, sub), sub)
            y = x[layer, rows, :].astype(F32) + ownp[phase % 2, r, :] + prow(layer, 7)
            for k in range(3):
                y = y + recvb[phase % 2, k, r, :].astype(F32)
            yst[r, :] = y
            if layer == 0:
                x[1, rows, :] = y.astype(BF)

        if layer == 0:
            for k in range(1, 4):
                x_copy(1, k).start()
        place(layer, yst, out_y, layer)

    def reduce_start(layer, p, buf):
        @pl.when(s != layer)
        def _():
            remote(buf.at[p], gsr.at[p], ghs.at[p], ghr.at[p], sib).start()

    def z_copy(p, j, buf):
        rows = pl.ds(other_z(j) * rows_z, rows_z)
        return remote(
            buf.at[p, rows],
            zrecv.at[p, j - 1],
            zs.at[p, j - 1],
            zr.at[p, j - 1],
            (s, other_z(j), t),
        )

    step = 48

    def reduce_cores(layer, p, buf):
        @pl.when(s == layer)
        def _():
            remote(buf.at[p], gsr.at[p], ghs.at[p], ghr.at[p], sib).wait_recv()

            @pl.loop(0, rows_z // step)
            def _(i):
                r = pl.ds(pl.multiple_of(i * step, 16), step)
                q = pl.ds(pl.multiple_of(z * rows_z + i * step, 16), step)
                wacc[p, r, :] = buf[p, q, :].astype(F32) + gsr[p, q, :].astype(F32)

            for j in range(1, n):
                base = other_z(j) * rows_z

                @pl.loop(0, rows_z // step)
                def _(i):
                    q = pl.ds(pl.multiple_of(base + i * step, 16), step)
                    buf[p, q, :] = (buf[p, q, :].astype(F32) + gsr[p, q, :].astype(F32)).astype(BF)

                z_copy(p, j, buf).start()

        @pl.when(s != layer)
        def _():
            remote(buf.at[p], gsr.at[p], ghs.at[p], ghr.at[p], sib).wait_send()

    def grad_part(layer, p, buf):
        for j in range(width // 256):
            cols = slice(j * 256, (j + 1) * 256)
            if p == 2:
                buf[p, cols, :] = mm(gb[layer, :, cols], hid[layer], TN).astype(BF)
            elif p == 1:
                buf[p, cols, :] = mm(mn[:, cols], du[...], TN).astype(BF)
            else:
                buf[p, cols, 0:512] = mm(an[:, cols], dqkv[:, 0:512], TN).astype(BF)
                buf[p, cols, 512:768] = (
                    mm(an[:, cols], dqkv[:, 512:768], TN) + mm(gb[layer, :, cols], cb[layer], TN)
                ).astype(BF)
        reduce_start(layer, p, buf)

    def backward_layer(layer, buf, between):
        phase = 3 - layer
        for k in range(1, 4):
            g_arrival(layer, k).wait_recv()
        grad_part(layer, 2, buf)

        @pl.loop(0, 4)
        def _(c):
            rows = pl.ds(pl.multiple_of(c * chunk, chunk), chunk)
            g = gb[layer, rows, :]
            for j in range(width // 256):
                cols = slice(j * 256, (j + 1) * 256)
                d = mm(g, w[layer, 2, :, cols], NN) * slope[layer, rows, cols].astype(F32)
                sm[layer, 6:7, cols] = sm[layer, 6:7, cols] + jnp.sum(d, axis=0, keepdims=True)
                du[rows, cols] = d.astype(BF)
            d = pltpu.roll(mm(g, w[layer, 0, :, 512:768], NN), HL - 64, 1)
            lane = lane_iota(chunk)
            dc[rows, :] = jnp.where(lane < heads * HEAD_DIM, d, 0.0).astype(BF)
            dk[rows, :] = jnp.zeros((chunk, HL), F32)
            dv[rows, :] = jnp.zeros((chunk, HL), F32)

        grad_part(layer, 1, buf)
        between(2)

        @pl.loop(0, nblk)
        def _(b):
            q0 = pl.multiple_of(b * BQ, BQ)
            k0 = pl.multiple_of(jnp.maximum(b * BQ - SEG_MOST, 0), BQ)
            qm = stack_heads(qb[layer, pl.ds(q0, BQ), :])
            dm = stack_heads(dc[pl.ds(q0, BQ), :])
            ls = lse[layer, b]
            total = None
            for i in range(BK // BQ):
                krows = pl.ds(k0 + i * BQ, BQ)
                irows = slice(i * BQ, (i + 1) * BQ)
                blk = bias[b, irows, :].astype(F32)
                sc = mm(kb[layer, krows, :], qm, NT) + jnp.concatenate([blk] * heads, axis=1)
                pr = jnp.exp(sc - ls)
                dp = mm(vb[layer, krows, :], dm, NT)
                dv[krows, :] = dv[krows, :] + mm(pr.astype(BF), dm, NN)
                pscr[irows, :] = pr
                dpscr[irows, :] = dp
                part = jnp.sum(pr * dp, axis=0, keepdims=True)
                total = part if total is None else total + part
            lane = lane_iota(BQ) >> 6
            acc = [jnp.zeros((BQ, HL), F32) for _ in range(heads)]
            for i in range(BK // BQ):
                krows = pl.ds(k0 + i * BQ, BQ)
                irows = slice(i * BQ, (i + 1) * BQ)
                ds = (pscr[irows, :] * (dpscr[irows, :] - total)).astype(BF)
                dk[krows, :] = dk[krows, :] + mm(ds, qm, NN)
                keys = kb[layer, krows, :]
                for h in range(heads):
                    acc[h] = acc[h] + mm(ds[:, h * BQ : (h + 1) * BQ], keys, TN)
            out = jnp.zeros((BQ, HL), F32)
            for h in range(heads):
                out = jnp.where(lane == h, acc[h], out)
            dq[pl.ds(q0, BQ), :] = out

        between(1)

        @pl.loop(0, 4)
        def _(c):
            rows = pl.ds(pl.multiple_of(c * chunk, chunk), chunk)
            b0 = c * (chunk // BQ)
            lane = lane_iota(chunk)
            gq = rope(dq[rows, :], b0, -1.0) * 0.125
            gk = rope(dk[rows, :], b0, -1.0)
            gv = dv[rows, :]
            sm[layer, 4:5, 0:HL] = sm[layer, 4:5, 0:HL] + jnp.sum(gq, axis=0, keepdims=True)
            sm[layer, 5:6, 0:HL] = sm[layer, 5:6, 0:HL] + jnp.sum(gv, axis=0, keepdims=True)
            rk = pltpu.roll(gk, 192, 1)
            rv = pltpu.roll(gv, 128, 1)
            dqkv[rows, 0:256] = jnp.where(lane < 192, gq, rk).astype(BF)
            dqkv[rows, 256:512] = jnp.where(lane < 128, rk, rv).astype(BF)
            dqkv[rows, 512:768] = jnp.where(lane < 64, rv, 0.0).astype(BF)

        for k in range(1, 4):
            part_copy(1 if layer == 1 else 2, k).wait_send()
        for k in (1, 2, 3, 0):
            rows = pl.ds(pl.multiple_of((t ^ k) * chunk, chunk), chunk)
            da_in = dqkv[rows, :]
            du_in = du[rows, :]
            m = mu[layer, rows, :]
            r = rstd[layer, rows, :]
            for j in range(width // 256):
                cols = slice(j * 256, (j + 1) * 256)
                da = mm(da_in, w[layer, 0, cols, :], NT)
                dm = mm(du_in, w[layer, 1, cols, :], NT)
                unit = (x[layer, rows, cols].astype(F32) - m) * r
                sums = [da * unit, dm * unit, da, dm]
                for i in range(4):
                    sm[layer, i : i + 1, cols] = sm[layer, i : i + 1, cols] + jnp.sum(
                        sums[i], axis=0, keepdims=True
                    )
                e = da * prow(layer, 0, cols) + dm * prow(layer, 1, cols)
                if k:
                    sendb[k - 1, :, cols] = e.astype(BF)
                else:
                    ownp[phase % 2, :, cols] = e
            if k:
                part_copy(phase, k).start()
        grad_part(layer, 0, buf)

    def finish_e(layer):
        phase = 3 - layer
        for k in range(1, 4):
            part_copy(phase, k).wait_recv()
        stage = gst.at[1 - layer]
        given = cotv if layer == 1 else gst.at[0]
        resid = jnp.zeros((1, width), F32)

        @pl.loop(0, chunk // sub)
        def _(i):
            r = pl.ds(pl.multiple_of(i * sub, sub), sub)
            rows = pl.ds(pl.multiple_of(t * chunk + i * sub, sub), sub)
            e = ownp[phase % 2, r, :]
            for k in range(3):
                e = e + recvb[phase % 2, k, r, :].astype(F32)
            rs = rstd[layer, rows, :]
            unit = (x[layer, rows, :].astype(F32) - mu[layer, rows, :]) * rs
            g = given[r, :]
            sm[layer, 7:8, :] = sm[layer, 7:8, :] + jnp.sum(g, axis=0, keepdims=True)
            d = rs * (
                e
                - jnp.mean(e, axis=-1, keepdims=True)
                - unit * jnp.mean(e * unit, axis=-1, keepdims=True)
            )
            g = g + d
            stage[r, :] = g
            if layer == 1:
                gb[0, rows, :] = g.astype(BF)

        if layer == 1:
            for k in range(1, 4):
                g_copy(0, k).start()
        place(layer, stage, out_g, 2 + layer)

    forward_layer(0)
    finish_y(0)
    forward_layer(1)
    backward_layer(1, gw, lambda p: None)
    finish_y(1)
    finish_e(1)
    renorm_all(0)
    for p in (2, 1, 0):
        reduce_cores(1, p, gw)
    late = w.at[1]
    for p in range(3):
        for j in range(1, n):
            w_copy(p, j).wait_send()

        @pl.when(s == 0)
        def _():
            forward(0, p).wait_send()

        @pl.when(s == 1)
        def _():
            forward(1, p).wait_send()

    backward_layer(0, late, lambda p: reduce_cores(0, p, late))
    finish_e(0)

    to_sib = remote(sm.at[1 - s], smr, sms.at[0], smrs.at[0], sib)
    to_sib.start()
    to_sib.wait()
    smt[...] = sm[s] + smr[...]
    for j in range(1, n):
        remote(
            smt, smz.at[j - 1], sms.at[j], smrs.at[j], (s, other_z(j), t)
        ).start()
    reduce_cores(0, 0, late)
    for j in range(1, n):
        remote(smt, smz.at[j - 1], sms.at[j], smrs.at[j], (s, other_z(j), t)).wait()
    total = smt[...]
    for j in range(1, n):
        total = total + smz[j - 1]
    tall[t] = total

    def small_copy(k):
        return remote(tall.at[t], tall.at[t], sms.at[n + k - 1], smrs.at[n + k - 1], plane(k))

    for k in range(1, 4):
        small_copy(k).start()

    for p in (2, 1, 0):
        for j in range(1, n):
            z_copy(p, j, late).wait_recv()

            @pl.loop(0, rows_z // step)
            def _(i):
                r = pl.ds(pl.multiple_of(i * step, 16), step)
                wacc[p, r, :] = wacc[p, r, :] + zrecv[p, j - 1, r, :].astype(F32)

        pltpu.make_async_copy(wacc.at[p], out_w.at[p], lsem.at[p]).start()
    for k in range(1, 4):
        small_copy(k).wait_send()
        remote(
            tall.at[t ^ k], tall.at[t ^ k], sms.at[n + k - 1], smrs.at[n + k - 1], plane(k)
        ).wait_recv()
    out_s[...] = tall[...]

    for p in range(3):
        pltpu.make_async_copy(wacc.at[p], out_w.at[p], lsem.at[p]).wait()
        for j in range(1, n):
            z_copy(p, j, late).wait_send()

    for k in range(1, 4):
        for layer in range(2):
            x_copy(layer, k).wait_send()
            g_copy(layer, k).wait_send()
        part_copy(3, k).wait_send()
    placed(1, yst, out_y, 1)
    placed(1, gst.at[0], out_g, 3)
    placed(0, gst.at[1], out_g, 2)
    remote(yst, out_y.at[1 - s], osend.at[0], orecv.at[0], sib).wait_recv()
    remote(gst.at[0], out_g.at[1 - s], osend.at[0], orecv.at[1], sib).wait_recv()


def rotary_rows(length, heads):
    rate = np.zeros((HL,), np.float64)
    for h in range(heads):
        for j in range(ROT // 2):
            value = math.exp(j * (-2.0 * math.log(10000.0) / ROT))
            rate[h * HEAD_DIM + j] = value
            rate[h * HEAD_DIM + j + ROT // 2] = value
    live = (np.arange(HL) < heads * HEAD_DIM).astype(np.float64)
    starts = np.arange(length // BQ)[:, None] * BQ * rate[None]
    offsets = np.arange(BQ)[:, None] * rate[None]
    first = np.stack([np.cos(starts), np.sin(starts)])[:, :, None].astype(np.float32)
    second = np.stack([np.cos(offsets) * live, np.sin(offsets) * live]).astype(np.float32)
    return first, second


def body(
    n,
    inputs,
    segment_ids,
    cotangent,
    qkv_weight,
    out_weight,
    up_weight,
    down_weight,
    norm_gain,
    norm_bias,
    qv_bias,
    up_bias,
    resid_bias,
):
    column = lax.axis_index("tensor")
    micro, _, chunk, width = inputs.shape
    length = segment_ids.shape[2]
    head_cols = qkv_weight.shape[3]
    rows_z = qkv_weight.shape[2]
    ff_local = up_weight.shape[2]
    heads = head_cols // HEAD_DIM
    assert micro == 2 and length == 4 * chunk and ff_local == width
    assert head_cols == 192 and width == 768

    packed = jnp.concatenate(
        [qkv_weight[0, 0], qkv_weight[0, 1], qkv_weight[0, 2], out_weight[0].T], axis=1
    )
    w_in = jnp.stack([packed, up_weight[0], down_weight[0].T])
    qv_local = lax.dynamic_slice_in_dim(qv_bias[0], column * head_cols, head_cols, 1)
    qv_local = jnp.pad(qv_local, ((0, 0), (0, width - head_cols)))
    up_local = lax.dynamic_slice_in_dim(up_bias, column * ff_local, ff_local, 1)
    par_in = jnp.concatenate([norm_gain[0], norm_bias[0], qv_local, up_local, resid_bias], axis=0)
    first, second = rotary_rows(length, heads)
    seg = segment_ids.reshape(micro, length)

    vm = pl.BlockSpec(memory_space=pltpu.VMEM)
    anywhere = pl.BlockSpec(memory_space=pl.ANY)
    blk = heads * BQ
    nblk = length // BQ
    dma = pltpu.SemaphoreType.DMA

    def vmem(*shape, dtype=BF):
        return pltpu.VMEM(shape, dtype)

    scratch = dict(
        w=vmem(2, 3, width, width),
        x=vmem(2, length, width),
        an=vmem(length, width),
        mn=vmem(length, width),
        mu=vmem(2, length, 1, dtype=F32),
        rstd=vmem(2, length, 1, dtype=F32),
        qb=vmem(2, length, HL),
        kb=vmem(2, length, HL),
        vb=vmem(2, length, HL),
        cb=vmem(2, length, HL),
        lse=vmem(2, nblk, 1, blk, dtype=F32),
        slope=vmem(2, length, width),
        hid=vmem(2, length, width),
        gb=vmem(2, length, width),
        du=vmem(length, width),
        dqkv=vmem(length, width),
        dc=vmem(length, HL),
        dq=vmem(length, HL, dtype=F32),
        dk=vmem(length, HL, dtype=F32),
        dv=vmem(length, HL, dtype=F32),
        bias=vmem(nblk, BK, BQ),
        pscr=vmem(BK, blk, dtype=F32),
        dpscr=vmem(BK, blk, dtype=F32),
        sendb=vmem(3, chunk, width),
        recvb=vmem(2, 3, chunk, width),
        ownp=vmem(2, chunk, width, dtype=F32),
        gw=vmem(3, width, width),
        gsr=vmem(3, width, width),
        zrecv=vmem(3, n - 1, rows_z, width),
        wacc=vmem(3, rows_z, width, dtype=F32),
        cotv=vmem(chunk, width, dtype=F32),
        yst=vmem(chunk, width, dtype=F32),
        gst=vmem(2, chunk, width, dtype=F32),
        segc=vmem(length, 1, dtype=jnp.int32),
        par=vmem(2, 8, width, dtype=F32),
        sm=vmem(2, 8, width, dtype=F32),
        smr=vmem(8, width, dtype=F32),
        smt=vmem(8, width, dtype=F32),
        smz=vmem(n - 1, 8, width, dtype=F32),
        tall=vmem(4, 8, width, dtype=F32),
        lsem=dma((8,)),
        psem=dma((2,)),
        xs=dma((2, 3)),
        xr=dma((2, 3)),
        gs=dma((2, 3)),
        gr=dma((2, 3)),
        ws=dma((3, n - 1)),
        wr=dma((3, n - 1)),
        fs=dma((3,)),
        fr=dma((3,)),
        rss=dma((4, 3)),
        rsr=dma((4, 3)),
        osend=dma((4,)),
        orecv=dma((2,)),
        ghs=dma((3,)),
        ghr=dma((3,)),
        zs=dma((3, n - 1)),
        zr=dma((3, n - 1)),
        sms=dma((n + 3,)),
        smrs=dma((n + 3,)),
    )
    out_y, out_g, out_w, out_s = pl.pallas_call(
        functools.partial(kernel, n, heads),
        out_shape=(
            jax.ShapeDtypeStruct((2, chunk, width), F32),
            jax.ShapeDtypeStruct((2, chunk, width), F32),
            jax.ShapeDtypeStruct((3, rows_z, width), F32),
            jax.ShapeDtypeStruct((4, 8, width), F32),
        ),
        in_specs=[anywhere, anywhere, anywhere, vm, anywhere, anywhere, vm, vm],
        out_specs=(anywhere, anywhere, anywhere, vm),
        scratch_shapes=list(scratch.values()),
        compiler_params=pltpu.CompilerParams(
            collective_id=0, has_side_effects=True, vmem_limit_bytes=67043328
        ),
        name="two_layers",
    )(
        inputs.reshape(micro, chunk, width),
        cotangent.reshape(micro, chunk, width),
        seg[:, :, None],
        seg,
        w_in,
        par_in,
        jnp.asarray(first),
        jnp.asarray(second),
    )
    qkv_grad = jnp.stack([out_w[0, :, i * head_cols : (i + 1) * head_cols] for i in range(3)])
    sums = jnp.sum(out_s, axis=0)
    return (
        out_y.reshape(1, micro, 1, chunk, width),
        out_g.reshape(1, micro, 1, chunk, width),
        qkv_grad[None],
        out_w[0, :, 3 * head_cols :].T[None],
        out_w[1][None],
        out_w[2].T[None],
        sums[None, 0:2],
        sums[None, 2:4],
        out_s[:, 4:6, :head_cols].transpose(1, 0, 2).reshape(1, 2, -1),
        out_s[:, 6, :].reshape(1, -1),
        sums[None, 7],
    )


def solution(mesh):
    return jax.shard_map(
        functools.partial(body, mesh.shape["dp"]),
        mesh=mesh,
        in_specs=(
            P(None, "dp", "tensor", None),
            P(None, "dp", None),
            P(None, "dp", "tensor", None),
            P("section", None, "dp", "tensor"),
            P("section", "tensor", "dp"),
            P("section", "dp", "tensor"),
            P("section", "tensor", "dp"),
            P("section", None, None),
            P("section", None, None),
            P("section", None, None),
            P("section", None),
            P("section", None),
        ),
        out_specs=(
            P("section", None, "dp", "tensor", None),
            P("section", None, "dp", "tensor", None),
            P("section", None, "dp", "tensor"),
            P("section", "tensor", "dp"),
            P("section", "dp", "tensor"),
            P("section", "tensor", "dp"),
            P("section", None, None),
            P("section", None, None),
            P("section", None, None),
            P("section", None),
            P("section", None),
        ),
        check_vma=False,
    )
```

```python
import functools
import math

import jax
import jax.numpy as jnp
import numpy as np
from jax import lax
from jax.experimental import pallas as pl
from jax.experimental.pallas import tpu as pltpu
from jax.sharding import PartitionSpec as P

HEAD_DIM = 64
ROT = 16
SEG_MOST = 384
EPS = 1e-05
MASKED = -1e30
ROOT_HALF = 0.7071067811865476
INV_ROOT_TAU = 0.3989422804014327

BF = jnp.bfloat16
F32 = jnp.float32
MESH = pl.DeviceIdType.MESH

NN = (((1,), (0,)), ((), ()))
NT = (((1,), (1,)), ((), ()))
TN = (((0,), (0,)), ((), ()))

BQ = 128
BK = BQ + SEG_MOST
HL = 256
QO, KO, VO, OO = 0, 192, 384, 576


def mm(a, b, dims):
    return lax.dot_general(a, b, dims, preferred_element_type=F32)


def lane_iota(rows, cols=HL):
    return lax.broadcasted_iota(jnp.int32, (rows, cols), 1)


def remote(src, dst, send, recv, dev):
    return pltpu.make_async_remote_copy(
        src_ref=src, dst_ref=dst, send_sem=send, recv_sem=recv, device_id=dev, device_id_type=MESH
    )


def kernel(
    n,
    heads,
    x_in,
    cot_in,
    seg_in,
    qkv_in,
    wo_in,
    up_in,
    down_in,
    gain_in,
    shift_in,
    qv_in,
    upb_in,
    resid_in,
    taba,
    tabb,
    out_y,
    out_g,
    out_w,
    out_s,
    w,
    x,
    an,
    mn,
    mu,
    rstd,
    qb,
    kb,
    vb,
    cb,
    lse,
    slope,
    hid,
    gb,
    du,
    dqkv,
    dc,
    dq,
    dk,
    dv,
    bias,
    pscr,
    dpscr,
    sendb,
    recvb,
    relayed,
    ownp,
    gw,
    gsr,
    zrecv,
    wacc,
    cotv,
    yst,
    gst,
    segc,
    segr,
    par,
    sm,
    smr,
    smt,
    smz,
    tall,
    lsem,
    psem,
    xs,
    xr,
    agx,
    agxr,
    agg,
    aggr,
    gs,
    gr,
    ws,
    wr,
    fs,
    fr,
    rss,
    rsr,
    osend,
    orecv,
    ghs,
    ghr,
    zs,
    zr,
    sms,
    smrs,
):
    s = lax.axis_index("section")
    z = lax.axis_index("dp")
    t = lax.axis_index("tensor")
    sib = (1 - s, z, t)
    width = x.shape[2]
    length = x.shape[1]
    chunk = length // 4
    rows_z = up_in.shape[1]
    half = chunk // 2
    nblk = length // BQ
    own = pl.ds(t * chunk, chunk)
    zrows = pl.ds(z * rows_z, rows_z)

    def plane(k):
        return (s, z, t ^ k)

    def other_z(j):
        return lax.rem(z + j, n)

    lx = pltpu.make_async_copy(x_in.at[s], x.at[0, own], lsem.at[0])
    lc = pltpu.make_async_copy(cot_in.at[s], cotv, lsem.at[1])
    lu = pltpu.make_async_copy(up_in.at[0], w.at[s, 1, zrows], lsem.at[3])
    ld = pltpu.make_async_copy(down_in, w.at[s, 2, zrows], lsem.at[4])
    lx.start()
    lu.start()
    ld.start()
    lc.start()

    head_cols = heads * HEAD_DIM

    def picks(first):
        rows = lax.broadcasted_iota(jnp.int32, (head_cols, width), 0)
        cols = lax.broadcasted_iota(jnp.int32, (head_cols, width), 1)
        return (rows + first == cols).astype(F32).astype(BF)

    packed = mm(qkv_in[0, 0], picks(QO), NN) + mm(qkv_in[0, 1], picks(KO), NN)
    packed = packed + mm(qkv_in[0, 2], picks(VO), NN) + mm(wo_in[0], picks(OO), TN)
    w[s, 0, zrows, :] = packed.astype(BF)

    par[s, 0:2, :] = gain_in[0]
    par[s, 2:4, :] = shift_in[0]
    par[s, 4:6, :] = qv_in[0]
    par[s, 6:7, :] = upb_in[0:1, pl.ds(pl.multiple_of(t * width, 128), width)]
    par[s, 7:8, :] = resid_in[...]
    rows8 = par[s]
    turned = rows8
    for i in range(1, 4):
        turned = jnp.where(t == i, pltpu.roll(rows8, width - i * head_cols, 1), turned)
    row = lax.broadcasted_iota(jnp.int32, (8, width), 0)
    par[s] = jnp.where((row == 4) | (row == 5), turned, rows8)

    barrier = pltpu.get_barrier_semaphore()
    pl.semaphore_signal(barrier, inc=1, device_id=sib, device_id_type=MESH)
    for k in range(1, 4):
        pl.semaphore_signal(barrier, inc=1, device_id=plane(k), device_id_type=MESH)
    for j in range(1, n):
        pl.semaphore_signal(barrier, inc=1, device_id=(s, other_z(j), t), device_id_type=MESH)
    pl.semaphore_wait(barrier, 4 + n - 1)

    right = (s, lax.rem(z + 1, n), t)
    left = (s, lax.rem(z + n - 1, n), t)

    def w_rows(origin):
        return pl.ds(origin * rows_z, rows_z)

    def line_copy(p, origin, dev):
        up = dev is right
        i = 0 if up else 1
        return remote(
            w.at[0, p, w_rows(origin)],
            w.at[0, p, w_rows(origin)],
            ws.at[i, p, origin],
            wr.at[i, p, origin],
            dev,
        )

    def across(p, origin):
        rows = w_rows(origin)
        return remote(w.at[0, p, rows], w.at[0, p, rows], fs.at[p, origin], fr.at[p, origin], sib)

    def w_copy(p, j):
        return remote(
            w.at[1, p, zrows],
            w.at[1, p, zrows],
            ws.at[0, p, j - 1],
            wr.at[0, p, j - 1],
            (s, other_z(j), t),
        )

    def w_arrival(p, j):
        rows = w_rows(other_z(n - j))
        return remote(
            w.at[1, p, rows], w.at[1, p, rows], ws.at[0, p, j - 1], wr.at[0, p, j - 1], sib
        )

    def forward(p):
        return remote(w.at[1, p], w.at[1, p], fs.at[p, 0], fr.at[p, 0], sib)

    def x_copy(k):
        return remote(x.at[0, own], x.at[0, own], xs.at[k - 1], xr.at[k - 1], plane(k))

    def x_arrival(k):
        rows = pl.ds((t ^ k) * chunk, chunk)
        return remote(x.at[0, rows], x.at[0, rows], xs.at[k - 1], xr.at[k - 1], plane(k))

    def g_copy(k):
        return remote(gb.at[1, own], gb.at[1, own], gs.at[k - 1], gr.at[k - 1], plane(k))

    def g_arrival(k):
        rows = pl.ds((t ^ k) * chunk, chunk)
        return remote(gb.at[1, rows], gb.at[1, rows], gs.at[k - 1], gr.at[k - 1], plane(k))

    hops = ((0, 0, 1), (0, 1, 2), (0, 1, 1), (0, 0, 2), (1, 0, 2), (2, 1, 1))

    def gather_copy(buf, send, recv, i):
        k, h, to = hops[i]
        rows = pl.ds((t ^ k) * chunk + h * half, half)
        return remote(buf.at[rows], buf.at[rows], send.at[i], recv.at[i], plane(to))

    def gather_arrival(buf, send, recv, i):
        k, h, to = hops[i]
        rows = pl.ds((t ^ k ^ to) * chunk + h * half, half)
        return remote(buf.at[rows], buf.at[rows], send.at[i], recv.at[i], plane(to))

    def gather_start(buf, send, recv):
        for i in range(4):
            gather_copy(buf, send, recv, i).start()

    def gather_pass(buf, send, recv):
        gather_arrival(buf, send, recv, 0).wait_recv()
        gather_copy(buf, send, recv, 4).start()
        gather_arrival(buf, send, recv, 1).wait_recv()
        gather_copy(buf, send, recv, 5).start()

    def gather_wait(buf, send, recv, k):
        for i in {1: (2,), 2: (3,), 3: (4, 5)}[k]:
            gather_arrival(buf, send, recv, i).wait_recv()

    def arrive(buf, send, recv, k):
        for i in range(1, 4):

            @pl.when(k == i)
            def _():
                gather_wait(buf, send, recv, i)

    def part_copy(phase, i):
        low, high = pl.ds(0, half), pl.ds(half, half)
        bank = phase % 2
        src, dst, to = (
            (sendb.at[2, low], relayed.at[bank, 0], 1),
            (sendb.at[2, high], relayed.at[bank, 1], 2),
            (sendb.at[0, low], recvb.at[bank, 0, low], 1),
            (sendb.at[1, high], recvb.at[bank, 1, high], 2),
            (sendb.at[1, low], recvb.at[bank, 1, low], 2),
            (sendb.at[0, high], recvb.at[bank, 0, high], 1),
        )[i]
        return remote(src, dst, rss.at[phase, i], rsr.at[phase, i], plane(to))

    def parts_start(phase, k):
        for i in {3: (0, 1), 1: (2,), 2: (3,)}[k]:
            part_copy(phase, i).start()

    def parts_pass(phase):
        for i in range(2):
            part_copy(phase, i).wait_recv()
            rows = slice(i * half, (i + 1) * half)
            mine = sendb[1 - i, rows, :].astype(F32)
            sendb[1 - i, rows, :] = (mine + relayed[phase % 2, i].astype(F32)).astype(BF)
            part_copy(phase, 4 + i).start()

    def parts_sent(phase):
        for i in range(6):
            part_copy(phase, i).wait_send()

    def parts_wait(phase):
        for i in range(2, 6):
            part_copy(phase, i).wait_recv()

    ag_x = (x.at[1], agx, agxr)
    ag_g = (gb.at[0], agg, aggr)

    def send_own(p):
        @pl.when(z + 1 < n)
        def _():
            line_copy(p, z, right).start()

        @pl.when(z > 0)
        def _():
            line_copy(p, z, left).start()

    @pl.when(s == 0)
    def _():
        send_own(0)

    lx.wait()
    for k in range(1, 4):
        x_copy(k).start()
    par_copy = remote(par.at[s], par.at[s], psem.at[0], psem.at[1], sib)
    par_copy.start()
    lu.wait()
    ld.wait()

    @pl.when(s == 0)
    def _():
        for p in range(3):
            across(p, z).start()

    lc.wait()
    gb[1, own, :] = cotv[...].astype(BF)
    for k in range(1, 4):
        g_copy(k).start()

    for i in range(length // BQ):
        cols = slice(i * BQ, (i + 1) * BQ)
        ids = jnp.where(s == 0, seg_in[0, :, cols], seg_in[1, :, cols]).astype(F32)
        segr[:, cols] = ids
        segc[cols, :] = jnp.broadcast_to(ids, (BQ, BQ)).T

    @pl.loop(0, nblk)
    def _(b):
        q0 = pl.multiple_of(b * BQ, BQ)
        k0 = pl.multiple_of(jnp.maximum(b * BQ - SEG_MOST, 0), BQ)
        seg_k = segc[pl.ds(k0, BK), :]
        seg_q = segr[:, pl.ds(q0, BQ)]
        kpos = lax.broadcasted_iota(jnp.int32, (BK, BQ), 0) + k0
        qpos = lax.broadcasted_iota(jnp.int32, (BK, BQ), 1) + q0
        allowed = (seg_k == seg_q) & (kpos <= qpos)
        bias[b] = jnp.where(allowed, 0.0, MASKED).astype(BF)

    par_wait = remote(par.at[1 - s], par.at[1 - s], psem.at[0], psem.at[1], sib)
    par_copy.wait_send()
    par_wait.wait_recv()

    @pl.loop(0, 2)
    def _(i):
        sm[i] = jnp.zeros((8, width), F32)

    def first_w(p):
        @pl.when(s == 0)
        def _():
            for d in range(1, n):

                @pl.when(z >= d)
                def _():
                    origin = jnp.maximum(z - d, 0)
                    line_copy(p, origin, right).wait_recv()

                    @pl.when(z + 1 < n)
                    def _():
                        line_copy(p, origin, right).start()

                    across(p, origin).start()

                @pl.when(z + d < n)
                def _():
                    origin = jnp.minimum(z + d, n - 1)
                    line_copy(p, origin, left).wait_recv()

                    @pl.when(z > 0)
                    def _():
                        line_copy(p, origin, left).start()

                    across(p, origin).start()

                if d == 1 and p < 2:
                    send_own(p + 1)

        @pl.when(s == 1)
        def _():
            for origin in range(n):
                across(p, origin).wait_recv()

    def first_w_sent():
        @pl.when(s == 0)
        def _():
            for p in range(3):
                for origin in range(n):

                    @pl.when((z >= origin) & (z + 1 < n))
                    def _():
                        line_copy(p, origin, right).wait_send()

                    @pl.when((z <= origin) & (z > 0))
                    def _():
                        line_copy(p, origin, left).wait_send()

                    across(p, origin).wait_send()

    def second_w_send():
        @pl.when(s == 1)
        def _():
            for p in range(3):
                for j in range(1, n):
                    w_copy(p, j).start()

    def second_w_pass(p):
        @pl.when(s == 1)
        def _():
            for j in range(1, n):
                w_arrival(p, j).wait_recv()
            forward(p).start()

    def second_w_wait(p):
        @pl.when(s == 0)
        def _():
            forward(p).wait_recv()

    def second_w_sent():
        @pl.when(s == 1)
        def _():
            for p in range(3):
                for j in range(1, n):
                    w_copy(p, j).wait_send()
                forward(p).wait_send()

    def prow(layer, r, cols=None):
        if cols is None:
            return par[layer, r : r + 1, :]
        return par[layer, r : r + 1, cols]

    def rope_tables(b, sign):
        ca = taba[0, b]
        sa = taba[1, b]
        c0 = tabb[0]
        s0 = tabb[1]
        cos = ca * c0 - sa * s0
        sin = sa * c0 + ca * s0
        lane = lane_iota(BQ) & (HEAD_DIM - 1)
        return cos, jnp.where(lane < ROT // 2, -sign, sign) * sin

    def rope(u, b, sign):
        halves = []
        lane = lane_iota(BQ) & (HEAD_DIM - 1)
        for i in range(u.shape[0] // BQ):
            part = u[i * BQ : (i + 1) * BQ]
            cos, sin = rope_tables(b + i, sign)
            partner = jnp.where(
                lane < ROT // 2,
                pltpu.roll(part, HL - ROT // 2, 1),
                pltpu.roll(part, ROT // 2, 1),
            )
            halves.append(part * cos + partner * sin)
        return jnp.concatenate(halves, axis=0)

    def stack_heads(block):
        lane = lane_iota(BQ) >> 6
        return jnp.concatenate(
            [jnp.where(lane == h, block, jnp.zeros_like(block)) for h in range(heads)], axis=0
        )

    sub = 64

    def norm_chunk(layer, c):
        @pl.loop(0, chunk // sub)
        def _(i):
            rows = pl.ds(pl.multiple_of(c * chunk + i * sub, sub), sub)
            v = x[layer, rows, :].astype(F32)
            m = jnp.mean(v, axis=-1, keepdims=True)
            v = v - m
            r = lax.rsqrt(jnp.mean(v * v, axis=-1, keepdims=True) + EPS)
            mu[layer, rows, :] = m
            rstd[layer, rows, :] = r
            v = v * r
            an[rows, :] = (v * prow(layer, 0) + prow(layer, 2)).astype(BF)
            mn[rows, :] = (v * prow(layer, 1) + prow(layer, 3)).astype(BF)

    def renorm_all(layer):
        @pl.loop(0, length // sub)
        def _(i):
            rows = pl.ds(pl.multiple_of(i * sub, sub), sub)
            v = (x[layer, rows, :].astype(F32) - mu[layer, rows, :]) * rstd[layer, rows, :]
            an[rows, :] = (v * prow(layer, 0) + prow(layer, 2)).astype(BF)
            mn[rows, :] = (v * prow(layer, 1) + prow(layer, 3)).astype(BF)

    def project_in(layer, c):
        rows = pl.ds(pl.multiple_of(c * chunk, chunk), chunk)
        a = an[rows, :]
        b0 = c * (chunk // BQ)
        lane = lane_iota(chunk)
        u = mm(a, w[layer, 0, :, QO : QO + HL], NN) + prow(layer, 4, slice(0, HL))
        qb[layer, rows, :] = (rope(u, b0, 1.0) * 0.125).astype(BF)
        u = mm(a, w[layer, 0, :, KO - 64 : KO - 64 + HL], NN)
        kb[layer, rows, :] = rope(pltpu.roll(u, HL - 64, 1), b0, 1.0).astype(BF)
        u = mm(a, w[layer, 0, :, VO : VO + HL], NN) + prow(layer, 5, slice(0, HL))
        vb[layer, rows, :] = jnp.where(lane < heads * HEAD_DIM, u, 0.0).astype(BF)

    def attend(layer):
        @pl.loop(0, nblk)
        def _(b):
            q0 = pl.multiple_of(b * BQ, BQ)
            k0 = pl.multiple_of(jnp.maximum(b * BQ - SEG_MOST, 0), BQ)
            qm = stack_heads(qb[layer, pl.ds(q0, BQ), :])
            top = None
            for i in range(BK // BQ):
                keys = kb[layer, pl.ds(k0 + i * BQ, BQ), :]
                blk = bias[b, i * BQ : (i + 1) * BQ, :].astype(F32)
                sc = mm(keys, qm, NT) + jnp.concatenate([blk] * heads, axis=1)
                pscr[i * BQ : (i + 1) * BQ, :] = sc
                peak = jnp.max(sc, axis=0, keepdims=True)
                top = peak if top is None else jnp.maximum(top, peak)
            total = None
            for i in range(BK // BQ):
                e = jnp.exp(pscr[i * BQ : (i + 1) * BQ, :] - top)
                pscr[i * BQ : (i + 1) * BQ, :] = e
                part = jnp.sum(e, axis=0, keepdims=True)
                total = part if total is None else total + part
            lse[layer, b] = top + jnp.log(total)
            inv = 1.0 / total
            lane = lane_iota(BQ) >> 6
            ctx = jnp.zeros((BQ, HL), F32)
            vals = vb[layer, pl.ds(k0, BK), :]
            for h in range(heads):
                cols = slice(h * BQ, (h + 1) * BQ)
                ph = (pscr[:, cols] * inv[:, cols]).astype(BF)
                ctx = jnp.where(lane == h, mm(ph, vals, TN), ctx)
            cb[layer, pl.ds(q0, BQ), :] = pltpu.roll(ctx, HL - heads * HEAD_DIM, 1).astype(BF)

    def hidden(layer, c):
        rows = pl.ds(pl.multiple_of(c * chunk, chunk), chunk)
        a = mn[rows, :]
        for j in range(width // 256):
            cols = slice(j * 256, (j + 1) * 256)
            u = mm(a, w[layer, 1, :, cols], NN) + prow(layer, 6, cols)
            phi = 0.5 * (1.0 + lax.erf(u * ROOT_HALF))
            hid[layer, rows, cols] = (u * phi).astype(BF)
            slope[layer, rows, cols] = (phi + u * INV_ROOT_TAU * jnp.exp(-0.5 * u * u)).astype(BF)

    def project_out(layer):
        phase = layer
        if layer == 1:
            parts_sent(0)
        for k in (3, 1, 2, 0):
            rows = pl.ds(pl.multiple_of((t ^ k) * chunk, chunk), chunk)
            c = cb[layer, rows, :]
            h = hid[layer, rows, :]
            for j in range(width // 256):
                cols = slice(j * 256, (j + 1) * 256)
                y = mm(c, w[layer, 0, cols, 512:768], NT) + mm(h, w[layer, 2, cols, :], NT)
                if k:
                    sendb[k - 1, :, cols] = y.astype(BF)
                else:
                    ownp[phase % 2, :, cols] = y
            if k:
                parts_start(phase, k)

    def place(layer, stage, out, idx):
        @pl.when(s == layer)
        def _():
            pltpu.make_async_copy(stage, out.at[s], osend.at[idx]).start()

        @pl.when(s != layer)
        def _():
            remote(stage, out.at[s], osend.at[idx], orecv.at[idx // 2], sib).start()

    def placed(layer, stage, out, idx):
        @pl.when(s == layer)
        def _():
            pltpu.make_async_copy(stage, out.at[s], osend.at[idx]).wait()

        @pl.when(s != layer)
        def _():
            remote(stage, out.at[s], osend.at[idx], orecv.at[idx // 2], sib).wait_send()

    def finish_y(layer):
        phase = layer
        parts_wait(phase)
        if layer == 1:
            placed(0, yst, out_y, 0)

        @pl.loop(0, chunk // sub)
        def _(i):
            r = pl.ds(pl.multiple_of(i * sub, sub), sub)
            rows = pl.ds(pl.multiple_of(t * chunk + i * sub, sub), sub)
            y = x[layer, rows, :].astype(F32) + ownp[phase % 2, r, :] + prow(layer, 7)
            for k in range(2):
                y = y + recvb[phase % 2, k, r, :].astype(F32)
            yst[r, :] = y
            if layer == 0:
                x[1, rows, :] = y.astype(BF)

        if layer == 0:
            gather_start(*ag_x)
        place(layer, yst, out_y, layer)

    def reduce_start(layer, p, buf):
        @pl.when(s != layer)
        def _():
            remote(buf.at[p], gsr.at[p], ghs.at[p], ghr.at[p], sib).start()

    def z_copy(p, j, buf):
        rows = pl.ds(other_z(j) * rows_z, rows_z)
        return remote(
            buf.at[p, rows],
            zrecv.at[p, j - 1],
            zs.at[p, j - 1],
            zr.at[p, j - 1],
            (s, other_z(j), t),
        )

    step = 48

    def reduce_cores(layer, p, buf):
        @pl.when(s == layer)
        def _():
            remote(buf.at[p], gsr.at[p], ghs.at[p], ghr.at[p], sib).wait_recv()

            @pl.loop(0, rows_z // step)
            def _(i):
                r = pl.ds(pl.multiple_of(i * step, 16), step)
                q = pl.ds(pl.multiple_of(z * rows_z + i * step, 16), step)
                wacc[p, r, :] = buf[p, q, :].astype(F32) + gsr[p, q, :].astype(F32)

            for j in range(1, n):
                base = other_z(j) * rows_z

                @pl.loop(0, rows_z // step)
                def _(i):
                    q = pl.ds(pl.multiple_of(base + i * step, 16), step)
                    buf[p, q, :] = (buf[p, q, :].astype(F32) + gsr[p, q, :].astype(F32)).astype(BF)

                z_copy(p, j, buf).start()

        @pl.when(s != layer)
        def _():
            remote(buf.at[p], gsr.at[p], ghs.at[p], ghr.at[p], sib).wait_send()

    def grad_part(layer, p, buf):
        for j in range(width // 256):
            cols = slice(j * 256, (j + 1) * 256)
            if p == 2:
                buf[p, cols, :] = mm(gb[layer, :, cols], hid[layer], TN).astype(BF)
            elif p == 1:
                buf[p, cols, :] = mm(mn[:, cols], du[...], TN).astype(BF)
            else:
                buf[p, cols, 0:512] = mm(an[:, cols], dqkv[:, 0:512], TN).astype(BF)
                buf[p, cols, 512:768] = (
                    mm(an[:, cols], dqkv[:, 512:768], TN) + mm(gb[layer, :, cols], cb[layer], TN)
                ).astype(BF)
        reduce_start(layer, p, buf)

    def hidden_back(layer, c):
        rows = pl.ds(pl.multiple_of(c * chunk, chunk), chunk)
        g = gb[layer, rows, :]
        for j in range(width // 256):
            cols = slice(j * 256, (j + 1) * 256)
            d = mm(g, w[layer, 2, :, cols], NN) * slope[layer, rows, cols].astype(F32)
            sm[layer, 6:7, cols] = sm[layer, 6:7, cols] + jnp.sum(d, axis=0, keepdims=True)
            du[rows, cols] = d.astype(BF)
        d = pltpu.roll(mm(g, w[layer, 0, :, 512:768], NN), HL - 64, 1)
        lane = lane_iota(chunk)
        dc[rows, :] = jnp.where(lane < heads * HEAD_DIM, d, 0.0).astype(BF)

    def zero_sums():
        @pl.loop(0, length // sub)
        def _(i):
            rows = pl.ds(pl.multiple_of(i * sub, sub), sub)
            dk[rows, :] = jnp.zeros((sub, HL), F32)
            dv[rows, :] = jnp.zeros((sub, HL), F32)

    def attend_back(layer, first, last):
        @pl.loop(first, last)
        def _(b):
            q0 = pl.multiple_of(b * BQ, BQ)
            k0 = pl.multiple_of(jnp.maximum(b * BQ - SEG_MOST, 0), BQ)
            qm = stack_heads(qb[layer, pl.ds(q0, BQ), :])
            dm = stack_heads(dc[pl.ds(q0, BQ), :])
            ls = lse[layer, b]
            total = None
            for i in range(BK // BQ):
                krows = pl.ds(k0 + i * BQ, BQ)
                irows = slice(i * BQ, (i + 1) * BQ)
                blk = bias[b, irows, :].astype(F32)
                sc = mm(kb[layer, krows, :], qm, NT) + jnp.concatenate([blk] * heads, axis=1)
                pr = jnp.exp(sc - ls)
                dp = mm(vb[layer, krows, :], dm, NT)
                dv[krows, :] = dv[krows, :] + mm(pr.astype(BF), dm, NN)
                pscr[irows, :] = pr
                dpscr[irows, :] = dp
                part = jnp.sum(pr * dp, axis=0, keepdims=True)
                total = part if total is None else total + part
            lane = lane_iota(BQ) >> 6
            acc = [jnp.zeros((BQ, HL), F32) for _ in range(heads)]
            for i in range(BK // BQ):
                krows = pl.ds(k0 + i * BQ, BQ)
                irows = slice(i * BQ, (i + 1) * BQ)
                ds = (pscr[irows, :] * (dpscr[irows, :] - total)).astype(BF)
                dk[krows, :] = dk[krows, :] + mm(ds, qm, NN)
                keys = kb[layer, krows, :]
                for h in range(heads):
                    acc[h] = acc[h] + mm(ds[:, h * BQ : (h + 1) * BQ], keys, TN)
            out = jnp.zeros((BQ, HL), F32)
            for h in range(heads):
                out = jnp.where(lane == h, acc[h], out)
            dq[pl.ds(q0, BQ), :] = out

    def pack_qkv(layer):
        @pl.loop(0, 4)
        def _(c):
            rows = pl.ds(pl.multiple_of(c * chunk, chunk), chunk)
            b0 = c * (chunk // BQ)
            lane = lane_iota(chunk)
            gq = rope(dq[rows, :], b0, -1.0) * 0.125
            gk = rope(dk[rows, :], b0, -1.0)
            gv = dv[rows, :]
            sm[layer, 4:5, 0:HL] = sm[layer, 4:5, 0:HL] + jnp.sum(gq, axis=0, keepdims=True)
            sm[layer, 5:6, 0:HL] = sm[layer, 5:6, 0:HL] + jnp.sum(gv, axis=0, keepdims=True)
            rk = pltpu.roll(gk, 192, 1)
            rv = pltpu.roll(gv, 128, 1)
            dqkv[rows, 0:256] = jnp.where(lane < 192, gq, rk).astype(BF)
            dqkv[rows, 256:512] = jnp.where(lane < 128, rk, rv).astype(BF)
            dqkv[rows, 512:768] = jnp.where(lane < 64, rv, 0.0).astype(BF)

    def project_back(layer):
        phase = 3 - layer
        parts_sent(1 if layer == 1 else 2)
        for k in (3, 1, 2, 0):
            rows = pl.ds(pl.multiple_of((t ^ k) * chunk, chunk), chunk)
            da_in = dqkv[rows, :]
            du_in = du[rows, :]
            m = mu[layer, rows, :]
            r = rstd[layer, rows, :]
            for j in range(width // 256):
                cols = slice(j * 256, (j + 1) * 256)
                da = mm(da_in, w[layer, 0, cols, :], NT)
                dm = mm(du_in, w[layer, 1, cols, :], NT)
                unit = (x[layer, rows, cols].astype(F32) - m) * r
                sums = [da * unit, dm * unit, da, dm]
                for i in range(4):
                    sm[layer, i : i + 1, cols] = sm[layer, i : i + 1, cols] + jnp.sum(
                        sums[i], axis=0, keepdims=True
                    )
                e = da * prow(layer, 0, cols) + dm * prow(layer, 1, cols)
                if k:
                    sendb[k - 1, :, cols] = e.astype(BF)
                else:
                    ownp[phase % 2, :, cols] = e
            if k:
                parts_start(phase, k)

    def finish_e(layer):
        phase = 3 - layer
        parts_wait(phase)
        stage = gst.at[1 - layer]
        given = cotv if layer == 1 else gst.at[0]

        @pl.loop(0, chunk // sub)
        def _(i):
            r = pl.ds(pl.multiple_of(i * sub, sub), sub)
            rows = pl.ds(pl.multiple_of(t * chunk + i * sub, sub), sub)
            e = ownp[phase % 2, r, :]
            for k in range(2):
                e = e + recvb[phase % 2, k, r, :].astype(F32)
            rs = rstd[layer, rows, :]
            unit = (x[layer, rows, :].astype(F32) - mu[layer, rows, :]) * rs
            g = given[r, :]
            sm[layer, 7:8, :] = sm[layer, 7:8, :] + jnp.sum(g, axis=0, keepdims=True)
            d = rs * (
                e
                - jnp.mean(e, axis=-1, keepdims=True)
                - unit * jnp.mean(e * unit, axis=-1, keepdims=True)
            )
            g = g + d
            stage[r, :] = g
            if layer == 1:
                gb[0, rows, :] = g.astype(BF)

        if layer == 1:
            gather_start(*ag_g)
        place(layer, stage, out_g, 2 + layer)

    norm_chunk(0, t)
    first_w(0)
    for k in range(1, 4):
        x_arrival(k).wait_recv()
        norm_chunk(0, t ^ k)

    @pl.loop(0, 4)
    def _(c):
        project_in(0, c)

    attend(0)
    first_w(1)

    @pl.loop(0, 4)
    def _(c):
        hidden(0, c)

    first_w(2)
    second_w_send()
    project_out(0)
    parts_pass(0)
    second_w_pass(0)
    finish_y(0)

    second_w_wait(0)
    @pl.loop(0, 4)
    def _(k):
        arrive(*ag_x, k)
        norm_chunk(1, t ^ k)
        project_in(1, t ^ k)

        @pl.when(k == 0)
        def _():
            gather_pass(*ag_x)
            second_w_pass(1)
            second_w_wait(1)

        hidden(1, t ^ k)

    second_w_pass(2)
    attend(1)
    second_w_wait(2)
    project_out(1)

    for k in range(1, 4):
        g_arrival(k).wait_recv()
    zero_sums()

    @pl.loop(0, 4)
    def _(c):
        hidden_back(1, c)

    parts_pass(1)
    attend_back(1, 0, nblk)
    pack_qkv(1)
    project_back(1)
    grad_part(1, 2, gw)
    parts_pass(2)
    grad_part(1, 1, gw)
    grad_part(1, 0, gw)
    finish_y(1)
    finish_e(1)

    late = w.at[1]
    per = chunk // BQ
    first_w_sent()
    second_w_sent()
    zero_sums()

    @pl.loop(0, 8)
    def _(step_no):
        k = jnp.where(step_no < 2, 0, jnp.where(step_no < 5, step_no - 1, step_no - 4))

        @pl.when((step_no == 0) | ((step_no >= 2) & (step_no < 5)))
        def _():
            arrive(*ag_g, k)
            hidden_back(0, t ^ k)

        @pl.when(step_no == 5)
        def _():
            grad_part(0, 2, late)
            grad_part(0, 1, late)

        @pl.when(step_no == 6)
        def _():
            reduce_cores(0, 2, late)

        @pl.when(step_no == 7)
        def _():
            reduce_cores(0, 1, late)

        @pl.when((step_no == 1) | (step_no >= 5))
        def _():
            attend_back(0, (t ^ k) * per, ((t ^ k) + 1) * per)

        @pl.when(step_no == 1)
        def _():
            gather_pass(*ag_g)
            for p in (2, 1, 0):
                reduce_cores(1, p, gw)
            renorm_all(0)

    pack_qkv(0)
    project_back(0)
    grad_part(0, 0, late)
    parts_pass(3)
    reduce_cores(0, 0, late)
    finish_e(0)

    to_sib = remote(sm.at[1 - s], smr, sms.at[0], smrs.at[0], sib)
    to_sib.start()
    to_sib.wait()
    smt[...] = sm[s] + smr[...]
    for j in range(1, n):
        remote(
            smt, smz.at[j - 1], sms.at[j], smrs.at[j], (s, other_z(j), t)
        ).start()
    for j in range(1, n):
        remote(smt, smz.at[j - 1], sms.at[j], smrs.at[j], (s, other_z(j), t)).wait()
    total = smt[...]
    for j in range(1, n):
        total = total + smz[j - 1]
    tall[t] = total

    def small_copy(k):
        return remote(tall.at[t], tall.at[t], sms.at[n + k - 1], smrs.at[n + k - 1], plane(k))

    for k in range(1, 4):
        small_copy(k).start()

    for p in (2, 1, 0):
        for j in range(1, n):
            z_copy(p, j, late).wait_recv()

            @pl.loop(0, rows_z // step)
            def _(i):
                r = pl.ds(pl.multiple_of(i * step, 16), step)
                wacc[p, r, :] = wacc[p, r, :] + zrecv[p, j - 1, r, :].astype(F32)

        pltpu.make_async_copy(wacc.at[p], out_w.at[p], lsem.at[p]).start()
    for k in range(1, 4):
        small_copy(k).wait_send()
        remote(
            tall.at[t ^ k], tall.at[t ^ k], sms.at[n + k - 1], smrs.at[n + k - 1], plane(k)
        ).wait_recv()
    out_s[...] = tall[...]

    for p in range(3):
        pltpu.make_async_copy(wacc.at[p], out_w.at[p], lsem.at[p]).wait()
        for j in range(1, n):
            z_copy(p, j, late).wait_send()

    for k in range(1, 4):
        x_copy(k).wait_send()
        g_copy(k).wait_send()
    for i in range(6):
        gather_copy(*ag_x, i).wait_send()
        gather_copy(*ag_g, i).wait_send()
    parts_sent(3)
    placed(1, yst, out_y, 1)
    placed(1, gst.at[0], out_g, 3)
    placed(0, gst.at[1], out_g, 2)
    remote(yst, out_y.at[1 - s], osend.at[0], orecv.at[0], sib).wait_recv()
    remote(gst.at[0], out_g.at[1 - s], osend.at[0], orecv.at[1], sib).wait_recv()


def rotary_rows(length, heads):
    rate = np.zeros((HL,), np.float64)
    for h in range(heads):
        for j in range(ROT // 2):
            value = math.exp(j * (-2.0 * math.log(10000.0) / ROT))
            rate[h * HEAD_DIM + j] = value
            rate[h * HEAD_DIM + j + ROT // 2] = value
    live = (np.arange(HL) < heads * HEAD_DIM).astype(np.float64)
    starts = np.arange(length // BQ)[:, None] * BQ * rate[None]
    offsets = np.arange(BQ)[:, None] * rate[None]
    first = np.stack([np.cos(starts), np.sin(starts)])[:, :, None].astype(np.float32)
    second = np.stack([np.cos(offsets) * live, np.sin(offsets) * live]).astype(np.float32)
    return first, second


def body(
    n,
    inputs,
    segment_ids,
    cotangent,
    qkv_weight,
    out_weight,
    up_weight,
    down_weight,
    norm_gain,
    norm_bias,
    qv_bias,
    up_bias,
    resid_bias,
):
    micro, _, chunk, width = inputs.shape
    length = segment_ids.shape[2]
    head_cols = qkv_weight.shape[3]
    rows_z = qkv_weight.shape[2]
    ff_local = up_weight.shape[2]
    heads = head_cols // HEAD_DIM
    assert micro == 2 and length == 4 * chunk and ff_local == width
    assert head_cols == 192 and width == 768

    first, second = rotary_rows(length, heads)

    vm = pl.BlockSpec(memory_space=pltpu.VMEM)
    anywhere = pl.BlockSpec(memory_space=pl.ANY)
    blk = heads * BQ
    nblk = length // BQ
    dma = pltpu.SemaphoreType.DMA

    def vmem(*shape, dtype=BF):
        return pltpu.VMEM(shape, dtype)

    scratch = dict(
        w=vmem(2, 3, width, width),
        x=vmem(2, length, width),
        an=vmem(length, width),
        mn=vmem(length, width),
        mu=vmem(2, length, 1, dtype=F32),
        rstd=vmem(2, length, 1, dtype=F32),
        qb=vmem(2, length, HL),
        kb=vmem(2, length, HL),
        vb=vmem(2, length, HL),
        cb=vmem(2, length, HL),
        lse=vmem(2, nblk, 1, blk, dtype=F32),
        slope=vmem(2, length, width),
        hid=vmem(2, length, width),
        gb=vmem(2, length, width),
        du=vmem(length, width),
        dqkv=vmem(length, width),
        dc=vmem(length, HL),
        dq=vmem(length, HL, dtype=F32),
        dk=vmem(length, HL, dtype=F32),
        dv=vmem(length, HL, dtype=F32),
        bias=vmem(nblk, BK, BQ),
        pscr=vmem(BK, blk, dtype=F32),
        dpscr=vmem(BK, blk, dtype=F32),
        sendb=vmem(3, chunk, width),
        recvb=vmem(2, 2, chunk, width),
        relayed=vmem(2, 2, chunk // 2, width),
        ownp=vmem(2, chunk, width, dtype=F32),
        gw=vmem(3, width, width),
        gsr=vmem(3, width, width),
        zrecv=vmem(3, n - 1, rows_z, width),
        wacc=vmem(3, rows_z, width, dtype=F32),
        cotv=vmem(chunk, width, dtype=F32),
        yst=vmem(chunk, width, dtype=F32),
        gst=vmem(2, chunk, width, dtype=F32),
        segc=vmem(length, BQ, dtype=F32),
        segr=vmem(1, length, dtype=F32),
        par=vmem(2, 8, width, dtype=F32),
        sm=vmem(2, 8, width, dtype=F32),
        smr=vmem(8, width, dtype=F32),
        smt=vmem(8, width, dtype=F32),
        smz=vmem(n - 1, 8, width, dtype=F32),
        tall=vmem(4, 8, width, dtype=F32),
        lsem=dma((8,)),
        psem=dma((2,)),
        xs=dma((3,)),
        xr=dma((3,)),
        agx=dma((6,)),
        agxr=dma((6,)),
        agg=dma((6,)),
        aggr=dma((6,)),
        gs=dma((3,)),
        gr=dma((3,)),
        ws=dma((2, 3, n)),
        wr=dma((2, 3, n)),
        fs=dma((3, n)),
        fr=dma((3, n)),
        rss=dma((4, 6)),
        rsr=dma((4, 6)),
        osend=dma((4,)),
        orecv=dma((2,)),
        ghs=dma((3,)),
        ghr=dma((3,)),
        zs=dma((3, n - 1)),
        zr=dma((3, n - 1)),
        sms=dma((n + 3,)),
        smrs=dma((n + 3,)),
    )
    out_y, out_g, out_w, out_s = pl.pallas_call(
        functools.partial(kernel, n, heads),
        out_shape=(
            jax.ShapeDtypeStruct((2, chunk, width), F32),
            jax.ShapeDtypeStruct((2, chunk, width), F32),
            jax.ShapeDtypeStruct((3, rows_z, width), F32),
            jax.ShapeDtypeStruct((4, 8, width), F32),
        ),
        in_specs=[anywhere, anywhere, vm, vm, vm, anywhere, anywhere] + [vm] * 7,
        out_specs=(anywhere, anywhere, anywhere, vm),
        scratch_shapes=list(scratch.values()),
        compiler_params=pltpu.CompilerParams(
            collective_id=0, has_side_effects=True, vmem_limit_bytes=67043328
        ),
        name="two_layers",
    )(
        inputs.reshape(micro, chunk, width),
        cotangent.reshape(micro, chunk, width),
        segment_ids,
        qkv_weight,
        out_weight,
        up_weight,
        down_weight[0].T,
        norm_gain,
        norm_bias,
        qv_bias,
        up_bias,
        resid_bias,
        jnp.asarray(first),
        jnp.asarray(second),
    )
    qkv_grad = jnp.stack([out_w[0, :, i * head_cols : (i + 1) * head_cols] for i in range(3)])
    sums = jnp.sum(out_s, axis=0)
    return (
        out_y.reshape(1, micro, 1, chunk, width),
        out_g.reshape(1, micro, 1, chunk, width),
        qkv_grad[None],
        out_w[0, :, 3 * head_cols :].T[None],
        out_w[1][None],
        out_w[2].T[None],
        sums[None, 0:2],
        sums[None, 2:4],
        out_s[:, 4:6, :head_cols].transpose(1, 0, 2).reshape(1, 2, -1),
        out_s[:, 6, :].reshape(1, -1),
        sums[None, 7],
    )


def solution(mesh):
    return jax.shard_map(
        functools.partial(body, mesh.shape["dp"]),
        mesh=mesh,
        in_specs=(
            P(None, "dp", "tensor", None),
            P(None, "dp", None),
            P(None, "dp", "tensor", None),
            P("section", None, "dp", "tensor"),
            P("section", "tensor", "dp"),
            P("section", "dp", "tensor"),
            P("section", "tensor", "dp"),
            P("section", None, None),
            P("section", None, None),
            P("section", None, None),
            P("section", None),
            P("section", None),
        ),
        out_specs=(
            P("section", None, "dp", "tensor", None),
            P("section", None, "dp", "tensor", None),
            P("section", None, "dp", "tensor"),
            P("section", "tensor", "dp"),
            P("section", "dp", "tensor"),
            P("section", "tensor", "dp"),
            P("section", None, None),
            P("section", None, None),
            P("section", None, None),
            P("section", None),
            P("section", None),
        ),
        check_vma=False,
    )
```

```python
import functools
import math

import jax
import jax.numpy as jnp
import numpy as np
from jax import lax
from jax.experimental import pallas as pl
from jax.experimental.pallas import tpu as pltpu
from jax.sharding import PartitionSpec as P

HEAD_DIM = 64
ROT = 16
SEG_MOST = 384
EPS = 1e-05
MASKED = -1e30
ROOT_HALF = 0.7071067811865476
INV_ROOT_TAU = 0.3989422804014327

BF = jnp.bfloat16
F32 = jnp.float32
MESH = pl.DeviceIdType.MESH

NN = (((1,), (0,)), ((), ()))
NT = (((1,), (1,)), ((), ()))
TN = (((0,), (0,)), ((), ()))

BQ = 128
BK = BQ + SEG_MOST
HL = 256
QO, KO, VO, OO = 0, 192, 384, 576


def mm(a, b, dims):
    return lax.dot_general(a, b, dims, preferred_element_type=F32)


def lane_iota(rows, cols=HL):
    return lax.broadcasted_iota(jnp.int32, (rows, cols), 1)


def remote(src, dst, send, recv, dev):
    return pltpu.make_async_remote_copy(
        src_ref=src, dst_ref=dst, send_sem=send, recv_sem=recv, device_id=dev, device_id_type=MESH
    )


def kernel(
    n,
    heads,
    x_in,
    cot_in,
    seg_in,
    qkv_in,
    wo_in,
    up_in,
    down_in,
    gain_in,
    shift_in,
    qv_in,
    upb_in,
    resid_in,
    taba,
    tabb,
    out_y,
    out_g,
    out_w,
    out_s,
    w,
    x,
    an,
    mn,
    mu,
    rstd,
    qb,
    kb,
    vb,
    cb,
    lse,
    slope,
    hid,
    gb,
    du,
    dqkv,
    dc,
    dq,
    dk,
    dv,
    bias,
    pscr,
    dpscr,
    sendb,
    recvb,
    relayed,
    ownp,
    gw,
    gsr,
    zrecv,
    zacc,
    wacc,
    cotv,
    yst,
    gst,
    segc,
    segr,
    par,
    sm,
    smr,
    smt,
    smz,
    tall,
    lsem,
    psem,
    xs,
    xr,
    agx,
    agxr,
    agg,
    aggr,
    gs,
    gr,
    ws,
    wr,
    fs,
    fr,
    rss,
    rsr,
    osend,
    orecv,
    ghs,
    ghr,
    zs,
    zr,
    za,
    sms,
    smrs,
):
    s = lax.axis_index("section")
    z = lax.axis_index("dp")
    t = lax.axis_index("tensor")
    sib = (1 - s, z, t)
    width = x.shape[2]
    length = x.shape[1]
    chunk = length // 4
    rows_z = up_in.shape[1]
    half = chunk // 2
    nblk = length // BQ
    own = pl.ds(t * chunk, chunk)
    zrows = pl.ds(z * rows_z, rows_z)

    def plane(k):
        return (s, z, t ^ k)

    def other_z(j):
        return lax.rem(z + j, n)

    lx = pltpu.make_async_copy(x_in.at[s], x.at[0, own], lsem.at[0])
    lc = pltpu.make_async_copy(cot_in.at[s], cotv, lsem.at[1])
    lu = pltpu.make_async_copy(up_in.at[0], w.at[s, 1, zrows], lsem.at[3])
    ld = pltpu.make_async_copy(down_in, w.at[s, 2, zrows], lsem.at[4])
    lx.start()
    lu.start()
    ld.start()
    lc.start()

    barrier = pltpu.get_barrier_semaphore()
    pl.semaphore_signal(barrier, inc=1, device_id=sib, device_id_type=MESH)
    for k in range(1, 4):
        pl.semaphore_signal(barrier, inc=1, device_id=plane(k), device_id_type=MESH)
    for j in range(1, n):
        pl.semaphore_signal(barrier, inc=1, device_id=(s, other_z(j), t), device_id_type=MESH)
    pl.semaphore_wait(barrier, 4 + n - 1)

    head_cols = heads * HEAD_DIM

    def picks(first):
        rows = lax.broadcasted_iota(jnp.int32, (head_cols, width), 0)
        cols = lax.broadcasted_iota(jnp.int32, (head_cols, width), 1)
        return (rows + first == cols).astype(F32).astype(BF)

    def pack_share():
        packed = mm(qkv_in[0, 0], picks(QO), NN) + mm(qkv_in[0, 1], picks(KO), NN)
        packed = packed + mm(qkv_in[0, 2], picks(VO), NN) + mm(wo_in[0], picks(OO), TN)
        w[s, 0, zrows, :] = packed.astype(BF)

    def pack_params():
        par[s, 0:2, :] = gain_in[0]
        par[s, 2:4, :] = shift_in[0]
        par[s, 4:6, :] = qv_in[0]
        par[s, 6:7, :] = upb_in[0:1, pl.ds(pl.multiple_of(t * width, 128), width)]
        par[s, 7:8, :] = resid_in[...]
        rows8 = par[s]
        turned = rows8
        for i in range(1, 4):
            turned = jnp.where(t == i, pltpu.roll(rows8, width - i * head_cols, 1), turned)
        row = lax.broadcasted_iota(jnp.int32, (8, width), 0)
        par[s] = jnp.where((row == 4) | (row == 5), turned, rows8)

    def w_rows(origin):
        return pl.ds(origin * rows_z, rows_z)

    def w_step(p, origin, far, src=None):
        rows = w_rows(origin)
        i = {1: 0, 2: 1, -1: 2, -2: 3}[far]
        return remote(
            w.at[s, p, rows] if src is None else src,
            w.at[s, p, rows],
            ws.at[i, p, origin],
            wr.at[p, origin],
            (s, lax.rem(z + far + n, n), t),
        )

    def inside(far):
        return (z + far < n) if far > 0 else (z + far >= 0)

    def w_send(p, src=None):
        for far in (1, -1, 2, -2):

            @pl.when(inside(far))
            def _():
                w_step(p, z, far, src).start()

    def w_arrive(p, distances, passed, then):
        for e in distances:
            for sign in (1, -1):

                @pl.when(inside(-sign * e))
                def _():
                    origin = lax.rem(z - sign * e + n, n)
                    w_step(p, origin, sign).wait_recv()
                    if passed:
                        for far in (sign, 2 * sign):

                            @pl.when(inside(far))
                            def _():
                                w_step(p, origin, far).start()

                    if then is not None:
                        then(p, origin)

    def w_sent(p):
        for far in (1, -1, 2, -2):

            @pl.when(inside(far))
            def _():
                w_step(p, z, far).wait_send()

            sign = 1 if far > 0 else -1
            for e in range(2, n, 2):

                @pl.when(inside(-sign * e) & inside(far))
                def _():
                    w_step(p, lax.rem(z - sign * e + n, n), far).wait_send()

    def across(p, origin):
        rows = w_rows(origin)
        return remote(w.at[0, p, rows], w.at[0, p, rows], fs.at[p, origin], fr.at[p, origin], sib)

    def forward(p):
        return remote(w.at[1, p], w.at[1, p], fs.at[p, 0], fr.at[p, 0], sib)

    def g_copy(k):
        return remote(gb.at[1, own], gb.at[1, own], gs.at[k - 1], gr.at[k - 1], plane(k))

    def g_arrival(k):
        rows = pl.ds((t ^ k) * chunk, chunk)
        return remote(gb.at[1, rows], gb.at[1, rows], gs.at[k - 1], gr.at[k - 1], plane(k))

    hops = ((0, 0, 1), (0, 1, 2), (0, 1, 1), (0, 0, 2), (1, 0, 2), (2, 1, 1))

    def gather_copy(buf, send, recv, i):
        k, h, to = hops[i]
        rows = pl.ds((t ^ k) * chunk + h * half, half)
        return remote(buf.at[rows], buf.at[rows], send.at[i], recv.at[i], plane(to))

    def gather_arrival(buf, send, recv, i):
        k, h, to = hops[i]
        rows = pl.ds((t ^ k ^ to) * chunk + h * half, half)
        return remote(buf.at[rows], buf.at[rows], send.at[i], recv.at[i], plane(to))

    def gather_start(buf, send, recv):
        for i in range(4):
            gather_copy(buf, send, recv, i).start()

    def gather_pass(buf, send, recv):
        gather_arrival(buf, send, recv, 0).wait_recv()
        gather_copy(buf, send, recv, 4).start()
        gather_arrival(buf, send, recv, 1).wait_recv()
        gather_copy(buf, send, recv, 5).start()

    def gather_wait(buf, send, recv, k):
        for i in {1: (2,), 2: (3,), 3: (4, 5)}[k]:
            gather_arrival(buf, send, recv, i).wait_recv()

    def arrive(buf, send, recv, k):
        for i in range(1, 4):

            @pl.when(k == i)
            def _():
                gather_wait(buf, send, recv, i)

    def part_copy(phase, i):
        low, high = pl.ds(0, half), pl.ds(half, half)
        bank = phase % 2
        src, dst, to = (
            (sendb.at[2, low], relayed.at[bank, 0], 1),
            (sendb.at[2, high], relayed.at[bank, 1], 2),
            (sendb.at[0, low], recvb.at[bank, 0, low], 1),
            (sendb.at[1, high], recvb.at[bank, 1, high], 2),
            (sendb.at[1, low], recvb.at[bank, 1, low], 2),
            (sendb.at[0, high], recvb.at[bank, 0, high], 1),
        )[i]
        return remote(src, dst, rss.at[phase, i], rsr.at[phase, i], plane(to))

    def parts_start(phase, k):
        for i in {3: (0, 1), 1: (2,), 2: (3,)}[k]:
            part_copy(phase, i).start()

    def parts_pass(phase):
        for i in range(2):
            part_copy(phase, i).wait_recv()
            rows = slice(i * half, (i + 1) * half)
            mine = sendb[1 - i, rows, :].astype(F32)
            sendb[1 - i, rows, :] = (mine + relayed[phase % 2, i].astype(F32)).astype(BF)
            part_copy(phase, 4 + i).start()

    def parts_sent(phase):
        for i in range(6):
            part_copy(phase, i).wait_send()

    def parts_wait(phase):
        for i in range(2, 6):
            part_copy(phase, i).wait_recv()

    ag_i = (x.at[0], xs, xr)
    ag_x = (x.at[1], agx, agxr)
    ag_g = (gb.at[0], agg, aggr)

    @pl.when(s == 0)
    def _():
        w_send(1, up_in.at[0])

    lx.wait()
    gather_start(*ag_i)
    pack_share()

    @pl.when(s == 0)
    def _():
        w_send(0)
        w_send(2, down_in)

    pack_params()
    par_copy = remote(par.at[s], par.at[s], psem.at[0], psem.at[1], sib)
    par_copy.start()
    lu.wait()
    ld.wait()

    @pl.when(s == 0)
    def _():
        for p in (1, 0, 2):
            across(p, z).start()

    for i in range(length // BQ):
        cols = slice(i * BQ, (i + 1) * BQ)
        ids = jnp.where(s == 0, seg_in[0, :, cols], seg_in[1, :, cols]).astype(F32)
        segr[:, cols] = ids
        segc[cols, :] = jnp.broadcast_to(ids, (BQ, BQ)).T

    @pl.loop(0, nblk)
    def _(b):
        q0 = pl.multiple_of(b * BQ, BQ)
        k0 = pl.multiple_of(jnp.maximum(b * BQ - SEG_MOST, 0), BQ)
        seg_k = segc[pl.ds(k0, BK), :]
        seg_q = segr[:, pl.ds(q0, BQ)]
        kpos = lax.broadcasted_iota(jnp.int32, (BK, BQ), 0) + k0
        qpos = lax.broadcasted_iota(jnp.int32, (BK, BQ), 1) + q0
        allowed = (seg_k == seg_q) & (kpos <= qpos)
        bias[b] = jnp.where(allowed, 0.0, MASKED).astype(BF)

    par_wait = remote(par.at[1 - s], par.at[1 - s], psem.at[0], psem.at[1], sib)
    par_copy.wait_send()
    par_wait.wait_recv()

    @pl.loop(0, 2)
    def _(i):
        sm[i] = jnp.zeros((8, width), F32)

    def first_w_pass(p):
        @pl.when(s == 0)
        def _():
            w_arrive(p, range(2, n, 2), True, lambda p, origin: across(p, origin).start())

    def first_w(p):
        @pl.when(s == 0)
        def _():
            w_arrive(p, range(1, n, 2), False, lambda p, origin: across(p, origin).start())

        @pl.when(s == 1)
        def _():
            for origin in range(n):
                across(p, origin).wait_recv()

    def first_w_sent():
        @pl.when(s == 0)
        def _():
            for p in range(3):
                w_sent(p)
                for origin in range(n):
                    across(p, origin).wait_send()

    def second_w_send():
        @pl.when(s == 1)
        def _():
            w_send(1, up_in.at[0])
            w_send(0)
            w_send(2, down_in)

    def second_w_pass(p):
        @pl.when(s == 1)
        def _():
            w_arrive(p, range(2, n, 2), True, None)

    def second_w_give(p):
        @pl.when(s == 1)
        def _():
            w_arrive(p, range(1, n, 2), False, None)
            forward(p).start()

    def second_w(p):
        @pl.when(s == 0)
        def _():
            forward(p).wait_recv()

    def second_w_sent():
        @pl.when(s == 1)
        def _():
            for p in range(3):
                w_sent(p)
                forward(p).wait_send()

    def prow(layer, r, cols=None):
        if cols is None:
            return par[layer, r : r + 1, :]
        return par[layer, r : r + 1, cols]

    def rope_tables(b, sign):
        ca = taba[0, b]
        sa = taba[1, b]
        c0 = tabb[0]
        s0 = tabb[1]
        cos = ca * c0 - sa * s0
        sin = sa * c0 + ca * s0
        lane = lane_iota(BQ) & (HEAD_DIM - 1)
        return cos, jnp.where(lane < ROT // 2, -sign, sign) * sin

    def rope(u, b, sign):
        halves = []
        lane = lane_iota(BQ) & (HEAD_DIM - 1)
        for i in range(u.shape[0] // BQ):
            part = u[i * BQ : (i + 1) * BQ]
            cos, sin = rope_tables(b + i, sign)
            partner = jnp.where(
                lane < ROT // 2,
                pltpu.roll(part, HL - ROT // 2, 1),
                pltpu.roll(part, ROT // 2, 1),
            )
            halves.append(part * cos + partner * sin)
        return jnp.concatenate(halves, axis=0)

    def stack_heads(block):
        lane = lane_iota(BQ) >> 6
        return jnp.concatenate(
            [jnp.where(lane == h, block, jnp.zeros_like(block)) for h in range(heads)], axis=0
        )

    sub = 64

    def norm_chunk(layer, c):
        @pl.loop(0, chunk // sub)
        def _(i):
            rows = pl.ds(pl.multiple_of(c * chunk + i * sub, sub), sub)
            v = x[layer, rows, :].astype(F32)
            m = jnp.mean(v, axis=-1, keepdims=True)
            v = v - m
            r = lax.rsqrt(jnp.mean(v * v, axis=-1, keepdims=True) + EPS)
            mu[layer, rows, :] = m
            rstd[layer, rows, :] = r
            v = v * r
            an[rows, :] = (v * prow(layer, 0) + prow(layer, 2)).astype(BF)
            mn[rows, :] = (v * prow(layer, 1) + prow(layer, 3)).astype(BF)

    def renorm_all(layer):
        @pl.loop(0, length // sub)
        def _(i):
            rows = pl.ds(pl.multiple_of(i * sub, sub), sub)
            v = (x[layer, rows, :].astype(F32) - mu[layer, rows, :]) * rstd[layer, rows, :]
            an[rows, :] = (v * prow(layer, 0) + prow(layer, 2)).astype(BF)
            mn[rows, :] = (v * prow(layer, 1) + prow(layer, 3)).astype(BF)

    def project_in(layer, c):
        rows = pl.ds(pl.multiple_of(c * chunk, chunk), chunk)
        a = an[rows, :]
        b0 = c * (chunk // BQ)
        lane = lane_iota(chunk)
        u = mm(a, w[layer, 0, :, QO : QO + HL], NN) + prow(layer, 4, slice(0, HL))
        qb[layer, rows, :] = (rope(u, b0, 1.0) * 0.125).astype(BF)
        u = mm(a, w[layer, 0, :, KO - 64 : KO - 64 + HL], NN)
        kb[layer, rows, :] = rope(pltpu.roll(u, HL - 64, 1), b0, 1.0).astype(BF)
        u = mm(a, w[layer, 0, :, VO : VO + HL], NN) + prow(layer, 5, slice(0, HL))
        vb[layer, rows, :] = jnp.where(lane < heads * HEAD_DIM, u, 0.0).astype(BF)

    def attend(layer):
        @pl.loop(0, nblk)
        def _(b):
            q0 = pl.multiple_of(b * BQ, BQ)
            k0 = pl.multiple_of(jnp.maximum(b * BQ - SEG_MOST, 0), BQ)
            qm = stack_heads(qb[layer, pl.ds(q0, BQ), :])
            top = None
            for i in range(BK // BQ):
                keys = kb[layer, pl.ds(k0 + i * BQ, BQ), :]
                blk = bias[b, i * BQ : (i + 1) * BQ, :].astype(F32)
                sc = mm(keys, qm, NT) + jnp.concatenate([blk] * heads, axis=1)
                pscr[i * BQ : (i + 1) * BQ, :] = sc
                peak = jnp.max(sc, axis=0, keepdims=True)
                top = peak if top is None else jnp.maximum(top, peak)
            total = None
            for i in range(BK // BQ):
                e = jnp.exp(pscr[i * BQ : (i + 1) * BQ, :] - top)
                pscr[i * BQ : (i + 1) * BQ, :] = e
                part = jnp.sum(e, axis=0, keepdims=True)
                total = part if total is None else total + part
            lse[layer, b] = top + jnp.log(total)
            inv = 1.0 / total
            lane = lane_iota(BQ) >> 6
            ctx = jnp.zeros((BQ, HL), F32)
            vals = vb[layer, pl.ds(k0, BK), :]
            for h in range(heads):
                cols = slice(h * BQ, (h + 1) * BQ)
                ph = (pscr[:, cols] * inv[:, cols]).astype(BF)
                ctx = jnp.where(lane == h, mm(ph, vals, TN), ctx)
            cb[layer, pl.ds(q0, BQ), :] = pltpu.roll(ctx, HL - heads * HEAD_DIM, 1).astype(BF)

    def hidden(layer, c):
        rows = pl.ds(pl.multiple_of(c * chunk, chunk), chunk)
        a = mn[rows, :]
        for j in range(width // 256):
            cols = slice(j * 256, (j + 1) * 256)
            u = mm(a, w[layer, 1, :, cols], NN) + prow(layer, 6, cols)
            phi = 0.5 * (1.0 + lax.erf(u * ROOT_HALF))
            hid[layer, rows, cols] = (u * phi).astype(BF)
            slope[layer, rows, cols] = (phi + u * INV_ROOT_TAU * jnp.exp(-0.5 * u * u)).astype(BF)

    def project_out(layer):
        phase = layer
        if layer == 1:
            parts_sent(0)
        for k in (3, 1, 2, 0):
            rows = pl.ds(pl.multiple_of((t ^ k) * chunk, chunk), chunk)
            c = cb[layer, rows, :]
            h = hid[layer, rows, :]
            for j in range(width // 256):
                cols = slice(j * 256, (j + 1) * 256)
                y = mm(c, w[layer, 0, cols, 512:768], NT) + mm(h, w[layer, 2, cols, :], NT)
                if k:
                    sendb[k - 1, :, cols] = y.astype(BF)
                else:
                    ownp[phase % 2, :, cols] = y
            if k:
                parts_start(phase, k)

    def place(layer, stage, out, idx):
        @pl.when(s == layer)
        def _():
            pltpu.make_async_copy(stage, out.at[s], osend.at[idx]).start()

        @pl.when(s != layer)
        def _():
            remote(stage, out.at[s], osend.at[idx], orecv.at[idx // 2], sib).start()

    def placed(layer, stage, out, idx):
        @pl.when(s == layer)
        def _():
            pltpu.make_async_copy(stage, out.at[s], osend.at[idx]).wait()

        @pl.when(s != layer)
        def _():
            remote(stage, out.at[s], osend.at[idx], orecv.at[idx // 2], sib).wait_send()

    def finish_y(layer):
        phase = layer
        parts_wait(phase)
        if layer == 1:
            placed(0, yst, out_y, 0)

        @pl.loop(0, chunk // sub)
        def _(i):
            r = pl.ds(pl.multiple_of(i * sub, sub), sub)
            rows = pl.ds(pl.multiple_of(t * chunk + i * sub, sub), sub)
            y = x[layer, rows, :].astype(F32) + ownp[phase % 2, r, :] + prow(layer, 7)
            for k in range(2):
                y = y + recvb[phase % 2, k, r, :].astype(F32)
            yst[r, :] = y
            if layer == 0:
                x[1, rows, :] = y.astype(BF)

        if layer == 0:
            gather_start(*ag_x)
        place(layer, yst, out_y, layer)

    def reduce_start(layer, p, buf):
        @pl.when(s != layer)
        def _():
            remote(buf.at[p], gsr.at[p], ghs.at[p], ghr.at[p], sib).start()

    def z_item(p, e, sign, buf):
        dest = lax.rem(z + sign * e + n, n)
        way = 0 if sign > 0 else 1
        if e <= 2:
            slot = 2 * way + e - 1
            dst, recv, far = zrecv.at[p, slot], zr.at[p, slot], e
        else:
            place_no = e - 3 if sign > 0 else n - z + e - 4
            dst, recv, far = zacc.at[p, place_no], za.at[way, p, e - 3], 1
        return remote(
            buf.at[p, w_rows(dest)],
            dst,
            zs.at[way, p, e - 1],
            recv,
            (s, lax.rem(z + sign * far + n, n), t),
        )

    def first_of(sign):
        return (z == 0) if sign > 0 else (z == n - 1)

    def z_send(p, buf):
        for e in range(n - 1, 0, -1):
            for sign in (1, -1):
                go = inside(sign * e)
                if e > 1:
                    go = go & first_of(sign)

                @pl.when(go)
                def _():
                    z_item(p, e, sign, buf).start()

    def z_pass(layer, p, buf):
        @pl.when(s == layer)
        def _():
            for e in range(n - 2, 1, -1):
                for sign in (1, -1):

                    @pl.when(inside(sign * e) & inside(-sign))
                    def _():
                        way = 0 if sign > 0 else 1
                        place_no = e - 2 if sign > 0 else n - z + e - 4
                        got = zacc.at[p, place_no]
                        remote(got, got, zs.at[way, p, e - 1], za.at[way, p, e - 2], sib).wait_recv()
                        base = lax.rem(z + sign * e + n, n) * rows_z

                        @pl.loop(0, rows_z // step)
                        def _(i):
                            r = pl.ds(pl.multiple_of(i * step, 16), step)
                            q = pl.ds(pl.multiple_of(base + i * step, 16), step)
                            more = zacc[p, place_no, r, :].astype(F32)
                            buf[p, q, :] = (buf[p, q, :].astype(F32) + more).astype(BF)

                        z_item(p, e, sign, buf).start()

    def z_end(p, buf):
        for slot in range(4):
            sign = 1 if slot < 2 else -1
            e = slot % 2 + 1

            @pl.when(inside(-sign * e))
            def _():
                got = zrecv.at[p, slot]
                remote(got, got, zs.at[0, p, 0], zr.at[p, slot], sib).wait_recv()

                @pl.loop(0, rows_z // step)
                def _(i):
                    r = pl.ds(pl.multiple_of(i * step, 16), step)
                    wacc[p, r, :] = wacc[p, r, :] + zrecv[p, slot, r, :].astype(F32)

    def z_sent(p, buf):
        for e in range(1, n):
            for sign in (1, -1):

                @pl.when(inside(sign * e))
                def _():
                    z_item(p, e, sign, buf).wait_send()

    step = 48

    def reduce_cores(layer, p, buf):
        @pl.when(s == layer)
        def _():
            remote(buf.at[p], gsr.at[p], ghs.at[p], ghr.at[p], sib).wait_recv()

            @pl.loop(0, rows_z // step)
            def _(i):
                r = pl.ds(pl.multiple_of(i * step, 16), step)
                q = pl.ds(pl.multiple_of(z * rows_z + i * step, 16), step)
                wacc[p, r, :] = buf[p, q, :].astype(F32) + gsr[p, q, :].astype(F32)

            for j in range(1, n):
                base = other_z(j) * rows_z

                @pl.loop(0, rows_z // step)
                def _(i):
                    q = pl.ds(pl.multiple_of(base + i * step, 16), step)
                    buf[p, q, :] = (buf[p, q, :].astype(F32) + gsr[p, q, :].astype(F32)).astype(BF)

            z_send(p, buf)

        @pl.when(s != layer)
        def _():
            remote(buf.at[p], gsr.at[p], ghs.at[p], ghr.at[p], sib).wait_send()

    def grad_part(layer, p, buf):
        for j in range(width // 256):
            cols = slice(j * 256, (j + 1) * 256)
            if p == 2:
                buf[p, cols, :] = mm(gb[layer, :, cols], hid[layer], TN).astype(BF)
            elif p == 1:
                buf[p, cols, :] = mm(mn[:, cols], du[...], TN).astype(BF)
            else:
                buf[p, cols, 0:512] = mm(an[:, cols], dqkv[:, 0:512], TN).astype(BF)
                buf[p, cols, 512:768] = (
                    mm(an[:, cols], dqkv[:, 512:768], TN) + mm(gb[layer, :, cols], cb[layer], TN)
                ).astype(BF)
        reduce_start(layer, p, buf)

    def hidden_back(layer, c):
        rows = pl.ds(pl.multiple_of(c * chunk, chunk), chunk)
        g = gb[layer, rows, :]
        for j in range(width // 256):
            cols = slice(j * 256, (j + 1) * 256)
            d = mm(g, w[layer, 2, :, cols], NN) * slope[layer, rows, cols].astype(F32)
            sm[layer, 6:7, cols] = sm[layer, 6:7, cols] + jnp.sum(d, axis=0, keepdims=True)
            du[rows, cols] = d.astype(BF)
        d = pltpu.roll(mm(g, w[layer, 0, :, 512:768], NN), HL - 64, 1)
        lane = lane_iota(chunk)
        dc[rows, :] = jnp.where(lane < heads * HEAD_DIM, d, 0.0).astype(BF)

    def zero_sums():
        @pl.loop(0, length // sub)
        def _(i):
            rows = pl.ds(pl.multiple_of(i * sub, sub), sub)
            dk[rows, :] = jnp.zeros((sub, HL), F32)
            dv[rows, :] = jnp.zeros((sub, HL), F32)

    def attend_back(layer, first, last):
        @pl.loop(first, last)
        def _(b):
            q0 = pl.multiple_of(b * BQ, BQ)
            k0 = pl.multiple_of(jnp.maximum(b * BQ - SEG_MOST, 0), BQ)
            qm = stack_heads(qb[layer, pl.ds(q0, BQ), :])
            dm = stack_heads(dc[pl.ds(q0, BQ), :])
            ls = lse[layer, b]
            total = None
            for i in range(BK // BQ):
                krows = pl.ds(k0 + i * BQ, BQ)
                irows = slice(i * BQ, (i + 1) * BQ)
                blk = bias[b, irows, :].astype(F32)
                sc = mm(kb[layer, krows, :], qm, NT) + jnp.concatenate([blk] * heads, axis=1)
                pr = jnp.exp(sc - ls)
                dp = mm(vb[layer, krows, :], dm, NT)
                dv[krows, :] = dv[krows, :] + mm(pr.astype(BF), dm, NN)
                pscr[irows, :] = pr
                dpscr[irows, :] = dp
                part = jnp.sum(pr * dp, axis=0, keepdims=True)
                total = part if total is None else total + part
            lane = lane_iota(BQ) >> 6
            acc = [jnp.zeros((BQ, HL), F32) for _ in range(heads)]
            for i in range(BK // BQ):
                krows = pl.ds(k0 + i * BQ, BQ)
                irows = slice(i * BQ, (i + 1) * BQ)
                ds = (pscr[irows, :] * (dpscr[irows, :] - total)).astype(BF)
                dk[krows, :] = dk[krows, :] + mm(ds, qm, NN)
                keys = kb[layer, krows, :]
                for h in range(heads):
                    acc[h] = acc[h] + mm(ds[:, h * BQ : (h + 1) * BQ], keys, TN)
            out = jnp.zeros((BQ, HL), F32)
            for h in range(heads):
                out = jnp.where(lane == h, acc[h], out)
            dq[pl.ds(q0, BQ), :] = out

    def pack_qkv(layer):
        @pl.loop(0, 4)
        def _(c):
            rows = pl.ds(pl.multiple_of(c * chunk, chunk), chunk)
            b0 = c * (chunk // BQ)
            lane = lane_iota(chunk)
            gq = rope(dq[rows, :], b0, -1.0) * 0.125
            gk = rope(dk[rows, :], b0, -1.0)
            gv = dv[rows, :]
            sm[layer, 4:5, 0:HL] = sm[layer, 4:5, 0:HL] + jnp.sum(gq, axis=0, keepdims=True)
            sm[layer, 5:6, 0:HL] = sm[layer, 5:6, 0:HL] + jnp.sum(gv, axis=0, keepdims=True)
            rk = pltpu.roll(gk, 192, 1)
            rv = pltpu.roll(gv, 128, 1)
            dqkv[rows, 0:256] = jnp.where(lane < 192, gq, rk).astype(BF)
            dqkv[rows, 256:512] = jnp.where(lane < 128, rk, rv).astype(BF)
            dqkv[rows, 512:768] = jnp.where(lane < 64, rv, 0.0).astype(BF)

    def project_back(layer):
        phase = 3 - layer
        parts_sent(1 if layer == 1 else 2)
        for k in (3, 1, 2, 0):
            rows = pl.ds(pl.multiple_of((t ^ k) * chunk, chunk), chunk)
            da_in = dqkv[rows, :]
            du_in = du[rows, :]
            m = mu[layer, rows, :]
            r = rstd[layer, rows, :]
            for j in range(width // 256):
                cols = slice(j * 256, (j + 1) * 256)
                da = mm(da_in, w[layer, 0, cols, :], NT)
                dm = mm(du_in, w[layer, 1, cols, :], NT)
                unit = (x[layer, rows, cols].astype(F32) - m) * r
                sums = [da * unit, dm * unit, da, dm]
                for i in range(4):
                    sm[layer, i : i + 1, cols] = sm[layer, i : i + 1, cols] + jnp.sum(
                        sums[i], axis=0, keepdims=True
                    )
                e = da * prow(layer, 0, cols) + dm * prow(layer, 1, cols)
                if k:
                    sendb[k - 1, :, cols] = e.astype(BF)
                else:
                    ownp[phase % 2, :, cols] = e
            if k:
                parts_start(phase, k)

    def finish_e(layer):
        phase = 3 - layer
        parts_wait(phase)
        stage = gst.at[1 - layer]
        given = cotv if layer == 1 else gst.at[0]

        @pl.loop(0, chunk // sub)
        def _(i):
            r = pl.ds(pl.multiple_of(i * sub, sub), sub)
            rows = pl.ds(pl.multiple_of(t * chunk + i * sub, sub), sub)
            e = ownp[phase % 2, r, :]
            for k in range(2):
                e = e + recvb[phase % 2, k, r, :].astype(F32)
            rs = rstd[layer, rows, :]
            unit = (x[layer, rows, :].astype(F32) - mu[layer, rows, :]) * rs
            g = given[r, :]
            sm[layer, 7:8, :] = sm[layer, 7:8, :] + jnp.sum(g, axis=0, keepdims=True)
            d = rs * (
                e
                - jnp.mean(e, axis=-1, keepdims=True)
                - unit * jnp.mean(e * unit, axis=-1, keepdims=True)
            )
            g = g + d
            stage[r, :] = g
            if layer == 1:
                gb[0, rows, :] = g.astype(BF)

        if layer == 1:
            gather_start(*ag_g)
        place(layer, stage, out_g, 2 + layer)

    norm_chunk(0, t)
    gather_pass(*ag_i)
    lc.wait()
    gb[1, own, :] = cotv[...].astype(BF)
    for k in range(1, 4):
        g_copy(k).start()
    first_w_pass(1)

    @pl.loop(1, 4)
    def _(k):
        arrive(*ag_i, k)
        norm_chunk(0, t ^ k)

    first_w(1)

    @pl.loop(0, 4)
    def _(c):
        hidden(0, c)

    first_w_pass(0)
    first_w(0)

    @pl.loop(0, 4)
    def _(c):
        project_in(0, c)

    attend(0)
    first_w_pass(2)
    first_w(2)
    second_w_send()
    project_out(0)
    parts_pass(0)
    second_w_pass(1)
    finish_y(0)

    @pl.loop(0, 4)
    def _(k):
        arrive(*ag_x, k)
        norm_chunk(1, t ^ k)

        @pl.when(k == 0)
        def _():
            second_w_give(1)
            gather_pass(*ag_x)
            second_w_pass(0)
            second_w(1)

        hidden(1, t ^ k)

    second_w_give(0)
    second_w_pass(2)
    second_w(0)

    @pl.loop(0, 4)
    def _(c):
        project_in(1, c)

    attend(1)
    second_w_give(2)
    second_w(2)
    project_out(1)

    for k in range(1, 4):
        g_arrival(k).wait_recv()
    zero_sums()

    @pl.loop(0, 4)
    def _(c):
        hidden_back(1, c)

    grad_part(1, 2, gw)
    parts_pass(1)
    grad_part(1, 1, gw)
    attend_back(1, 0, nblk)
    reduce_cores(1, 2, gw)
    reduce_cores(1, 1, gw)
    pack_qkv(1)
    project_back(1)
    z_pass(1, 2, gw)
    grad_part(1, 0, gw)
    parts_pass(2)
    z_pass(1, 1, gw)
    finish_y(1)
    reduce_cores(1, 0, gw)
    finish_e(1)

    late = w.at[1]
    per = chunk // BQ
    first_w_sent()
    second_w_sent()
    zero_sums()

    @pl.loop(0, 8)
    def _(step_no):
        k = jnp.where(step_no < 2, 0, jnp.where(step_no < 5, step_no - 1, step_no - 4))

        @pl.when((step_no == 0) | ((step_no >= 2) & (step_no < 5)))
        def _():
            arrive(*ag_g, k)
            hidden_back(0, t ^ k)

        @pl.when(step_no == 5)
        def _():
            grad_part(0, 2, late)
            grad_part(0, 1, late)

        @pl.when(step_no == 6)
        def _():
            reduce_cores(0, 2, late)

        @pl.when(step_no == 7)
        def _():
            reduce_cores(0, 1, late)

        @pl.when((step_no == 1) | (step_no >= 5))
        def _():
            attend_back(0, (t ^ k) * per, ((t ^ k) + 1) * per)

        @pl.when(step_no == 1)
        def _():
            gather_pass(*ag_g)
            z_pass(1, 0, gw)
            renorm_all(0)

    z_pass(0, 2, late)
    pack_qkv(0)
    project_back(0)
    z_pass(0, 1, late)
    grad_part(0, 0, late)
    parts_pass(3)
    reduce_cores(0, 0, late)
    finish_e(0)

    to_sib = remote(sm.at[1 - s], smr, sms.at[0], smrs.at[0], sib)
    to_sib.start()
    to_sib.wait()
    smt[...] = sm[s] + smr[...]
    for j in range(1, n):
        remote(
            smt, smz.at[j - 1], sms.at[j], smrs.at[j], (s, other_z(j), t)
        ).start()
    for j in range(1, n):
        remote(smt, smz.at[j - 1], sms.at[j], smrs.at[j], (s, other_z(j), t)).wait()
    total = smt[...]
    for j in range(1, n):
        total = total + smz[j - 1]
    tall[t] = total

    def small_copy(k):
        return remote(tall.at[t], tall.at[t], sms.at[n + k - 1], smrs.at[n + k - 1], plane(k))

    for k in range(1, 4):
        small_copy(k).start()

    z_pass(0, 0, late)
    for p in (2, 1, 0):
        z_end(p, late)
        pltpu.make_async_copy(wacc.at[p], out_w.at[p], lsem.at[p]).start()
    for k in range(1, 4):
        small_copy(k).wait_send()
        remote(
            tall.at[t ^ k], tall.at[t ^ k], sms.at[n + k - 1], smrs.at[n + k - 1], plane(k)
        ).wait_recv()
    out_s[...] = tall[...]

    for p in range(3):
        pltpu.make_async_copy(wacc.at[p], out_w.at[p], lsem.at[p]).wait()
        z_sent(p, late)

    for k in range(1, 4):
        g_copy(k).wait_send()
    for i in range(6):
        gather_copy(*ag_i, i).wait_send()
        gather_copy(*ag_x, i).wait_send()
        gather_copy(*ag_g, i).wait_send()
    parts_sent(3)
    placed(1, yst, out_y, 1)
    placed(1, gst.at[0], out_g, 3)
    placed(0, gst.at[1], out_g, 2)
    remote(yst, out_y.at[1 - s], osend.at[0], orecv.at[0], sib).wait_recv()
    remote(gst.at[0], out_g.at[1 - s], osend.at[0], orecv.at[1], sib).wait_recv()


def write_outputs(
    head_cols, y, g, wg, small, y_out, g_out, up, down, qkv, out, gain, shift, qv, upb, resid, sem
):
    pairs = ((y, y_out), (g, g_out), (wg.at[1], up), (wg.at[2], down))
    copies = [pltpu.make_async_copy(src, dst, sem.at[i]) for i, (src, dst) in enumerate(pairs)]
    for copy in copies:
        copy.start()
    first = wg[0]
    width = first.shape[1]
    for i in range(3):
        turned = pltpu.roll(first, width - i * head_cols, 1) if i else first
        qkv[i] = turned[:, :head_cols]
    last = pltpu.roll(first, width - 3 * head_cols, 1)[:, :256]
    out[...] = last.T[:head_cols, :]
    total = small[0] + small[1] + small[2] + small[3]
    gain[...] = total[0:2]
    shift[...] = total[2:4]
    resid[...] = total[7:8]
    spread = small[0]
    upb[:, 0:width] = small[0, 6:7, :]
    for i in range(1, 4):
        spread = spread + pltpu.roll(small[i], i * head_cols, 1)
        upb[:, i * width : (i + 1) * width] = small[i, 6:7, :]
    qv[...] = spread[4:6]
    for copy in copies:
        copy.wait()


def rotary_rows(length, heads):
    rate = np.zeros((HL,), np.float64)
    for h in range(heads):
        for j in range(ROT // 2):
            value = math.exp(j * (-2.0 * math.log(10000.0) / ROT))
            rate[h * HEAD_DIM + j] = value
            rate[h * HEAD_DIM + j + ROT // 2] = value
    live = (np.arange(HL) < heads * HEAD_DIM).astype(np.float64)
    starts = np.arange(length // BQ)[:, None] * BQ * rate[None]
    offsets = np.arange(BQ)[:, None] * rate[None]
    first = np.stack([np.cos(starts), np.sin(starts)])[:, :, None].astype(np.float32)
    second = np.stack([np.cos(offsets) * live, np.sin(offsets) * live]).astype(np.float32)
    return first, second


def body(
    n,
    inputs,
    segment_ids,
    cotangent,
    qkv_weight,
    out_weight,
    up_weight,
    down_weight,
    norm_gain,
    norm_bias,
    qv_bias,
    up_bias,
    resid_bias,
):
    micro, _, chunk, width = inputs.shape
    length = segment_ids.shape[2]
    head_cols = qkv_weight.shape[3]
    rows_z = qkv_weight.shape[2]
    ff_local = up_weight.shape[2]
    heads = head_cols // HEAD_DIM
    assert micro == 2 and length == 4 * chunk and ff_local == width
    assert head_cols == 192 and width == 768

    first, second = rotary_rows(length, heads)

    vm = pl.BlockSpec(memory_space=pltpu.VMEM)
    anywhere = pl.BlockSpec(memory_space=pl.ANY)
    blk = heads * BQ
    nblk = length // BQ
    dma = pltpu.SemaphoreType.DMA

    def vmem(*shape, dtype=BF):
        return pltpu.VMEM(shape, dtype)

    scratch = dict(
        w=vmem(2, 3, width, width),
        x=vmem(2, length, width),
        an=vmem(length, width),
        mn=vmem(length, width),
        mu=vmem(2, length, 1, dtype=F32),
        rstd=vmem(2, length, 1, dtype=F32),
        qb=vmem(2, length, HL),
        kb=vmem(2, length, HL),
        vb=vmem(2, length, HL),
        cb=vmem(2, length, HL),
        lse=vmem(2, nblk, 1, blk, dtype=F32),
        slope=vmem(2, length, width),
        hid=vmem(2, length, width),
        gb=vmem(2, length, width),
        du=vmem(length, width),
        dqkv=vmem(length, width),
        dc=vmem(length, HL),
        dq=vmem(length, HL, dtype=F32),
        dk=vmem(length, HL, dtype=F32),
        dv=vmem(length, HL, dtype=F32),
        bias=vmem(nblk, BK, BQ),
        pscr=vmem(BK, blk, dtype=F32),
        dpscr=vmem(BK, blk, dtype=F32),
        sendb=vmem(3, chunk, width),
        recvb=vmem(2, 2, chunk, width),
        relayed=vmem(2, 2, chunk // 2, width),
        ownp=vmem(2, chunk, width, dtype=F32),
        gw=vmem(3, width, width),
        gsr=vmem(3, width, width),
        zrecv=vmem(3, 4, rows_z, width),
        zacc=vmem(3, max(n - 3, 1), rows_z, width),
        wacc=vmem(3, rows_z, width, dtype=F32),
        cotv=vmem(chunk, width, dtype=F32),
        yst=vmem(chunk, width, dtype=F32),
        gst=vmem(2, chunk, width, dtype=F32),
        segc=vmem(length, BQ, dtype=F32),
        segr=vmem(1, length, dtype=F32),
        par=vmem(2, 8, width, dtype=F32),
        sm=vmem(2, 8, width, dtype=F32),
        smr=vmem(8, width, dtype=F32),
        smt=vmem(8, width, dtype=F32),
        smz=vmem(n - 1, 8, width, dtype=F32),
        tall=vmem(4, 8, width, dtype=F32),
        lsem=dma((8,)),
        psem=dma((2,)),
        xs=dma((6,)),
        xr=dma((6,)),
        agx=dma((6,)),
        agxr=dma((6,)),
        agg=dma((6,)),
        aggr=dma((6,)),
        gs=dma((3,)),
        gr=dma((3,)),
        ws=dma((4, 3, n)),
        wr=dma((3, n)),
        fs=dma((3, n)),
        fr=dma((3, n)),
        rss=dma((4, 6)),
        rsr=dma((4, 6)),
        osend=dma((4,)),
        orecv=dma((2,)),
        ghs=dma((3,)),
        ghr=dma((3,)),
        zs=dma((2, 3, n)),
        zr=dma((3, 4)),
        za=dma((2, 3, n)),
        sms=dma((n + 3,)),
        smrs=dma((n + 3,)),
    )
    out_y, out_g, out_w, out_s = pl.pallas_call(
        functools.partial(kernel, n, heads),
        out_shape=(
            jax.ShapeDtypeStruct((2, chunk, width), F32),
            jax.ShapeDtypeStruct((2, chunk, width), F32),
            jax.ShapeDtypeStruct((3, rows_z, width), F32),
            jax.ShapeDtypeStruct((4, 8, width), F32),
        ),
        in_specs=[anywhere, anywhere, vm, vm, vm, anywhere, anywhere] + [vm] * 7,
        out_specs=(anywhere, anywhere, anywhere, vm),
        scratch_shapes=list(scratch.values()),
        compiler_params=pltpu.CompilerParams(
            collective_id=0, has_side_effects=True, vmem_limit_bytes=67043328
        ),
        name="two_layers",
    )(
        inputs.reshape(micro, chunk, width),
        cotangent.reshape(micro, chunk, width),
        segment_ids,
        qkv_weight,
        out_weight,
        up_weight,
        down_weight[0].T,
        norm_gain,
        norm_bias,
        qv_bias,
        up_bias,
        resid_bias,
        jnp.asarray(first),
        jnp.asarray(second),
    )
    shapes = (
        (2, chunk, width),
        (2, chunk, width),
        (rows_z, width),
        (rows_z, width),
        (3, rows_z, head_cols),
        (head_cols, rows_z),
        (2, width),
        (2, width),
        (2, width),
        (1, 4 * width),
        (1, width),
    )
    y, g, up_g, down_g, qkv_g, out_gr, gain_g, shift_g, qv_g, upb_g, resid_g = pl.pallas_call(
        functools.partial(write_outputs, head_cols),
        out_shape=tuple(jax.ShapeDtypeStruct(shape, F32) for shape in shapes),
        in_specs=[vm] * 4,
        out_specs=(anywhere,) * 4 + (vm,) * 7,
        scratch_shapes=[dma((4,))],
        name="outputs",
    )(out_y, out_g, out_w, out_s)
    return (
        y.reshape(1, micro, 1, chunk, width),
        g.reshape(1, micro, 1, chunk, width),
        qkv_g[None],
        out_gr[None],
        up_g[None],
        down_g.T[None],
        gain_g[None],
        shift_g[None],
        qv_g[None],
        upb_g,
        resid_g,
    )


def solution(mesh):
    return jax.shard_map(
        functools.partial(body, mesh.shape["dp"]),
        mesh=mesh,
        in_specs=(
            P(None, "dp", "tensor", None),
            P(None, "dp", None),
            P(None, "dp", "tensor", None),
            P("section", None, "dp", "tensor"),
            P("section", "tensor", "dp"),
            P("section", "dp", "tensor"),
            P("section", "tensor", "dp"),
            P("section", None, None),
            P("section", None, None),
            P("section", None, None),
            P("section", None),
            P("section", None),
        ),
        out_specs=(
            P("section", None, "dp", "tensor", None),
            P("section", None, "dp", "tensor", None),
            P("section", None, "dp", "tensor"),
            P("section", "tensor", "dp"),
            P("section", "dp", "tensor"),
            P("section", "tensor", "dp"),
            P("section", None, None),
            P("section", None, None),
            P("section", None, None),
            P("section", None),
            P("section", None),
        ),
        check_vma=False,
    )
```

```python
import functools
import math

import jax
import jax.numpy as jnp
import numpy as np
from jax import lax
from jax.experimental import pallas as pl
from jax.experimental.pallas import tpu as pltpu
from jax.sharding import PartitionSpec as P

HEAD_DIM = 64
ROT = 16
SEG_MOST = 384
EPS = 1e-05
MASKED = -1e30
ROOT_HALF = 0.7071067811865476
INV_ROOT_TAU = 0.3989422804014327

BF = jnp.bfloat16
F32 = jnp.float32
MESH = pl.DeviceIdType.MESH

NN = (((1,), (0,)), ((), ()))
NT = (((1,), (1,)), ((), ()))
TN = (((0,), (0,)), ((), ()))

BQ = 128
BK = BQ + SEG_MOST
HL = 256
QO, KO, VO, OO = 0, 192, 384, 576


def mm(a, b, dims):
    return lax.dot_general(a, b, dims, preferred_element_type=F32)


def lane_iota(rows, cols=HL):
    return lax.broadcasted_iota(jnp.int32, (rows, cols), 1)


def remote(src, dst, send, recv, dev):
    return pltpu.make_async_remote_copy(
        src_ref=src, dst_ref=dst, send_sem=send, recv_sem=recv, device_id=dev, device_id_type=MESH
    )


def kernel(
    n,
    heads,
    x_in,
    cot_in,
    seg_in,
    qkv_in,
    wo_in,
    up_in,
    down_in,
    gain_in,
    shift_in,
    qv_in,
    upb_in,
    resid_in,
    taba,
    tabb,
    out_y,
    out_g,
    out_w,
    out_s,
    w,
    x,
    an,
    mn,
    mu,
    rstd,
    qb,
    kb,
    vb,
    kt,
    vt,
    cb,
    lse,
    slope,
    hid,
    gb,
    du,
    dqkv,
    dc,
    dq,
    dk,
    dv,
    bias,
    pscr,
    dpscr,
    dscr,
    sendb,
    recvb,
    relayed,
    ownp,
    gw,
    gsr,
    zrecv,
    zacc,
    wacc,
    yst,
    gst,
    segr,
    par,
    sm,
    smr,
    smt,
    smz,
    tall,
    lsem,
    psem,
    xs,
    xr,
    agx,
    agxr,
    agg,
    aggr,
    gs,
    gr,
    ws,
    wr,
    fs,
    fr,
    rss,
    rsr,
    osend,
    orecv,
    ghs,
    ghr,
    zs,
    zr,
    za,
    sms,
    smrs,
):
    s = lax.axis_index("section")
    z = lax.axis_index("dp")
    t = lax.axis_index("tensor")
    sib = (1 - s, z, t)
    width = x.shape[2]
    length = x.shape[1]
    chunk = length // 4
    rows_z = up_in.shape[1]
    half = chunk // 2
    nblk = length // BQ
    own = pl.ds(t * chunk, chunk)
    zrows = pl.ds(z * rows_z, rows_z)

    def plane(k):
        return (s, z, t ^ k)

    def other_z(j):
        return lax.rem(z + j, n)

    lx = pltpu.make_async_copy(x_in.at[s], x.at[0, own], lsem.at[0])
    lc = pltpu.make_async_copy(cot_in.at[s], gst.at[0], lsem.at[1])
    lu = pltpu.make_async_copy(up_in.at[0], w.at[s, 1, zrows], lsem.at[3])
    ld = pltpu.make_async_copy(down_in, w.at[s, 2, zrows], lsem.at[4])
    lx.start()
    lu.start()
    ld.start()
    lc.start()

    barrier = pltpu.get_barrier_semaphore()
    pl.semaphore_signal(barrier, inc=1, device_id=sib, device_id_type=MESH)
    for k in range(1, 4):
        pl.semaphore_signal(barrier, inc=1, device_id=plane(k), device_id_type=MESH)
    for j in range(1, n):
        pl.semaphore_signal(barrier, inc=1, device_id=(s, other_z(j), t), device_id_type=MESH)
    pl.semaphore_wait(barrier, 4 + n - 1)

    head_cols = heads * HEAD_DIM

    def picks(first):
        rows = lax.broadcasted_iota(jnp.int32, (head_cols, width), 0)
        cols = lax.broadcasted_iota(jnp.int32, (head_cols, width), 1)
        return (rows + first == cols).astype(F32).astype(BF)

    def pack_share():
        packed = mm(qkv_in[0, 0], picks(QO), NN) + mm(qkv_in[0, 1], picks(KO), NN)
        packed = packed + mm(qkv_in[0, 2], picks(VO), NN) + mm(wo_in[0], picks(OO), TN)
        w[s, 0, zrows, :] = packed.astype(BF)

    def pack_params():
        par[s, 0:2, :] = gain_in[0]
        par[s, 2:4, :] = shift_in[0]
        par[s, 4:6, :] = qv_in[0]
        par[s, 6:7, :] = upb_in[0:1, pl.ds(pl.multiple_of(t * width, 128), width)]
        par[s, 7:8, :] = resid_in[...]
        rows8 = par[s]
        turned = rows8
        for i in range(1, 4):
            turned = jnp.where(t == i, pltpu.roll(rows8, width - i * head_cols, 1), turned)
        row = lax.broadcasted_iota(jnp.int32, (8, width), 0)
        par[s] = jnp.where((row == 4) | (row == 5), turned, rows8)

    def w_rows(origin):
        return pl.ds(origin * rows_z, rows_z)

    def w_step(p, origin, far, src=None):
        rows = w_rows(origin)
        i = {1: 0, 2: 1, -1: 2, -2: 3}[far]
        return remote(
            w.at[s, p, rows] if src is None else src,
            w.at[s, p, rows],
            ws.at[i, p, origin],
            wr.at[p, origin],
            (s, lax.rem(z + far + n, n), t),
        )

    def inside(far):
        return (z + far < n) if far > 0 else (z + far >= 0)

    def w_send(p, src=None):
        for far in (1, -1, 2, -2):

            @pl.when(inside(far))
            def _():
                w_step(p, z, far, src).start()

    def w_arrive(p, distances, passed, then):
        for e in distances:
            for sign in (1, -1):

                @pl.when(inside(-sign * e))
                def _():
                    origin = lax.rem(z - sign * e + n, n)
                    w_step(p, origin, sign).wait_recv()
                    if passed:
                        for far in (sign, 2 * sign):

                            @pl.when(inside(far))
                            def _():
                                w_step(p, origin, far).start()

                    if then is not None:
                        then(p, origin)

    def w_sent(p):
        for far in (1, -1, 2, -2):

            @pl.when(inside(far))
            def _():
                w_step(p, z, far).wait_send()

            sign = 1 if far > 0 else -1
            for e in range(2, n, 2):

                @pl.when(inside(-sign * e) & inside(far))
                def _():
                    w_step(p, lax.rem(z - sign * e + n, n), far).wait_send()

    def across(p, origin):
        rows = w_rows(origin)
        return remote(w.at[0, p, rows], w.at[0, p, rows], fs.at[p, origin], fr.at[p, origin], sib)

    def forward(p):
        return remote(w.at[1, p], w.at[1, p], fs.at[p, 0], fr.at[p, 0], sib)

    def g_copy(k):
        return remote(gb.at[1, own], gb.at[1, own], gs.at[k - 1], gr.at[k - 1], plane(k))

    def g_arrival(k):
        rows = pl.ds((t ^ k) * chunk, chunk)
        return remote(gb.at[1, rows], gb.at[1, rows], gs.at[k - 1], gr.at[k - 1], plane(k))

    hops = ((0, 0, 1), (0, 1, 2), (0, 1, 1), (0, 0, 2), (1, 0, 2), (2, 1, 1))

    def gather_copy(buf, send, recv, i):
        k, h, to = hops[i]
        rows = pl.ds((t ^ k) * chunk + h * half, half)
        return remote(buf.at[rows], buf.at[rows], send.at[i], recv.at[i], plane(to))

    def gather_arrival(buf, send, recv, i):
        k, h, to = hops[i]
        rows = pl.ds((t ^ k ^ to) * chunk + h * half, half)
        return remote(buf.at[rows], buf.at[rows], send.at[i], recv.at[i], plane(to))

    def gather_start(buf, send, recv):
        for i in range(4):
            gather_copy(buf, send, recv, i).start()

    def gather_pass(buf, send, recv):
        gather_arrival(buf, send, recv, 0).wait_recv()
        gather_copy(buf, send, recv, 4).start()
        gather_arrival(buf, send, recv, 1).wait_recv()
        gather_copy(buf, send, recv, 5).start()

    def gather_wait(buf, send, recv, k):
        for i in {1: (2,), 2: (3,), 3: (4, 5)}[k]:
            gather_arrival(buf, send, recv, i).wait_recv()

    def arrive(buf, send, recv, k):
        for i in range(1, 4):

            @pl.when(k == i)
            def _():
                gather_wait(buf, send, recv, i)

    def part_copy(phase, i):
        low, high = pl.ds(0, half), pl.ds(half, half)
        bank = phase % 2
        src, dst, to = (
            (sendb.at[2, low], relayed.at[bank, 0], 1),
            (sendb.at[2, high], relayed.at[bank, 1], 2),
            (sendb.at[0, low], recvb.at[bank, 0, low], 1),
            (sendb.at[1, high], recvb.at[bank, 1, high], 2),
            (sendb.at[1, low], recvb.at[bank, 1, low], 2),
            (sendb.at[0, high], recvb.at[bank, 0, high], 1),
        )[i]
        return remote(src, dst, rss.at[phase, i], rsr.at[phase, i], plane(to))

    def parts_start(phase, k):
        for i in {3: (0, 1), 1: (2,), 2: (3,)}[k]:
            part_copy(phase, i).start()

    def parts_pass(phase):
        for i in range(2):
            part_copy(phase, i).wait_recv()
            rows = slice(i * half, (i + 1) * half)
            mine = sendb[1 - i, rows, :].astype(F32)
            sendb[1 - i, rows, :] = (mine + relayed[phase % 2, i].astype(F32)).astype(BF)
            part_copy(phase, 4 + i).start()

    def parts_sent(phase):
        for i in range(6):
            part_copy(phase, i).wait_send()

    def parts_wait(phase):
        for i in range(2, 6):
            part_copy(phase, i).wait_recv()

    ag_i = (x.at[0], xs, xr)
    ag_x = (x.at[1], agx, agxr)
    ag_g = (gb.at[0], agg, aggr)

    @pl.when(s == 0)
    def _():
        w_send(1, up_in.at[0])

    lx.wait()
    gather_start(*ag_i)
    pack_share()

    @pl.when(s == 0)
    def _():
        w_send(0)
        w_send(2, down_in)

    pack_params()
    par_copy = remote(par.at[s], par.at[s], psem.at[0], psem.at[1], sib)
    par_copy.start()
    lu.wait()
    ld.wait()

    @pl.when(s == 0)
    def _():
        for p in (1, 0, 2):
            across(p, z).start()

    for i in range(length // BQ):
        cols = slice(i * BQ, (i + 1) * BQ)
        ids = jnp.where(s == 0, seg_in[0, :, cols], seg_in[1, :, cols]).astype(F32)
        segr[:, cols] = ids
        dq[cols, 0:BQ] = jnp.broadcast_to(ids, (BQ, BQ)).T

    @pl.loop(0, nblk)
    def _(b):
        q0 = pl.multiple_of(b * BQ, BQ)
        k0 = pl.multiple_of(jnp.maximum(b * BQ - SEG_MOST, 0), BQ)
        seg_k = dq[pl.ds(k0, BK), 0:BQ]
        seg_q = segr[:, pl.ds(q0, BQ)]
        kpos = lax.broadcasted_iota(jnp.int32, (BK, BQ), 0) + k0
        qpos = lax.broadcasted_iota(jnp.int32, (BK, BQ), 1) + q0
        allowed = (seg_k == seg_q) & (kpos <= qpos)
        bias[b] = jnp.where(allowed, 0.0, MASKED).astype(BF)

    par_wait = remote(par.at[1 - s], par.at[1 - s], psem.at[0], psem.at[1], sib)
    par_copy.wait_send()
    par_wait.wait_recv()

    @pl.loop(0, 2)
    def _(i):
        sm[i] = jnp.zeros((8, width), F32)

    def first_w_pass(p):
        @pl.when(s == 0)
        def _():
            w_arrive(p, range(2, n, 2), True, lambda p, origin: across(p, origin).start())

    def first_w(p):
        @pl.when(s == 0)
        def _():
            w_arrive(p, range(1, n, 2), False, lambda p, origin: across(p, origin).start())

        @pl.when(s == 1)
        def _():
            for origin in range(n):
                across(p, origin).wait_recv()

    def first_w_sent():
        @pl.when(s == 0)
        def _():
            for p in range(3):
                w_sent(p)
                for origin in range(n):
                    across(p, origin).wait_send()

    def second_w_send():
        @pl.when(s == 1)
        def _():
            w_send(1, up_in.at[0])
            w_send(0)
            w_send(2, down_in)

    def second_w_pass(p):
        @pl.when(s == 1)
        def _():
            w_arrive(p, range(2, n, 2), True, None)

    def second_w_give(p):
        @pl.when(s == 1)
        def _():
            w_arrive(p, range(1, n, 2), False, None)
            forward(p).start()

    def second_w(p):
        @pl.when(s == 0)
        def _():
            forward(p).wait_recv()

    def second_w_sent():
        @pl.when(s == 1)
        def _():
            for p in range(3):
                w_sent(p)
                forward(p).wait_send()

    def prow(layer, r, cols=None):
        if cols is None:
            return par[layer, r : r + 1, :]
        return par[layer, r : r + 1, cols]

    def rope_tables(b, sign):
        ca = taba[0, b]
        sa = taba[1, b]
        c0 = tabb[0]
        s0 = tabb[1]
        cos = ca * c0 - sa * s0
        sin = sa * c0 + ca * s0
        lane = lane_iota(BQ) & (HEAD_DIM - 1)
        return cos, jnp.where(lane < ROT // 2, -sign, sign) * sin

    def rope(u, b, sign):
        halves = []
        lane = lane_iota(BQ) & (HEAD_DIM - 1)
        for i in range(u.shape[0] // BQ):
            part = u[i * BQ : (i + 1) * BQ]
            cos, sin = rope_tables(b + i, sign)
            partner = jnp.where(
                lane < ROT // 2,
                pltpu.roll(part, HL - ROT // 2, 1),
                pltpu.roll(part, ROT // 2, 1),
            )
            halves.append(part * cos + partner * sin)
        return jnp.concatenate(halves, axis=0)

    def stack_heads(block):
        lane = lane_iota(BQ) >> 6
        return jnp.concatenate(
            [jnp.where(lane == h, block, jnp.zeros_like(block)) for h in range(heads)], axis=0
        )

    sub = 64

    def norm_chunk(layer, c):
        @pl.loop(0, chunk // sub)
        def _(i):
            rows = pl.ds(pl.multiple_of(c * chunk + i * sub, sub), sub)
            v = x[layer, rows, :].astype(F32)
            m = jnp.mean(v, axis=-1, keepdims=True)
            v = v - m
            r = lax.rsqrt(jnp.mean(v * v, axis=-1, keepdims=True) + EPS)
            mu[layer, rows, :] = m
            rstd[layer, rows, :] = r
            v = v * r
            an[rows, :] = (v * prow(layer, 0) + prow(layer, 2)).astype(BF)
            mn[rows, :] = (v * prow(layer, 1) + prow(layer, 3)).astype(BF)

    def renorm_all(layer):
        @pl.loop(0, length // sub)
        def _(i):
            rows = pl.ds(pl.multiple_of(i * sub, sub), sub)
            v = (x[layer, rows, :].astype(F32) - mu[layer, rows, :]) * rstd[layer, rows, :]
            an[rows, :] = (v * prow(layer, 0) + prow(layer, 2)).astype(BF)
            mn[rows, :] = (v * prow(layer, 1) + prow(layer, 3)).astype(BF)

    def project_in(layer, c):
        rows = pl.ds(pl.multiple_of(c * chunk, chunk), chunk)
        a = an[rows, :]
        b0 = c * (chunk // BQ)
        lane = lane_iota(chunk)
        u = mm(a, w[layer, 0, :, QO : QO + HL], NN) + prow(layer, 4, slice(0, HL))
        qb[layer, rows, :] = (rope(u, b0, 1.0) * 0.125).astype(BF)
        u = mm(a, w[layer, 0, :, KO - 64 : KO - 64 + HL], NN)
        u = rope(pltpu.roll(u, HL - 64, 1), b0, 1.0)
        kb[layer, rows, :] = u.astype(BF)
        kt[layer, :, rows] = u.T[: heads * HEAD_DIM].astype(BF)
        u = mm(a, w[layer, 0, :, VO : VO + HL], NN) + prow(layer, 5, slice(0, HL))
        u = jnp.where(lane < heads * HEAD_DIM, u, 0.0)
        vb[layer, rows, :] = u.astype(BF)
        vt[layer, :, rows] = u.T[: heads * HEAD_DIM].astype(BF)

    def attend(layer, within=None):
        @pl.loop(0, nblk)
        def _(b):
            if within is not None:
                pl.when(b == nblk // 2)(within)

            q0 = pl.multiple_of(b * BQ, BQ)
            k0 = pl.multiple_of(jnp.maximum(b * BQ - SEG_MOST, 0), BQ)
            qm = stack_heads(qb[layer, pl.ds(q0, BQ), :])
            top = None
            for i in range(BK // BQ):
                keys = kb[layer, pl.ds(k0 + i * BQ, BQ), :]
                blk = bias[b, i * BQ : (i + 1) * BQ, :].astype(F32)
                sc = mm(keys, qm, NT) + jnp.concatenate([blk] * heads, axis=1)
                pscr[i * BQ : (i + 1) * BQ, :] = sc
                peak = jnp.max(sc, axis=0, keepdims=True)
                top = peak if top is None else jnp.maximum(top, peak)
            total = None
            for i in range(BK // BQ):
                e = jnp.exp(pscr[i * BQ : (i + 1) * BQ, :] - top)
                pscr[i * BQ : (i + 1) * BQ, :] = e
                part = jnp.sum(e, axis=0, keepdims=True)
                total = part if total is None else total + part
            lse[layer, b] = top + jnp.log(total)
            inv = 1.0 / total
            ctx = [jnp.zeros((HL - heads * HEAD_DIM, BQ), F32)]
            for h in range(heads):
                cols = slice(h * BQ, (h + 1) * BQ)
                ph = (pscr[:, cols] * inv[:, cols]).astype(BF)
                vals = vt[layer, h * HEAD_DIM : (h + 1) * HEAD_DIM, pl.ds(k0, BK)]
                ctx.append(mm(vals, ph, NN))
            cb[layer, pl.ds(q0, BQ), :] = jnp.concatenate(ctx, axis=0).T.astype(BF)

    def hidden(layer, c):
        rows = pl.ds(pl.multiple_of(c * chunk, chunk), chunk)
        a = mn[rows, :]
        for j in range(width // 256):
            cols = slice(j * 256, (j + 1) * 256)
            u = mm(a, w[layer, 1, :, cols], NN) + prow(layer, 6, cols)
            phi = 0.5 * (1.0 + lax.erf(u * ROOT_HALF))
            hid[layer, rows, cols] = (u * phi).astype(BF)
            slope[layer, rows, cols] = (phi + u * INV_ROOT_TAU * jnp.exp(-0.5 * u * u)).astype(BF)

    def project_out(layer):
        phase = layer
        if layer == 1:
            parts_sent(0)
        for k in (3, 1, 2, 0):
            rows = pl.ds(pl.multiple_of((t ^ k) * chunk, chunk), chunk)
            c = cb[layer, rows, :]
            h = hid[layer, rows, :]
            for j in range(width // 256):
                cols = slice(j * 256, (j + 1) * 256)
                y = mm(c, w[layer, 0, cols, 512:768], NT) + mm(h, w[layer, 2, cols, :], NT)
                if k:
                    sendb[k - 1, :, cols] = y.astype(BF)
                else:
                    ownp[phase % 2, :, cols] = y
            if k:
                parts_start(phase, k)

    def place(layer, stage, out, idx):
        @pl.when(s == layer)
        def _():
            pltpu.make_async_copy(stage, out.at[s], osend.at[idx]).start()

        @pl.when(s != layer)
        def _():
            remote(stage, out.at[s], osend.at[idx], orecv.at[idx // 2], sib).start()

    def placed(layer, stage, out, idx):
        @pl.when(s == layer)
        def _():
            pltpu.make_async_copy(stage, out.at[s], osend.at[idx]).wait()

        @pl.when(s != layer)
        def _():
            remote(stage, out.at[s], osend.at[idx], orecv.at[idx // 2], sib).wait_send()

    def finish_y(layer):
        phase = layer
        parts_wait(phase)
        if layer == 1:
            placed(0, yst, out_y, 0)

        @pl.loop(0, chunk // sub)
        def _(i):
            r = pl.ds(pl.multiple_of(i * sub, sub), sub)
            rows = pl.ds(pl.multiple_of(t * chunk + i * sub, sub), sub)
            y = x[layer, rows, :].astype(F32) + ownp[phase % 2, r, :] + prow(layer, 7)
            for k in range(2):
                y = y + recvb[phase % 2, k, r, :].astype(F32)
            yst[r, :] = y
            if layer == 0:
                x[1, rows, :] = y.astype(BF)

        if layer == 0:
            gather_start(*ag_x)
        place(layer, yst, out_y, layer)

    def reduce_start(layer, p, buf):
        @pl.when(s != layer)
        def _():
            remote(buf.at[p], gsr.at[p], ghs.at[p], ghr.at[p], sib).start()

    def z_item(p, e, sign, buf):
        dest = lax.rem(z + sign * e + n, n)
        way = 0 if sign > 0 else 1
        if e <= 2:
            slot = 2 * way + e - 1
            dst, recv, far = zrecv.at[p, slot], zr.at[p, slot], e
        else:
            place_no = e - 3 if sign > 0 else n - z + e - 4
            dst, recv, far = zacc.at[p, place_no], za.at[way, p, e - 3], 1
        return remote(
            buf.at[p, w_rows(dest)],
            dst,
            zs.at[way, p, e - 1],
            recv,
            (s, lax.rem(z + sign * far + n, n), t),
        )

    def first_of(sign):
        return (z == 0) if sign > 0 else (z == n - 1)

    def z_send(p, buf):
        for e in range(n - 1, 0, -1):
            for sign in (1, -1):
                go = inside(sign * e)
                if e > 1:
                    go = go & first_of(sign)

                @pl.when(go)
                def _():
                    z_item(p, e, sign, buf).start()

    def z_pass(layer, p, buf):
        @pl.when(s == layer)
        def _():
            for e in range(n - 2, 1, -1):
                for sign in (1, -1):

                    @pl.when(inside(sign * e) & inside(-sign))
                    def _():
                        way = 0 if sign > 0 else 1
                        place_no = e - 2 if sign > 0 else n - z + e - 4
                        got = zacc.at[p, place_no]
                        remote(got, got, zs.at[way, p, e - 1], za.at[way, p, e - 2], sib).wait_recv()
                        base = lax.rem(z + sign * e + n, n) * rows_z

                        @pl.loop(0, rows_z // step)
                        def _(i):
                            r = pl.ds(pl.multiple_of(i * step, 16), step)
                            q = pl.ds(pl.multiple_of(base + i * step, 16), step)
                            more = zacc[p, place_no, r, :].astype(F32)
                            buf[p, q, :] = (buf[p, q, :].astype(F32) + more).astype(BF)

                        z_item(p, e, sign, buf).start()

    def z_end(p, buf):
        for slot in range(4):
            sign = 1 if slot < 2 else -1
            e = slot % 2 + 1

            @pl.when(inside(-sign * e))
            def _():
                got = zrecv.at[p, slot]
                remote(got, got, zs.at[0, p, 0], zr.at[p, slot], sib).wait_recv()

                @pl.loop(0, rows_z // step)
                def _(i):
                    r = pl.ds(pl.multiple_of(i * step, 16), step)
                    wacc[p, r, :] = wacc[p, r, :] + zrecv[p, slot, r, :].astype(F32)

    def z_sent(p, buf):
        for e in range(1, n):
            for sign in (1, -1):

                @pl.when(inside(sign * e))
                def _():
                    z_item(p, e, sign, buf).wait_send()

    step = 48

    def reduce_cores(layer, p, buf):
        @pl.when(s == layer)
        def _():
            remote(buf.at[p], gsr.at[p], ghs.at[p], ghr.at[p], sib).wait_recv()

            @pl.loop(0, rows_z // step)
            def _(i):
                r = pl.ds(pl.multiple_of(i * step, 16), step)
                q = pl.ds(pl.multiple_of(z * rows_z + i * step, 16), step)
                wacc[p, r, :] = buf[p, q, :].astype(F32) + gsr[p, q, :].astype(F32)

            for j in range(1, n):
                base = other_z(j) * rows_z

                @pl.loop(0, rows_z // step)
                def _(i):
                    q = pl.ds(pl.multiple_of(base + i * step, 16), step)
                    buf[p, q, :] = (buf[p, q, :].astype(F32) + gsr[p, q, :].astype(F32)).astype(BF)

            z_send(p, buf)

        @pl.when(s != layer)
        def _():
            remote(buf.at[p], gsr.at[p], ghs.at[p], ghr.at[p], sib).wait_send()

    def grad_part(layer, p, buf):
        for j in range(width // 256):
            cols = slice(j * 256, (j + 1) * 256)
            if p == 2:
                buf[p, cols, :] = mm(gb[layer, :, cols], hid[layer], TN).astype(BF)
            elif p == 1:
                buf[p, cols, :] = mm(mn[:, cols], du[...], TN).astype(BF)
            else:
                buf[p, cols, 0:512] = mm(an[:, cols], dqkv[:, 0:512], TN).astype(BF)
                buf[p, cols, 512:768] = (
                    mm(an[:, cols], dqkv[:, 512:768], TN) + mm(gb[layer, :, cols], cb[layer], TN)
                ).astype(BF)
        reduce_start(layer, p, buf)

    def hidden_back(layer, c):
        rows = pl.ds(pl.multiple_of(c * chunk, chunk), chunk)
        g = gb[layer, rows, :]
        for j in range(width // 256):
            cols = slice(j * 256, (j + 1) * 256)
            d = mm(g, w[layer, 2, :, cols], NN) * slope[layer, rows, cols].astype(F32)
            sm[layer, 6:7, cols] = sm[layer, 6:7, cols] + jnp.sum(d, axis=0, keepdims=True)
            du[rows, cols] = d.astype(BF)
        d = pltpu.roll(mm(g, w[layer, 0, :, 512:768], NN), HL - 64, 1)
        lane = lane_iota(chunk)
        dc[rows, :] = jnp.where(lane < heads * HEAD_DIM, d, 0.0).astype(BF)

    def zero_sums():
        @pl.loop(0, length // sub)
        def _(i):
            rows = pl.ds(pl.multiple_of(i * sub, sub), sub)
            dk[rows, :] = jnp.zeros((sub, HL), F32)
            dv[rows, :] = jnp.zeros((sub, HL), F32)

    def attend_back(layer, first, last, within=None):
        @pl.loop(first, last)
        def _(b):
            if within is not None:
                pl.when(b == first + 2)(within)

            q0 = pl.multiple_of(b * BQ, BQ)
            k0 = pl.multiple_of(jnp.maximum(b * BQ - SEG_MOST, 0), BQ)
            qm = stack_heads(qb[layer, pl.ds(q0, BQ), :])
            dm = stack_heads(dc[pl.ds(q0, BQ), :])
            ls = lse[layer, b]
            total = None
            for i in range(BK // BQ):
                krows = pl.ds(k0 + i * BQ, BQ)
                irows = slice(i * BQ, (i + 1) * BQ)
                blk = bias[b, irows, :].astype(F32)
                sc = mm(kb[layer, krows, :], qm, NT) + jnp.concatenate([blk] * heads, axis=1)
                pr = jnp.exp(sc - ls)
                dp = mm(vb[layer, krows, :], dm, NT)
                dv[krows, :] = dv[krows, :] + mm(pr.astype(BF), dm, NN)
                pscr[irows, :] = pr
                dpscr[irows, :] = dp
                part = jnp.sum(pr * dp, axis=0, keepdims=True)
                total = part if total is None else total + part
            for i in range(BK // BQ):
                krows = pl.ds(k0 + i * BQ, BQ)
                irows = slice(i * BQ, (i + 1) * BQ)
                ds = (pscr[irows, :] * (dpscr[irows, :] - total)).astype(BF)
                dscr[irows, :] = ds
                dk[krows, :] = dk[krows, :] + mm(ds, qm, NN)
            out = []
            for h in range(heads):
                keys = kt[layer, h * HEAD_DIM : (h + 1) * HEAD_DIM, pl.ds(k0, BK)]
                out.append(mm(keys, dscr[:, h * BQ : (h + 1) * BQ], NN))
            out.append(jnp.zeros((HL - heads * HEAD_DIM, BQ), F32))
            dq[pl.ds(q0, BQ), :] = jnp.concatenate(out, axis=0).T

    def pack_qkv(layer):
        @pl.loop(0, 4)
        def _(c):
            rows = pl.ds(pl.multiple_of(c * chunk, chunk), chunk)
            b0 = c * (chunk // BQ)
            lane = lane_iota(chunk)
            gq = rope(dq[rows, :], b0, -1.0) * 0.125
            gk = rope(dk[rows, :], b0, -1.0)
            gv = dv[rows, :]
            sm[layer, 4:5, 0:HL] = sm[layer, 4:5, 0:HL] + jnp.sum(gq, axis=0, keepdims=True)
            sm[layer, 5:6, 0:HL] = sm[layer, 5:6, 0:HL] + jnp.sum(gv, axis=0, keepdims=True)
            rk = pltpu.roll(gk, 192, 1)
            rv = pltpu.roll(gv, 128, 1)
            dqkv[rows, 0:256] = jnp.where(lane < 192, gq, rk).astype(BF)
            dqkv[rows, 256:512] = jnp.where(lane < 128, rk, rv).astype(BF)
            dqkv[rows, 512:768] = jnp.where(lane < 64, rv, 0.0).astype(BF)

    def project_back(layer):
        phase = 3 - layer
        parts_sent(1 if layer == 1 else 2)
        for k in (3, 1, 2, 0):
            rows = pl.ds(pl.multiple_of((t ^ k) * chunk, chunk), chunk)
            da_in = dqkv[rows, :]
            du_in = du[rows, :]
            m = mu[layer, rows, :]
            r = rstd[layer, rows, :]
            for j in range(width // 256):
                cols = slice(j * 256, (j + 1) * 256)
                da = mm(da_in, w[layer, 0, cols, :], NT)
                dm = mm(du_in, w[layer, 1, cols, :], NT)
                unit = (x[layer, rows, cols].astype(F32) - m) * r
                sums = [da * unit, dm * unit, da, dm]
                for i in range(4):
                    sm[layer, i : i + 1, cols] = sm[layer, i : i + 1, cols] + jnp.sum(
                        sums[i], axis=0, keepdims=True
                    )
                e = da * prow(layer, 0, cols) + dm * prow(layer, 1, cols)
                if k:
                    sendb[k - 1, :, cols] = e.astype(BF)
                else:
                    ownp[phase % 2, :, cols] = e
            if k:
                parts_start(phase, k)

    def finish_e(layer):
        phase = 3 - layer
        parts_wait(phase)
        stage = gst.at[1 - layer]
        given = gst.at[0]

        @pl.loop(0, chunk // sub)
        def _(i):
            r = pl.ds(pl.multiple_of(i * sub, sub), sub)
            rows = pl.ds(pl.multiple_of(t * chunk + i * sub, sub), sub)
            e = ownp[phase % 2, r, :]
            for k in range(2):
                e = e + recvb[phase % 2, k, r, :].astype(F32)
            rs = rstd[layer, rows, :]
            unit = (x[layer, rows, :].astype(F32) - mu[layer, rows, :]) * rs
            g = given[r, :]
            if layer == 1:
                sm[1, 7:8, :] = sm[1, 7:8, :] + jnp.sum(g, axis=0, keepdims=True)
            d = rs * (
                e
                - jnp.mean(e, axis=-1, keepdims=True)
                - unit * jnp.mean(e * unit, axis=-1, keepdims=True)
            )
            g = g + d
            stage[r, :] = g
            if layer == 1:
                sm[0, 7:8, :] = sm[0, 7:8, :] + jnp.sum(g, axis=0, keepdims=True)
                gb[0, rows, :] = g.astype(BF)

        if layer == 1:
            gather_start(*ag_g)
        place(layer, stage, out_g, 2 + layer)

    norm_chunk(0, t)
    gather_pass(*ag_i)
    lc.wait()
    gb[1, own, :] = gst[0].astype(BF)
    for k in range(1, 4):
        g_copy(k).start()
    first_w_pass(1)

    @pl.loop(1, 4)
    def _(k):
        arrive(*ag_i, k)
        norm_chunk(0, t ^ k)

    first_w(1)

    @pl.loop(0, 4)
    def _(c):
        hidden(0, c)

    first_w_pass(0)
    first_w(0)

    @pl.loop(0, 4)
    def _(c):
        project_in(0, c)

    attend(0, lambda: first_w_pass(2))
    second_w_send()
    first_w(2)
    project_out(0)
    parts_pass(0)
    second_w_pass(1)
    finish_y(0)

    @pl.loop(0, 4)
    def _(k):
        @pl.when(k == 2)
        def _():
            second_w_pass(2)
            second_w_give(0)

        arrive(*ag_x, k)
        norm_chunk(1, t ^ k)

        @pl.when(k == 0)
        def _():
            second_w_give(1)
            gather_pass(*ag_x)
            second_w_pass(0)
            second_w(1)

        hidden(1, t ^ k)

    second_w(0)

    @pl.loop(0, 4)
    def _(c):
        project_in(1, c)

    second_w_give(2)
    attend(1)
    second_w(2)
    project_out(1)

    for k in range(1, 4):
        g_arrival(k).wait_recv()
    zero_sums()

    @pl.loop(0, 4)
    def _(c):
        hidden_back(1, c)

    attend_back(1, 0, nblk, lambda: parts_pass(1))
    pack_qkv(1)
    project_back(1)
    grad_part(1, 2, gw)
    grad_part(1, 1, gw)
    parts_pass(2)
    reduce_cores(1, 2, gw)
    finish_y(1)
    grad_part(1, 0, gw)
    reduce_cores(1, 1, gw)
    finish_e(1)

    late = w.at[1]
    per = chunk // BQ
    first_w_sent()
    second_w_sent()
    zero_sums()
    z_pass(1, 2, gw)
    reduce_cores(1, 0, gw)

    @pl.loop(0, 8)
    def _(step_no):
        k = jnp.where(step_no < 2, 0, jnp.where(step_no < 5, step_no - 1, step_no - 4))

        @pl.when((step_no == 0) | ((step_no >= 2) & (step_no < 5)))
        def _():
            arrive(*ag_g, k)
            hidden_back(0, t ^ k)

        @pl.when(step_no == 5)
        def _():
            grad_part(0, 2, late)

        @pl.when(step_no == 4)
        def _():
            z_pass(1, 1, gw)

        @pl.when(step_no == 6)
        def _():
            reduce_cores(0, 2, late)
            grad_part(0, 1, late)
            z_pass(1, 0, gw)

        @pl.when(step_no == 7)
        def _():
            reduce_cores(0, 1, late)

        @pl.when((step_no == 1) | (step_no >= 5))
        def _():
            attend_back(0, (t ^ k) * per, ((t ^ k) + 1) * per)

        @pl.when(step_no == 1)
        def _():
            gather_pass(*ag_g)
            renorm_all(0)

    z_pass(0, 2, late)
    pack_qkv(0)
    project_back(0)

    to_sib = remote(sm.at[1 - s], smr, sms.at[0], smrs.at[0], sib)
    to_sib.start()
    grad_part(0, 0, late)
    to_sib.wait()
    smt[...] = sm[s] + smr[...]

    def small_z(j):
        return remote(smt, smz.at[j - 1], sms.at[j], smrs.at[j], (s, other_z(j), t))

    def small_copy(k):
        return remote(tall.at[t], tall.at[t], sms.at[n + k - 1], smrs.at[n + k - 1], plane(k))

    for j in range(1, n):
        small_z(j).start()
    parts_pass(3)
    z_pass(0, 1, late)
    reduce_cores(0, 0, late)

    def matrix_end(p):
        z_end(p, late)
        pltpu.make_async_copy(wacc.at[p], out_w.at[p], lsem.at[p]).start()

    matrix_end(2)
    for j in range(1, n):
        small_z(j).wait()
    total = smt[...]
    for j in range(1, n):
        total = total + smz[j - 1]
    tall[t] = total
    for k in range(1, 4):
        small_copy(k).start()
    z_pass(0, 0, late)
    finish_e(0)
    matrix_end(1)
    for k in range(1, 4):
        small_copy(k).wait_send()
        remote(
            tall.at[t ^ k], tall.at[t ^ k], sms.at[n + k - 1], smrs.at[n + k - 1], plane(k)
        ).wait_recv()
    out_s[...] = tall[...]
    matrix_end(0)

    for p in range(3):
        pltpu.make_async_copy(wacc.at[p], out_w.at[p], lsem.at[p]).wait()
        z_sent(p, late)

    for k in range(1, 4):
        g_copy(k).wait_send()
    for i in range(6):
        gather_copy(*ag_i, i).wait_send()
        gather_copy(*ag_x, i).wait_send()
        gather_copy(*ag_g, i).wait_send()
    parts_sent(3)
    placed(1, yst, out_y, 1)
    placed(1, gst.at[0], out_g, 3)
    placed(0, gst.at[1], out_g, 2)
    remote(yst, out_y.at[1 - s], osend.at[0], orecv.at[0], sib).wait_recv()
    remote(gst.at[0], out_g.at[1 - s], osend.at[0], orecv.at[1], sib).wait_recv()


def write_outputs(
    head_cols, y, g, wg, small, y_out, g_out, up, down, qkv, out, gain, shift, qv, upb, resid, sem
):
    pairs = ((y, y_out), (g, g_out), (wg.at[1], up), (wg.at[2], down))
    copies = [pltpu.make_async_copy(src, dst, sem.at[i]) for i, (src, dst) in enumerate(pairs)]
    for copy in copies:
        copy.start()
    first = wg[0]
    width = first.shape[1]
    for i in range(3):
        turned = pltpu.roll(first, width - i * head_cols, 1) if i else first
        qkv[i] = turned[:, :head_cols]
    last = pltpu.roll(first, width - 3 * head_cols, 1)[:, :256]
    out[...] = last.T[:head_cols, :]
    total = small[0] + small[1] + small[2] + small[3]
    gain[...] = total[0:2]
    shift[...] = total[2:4]
    resid[...] = total[7:8]
    spread = small[0]
    upb[:, 0:width] = small[0, 6:7, :]
    for i in range(1, 4):
        spread = spread + pltpu.roll(small[i], i * head_cols, 1)
        upb[:, i * width : (i + 1) * width] = small[i, 6:7, :]
    qv[...] = spread[4:6]
    for copy in copies:
        copy.wait()


def rotary_rows(length, heads):
    rate = np.zeros((HL,), np.float64)
    for h in range(heads):
        for j in range(ROT // 2):
            value = math.exp(j * (-2.0 * math.log(10000.0) / ROT))
            rate[h * HEAD_DIM + j] = value
            rate[h * HEAD_DIM + j + ROT // 2] = value
    live = (np.arange(HL) < heads * HEAD_DIM).astype(np.float64)
    starts = np.arange(length // BQ)[:, None] * BQ * rate[None]
    offsets = np.arange(BQ)[:, None] * rate[None]
    first = np.stack([np.cos(starts), np.sin(starts)])[:, :, None].astype(np.float32)
    second = np.stack([np.cos(offsets) * live, np.sin(offsets) * live]).astype(np.float32)
    return first, second


def body(
    n,
    inputs,
    segment_ids,
    cotangent,
    qkv_weight,
    out_weight,
    up_weight,
    down_weight,
    norm_gain,
    norm_bias,
    qv_bias,
    up_bias,
    resid_bias,
):
    micro, _, chunk, width = inputs.shape
    length = segment_ids.shape[2]
    head_cols = qkv_weight.shape[3]
    rows_z = qkv_weight.shape[2]
    ff_local = up_weight.shape[2]
    heads = head_cols // HEAD_DIM
    assert micro == 2 and length == 4 * chunk and ff_local == width
    assert head_cols == 192 and width == 768

    first, second = rotary_rows(length, heads)

    vm = pl.BlockSpec(memory_space=pltpu.VMEM)
    anywhere = pl.BlockSpec(memory_space=pl.ANY)
    blk = heads * BQ
    nblk = length // BQ
    dma = pltpu.SemaphoreType.DMA

    def vmem(*shape, dtype=BF):
        return pltpu.VMEM(shape, dtype)

    scratch = dict(
        w=vmem(2, 3, width, width),
        x=vmem(2, length, width),
        an=vmem(length, width),
        mn=vmem(length, width),
        mu=vmem(2, length, 1, dtype=F32),
        rstd=vmem(2, length, 1, dtype=F32),
        qb=vmem(2, length, HL),
        kb=vmem(2, length, HL),
        vb=vmem(2, length, HL),
        kt=vmem(2, heads * HEAD_DIM, length),
        vt=vmem(2, heads * HEAD_DIM, length),
        cb=vmem(2, length, HL),
        lse=vmem(2, nblk, 1, blk, dtype=F32),
        slope=vmem(2, length, width),
        hid=vmem(2, length, width),
        gb=vmem(2, length, width),
        du=vmem(length, width),
        dqkv=vmem(length, width),
        dc=vmem(length, HL),
        dq=vmem(length, HL, dtype=F32),
        dk=vmem(length, HL, dtype=F32),
        dv=vmem(length, HL, dtype=F32),
        bias=vmem(nblk, BK, BQ),
        pscr=vmem(BK, blk, dtype=F32),
        dpscr=vmem(BK, blk, dtype=F32),
        dscr=vmem(BK, blk),
        sendb=vmem(3, chunk, width),
        recvb=vmem(2, 2, chunk, width),
        relayed=vmem(2, 2, chunk // 2, width),
        ownp=vmem(2, chunk, width, dtype=F32),
        gw=vmem(3, width, width),
        gsr=vmem(3, width, width),
        zrecv=vmem(3, 4, rows_z, width),
        zacc=vmem(3, max(n - 3, 1), rows_z, width),
        wacc=vmem(3, rows_z, width, dtype=F32),
        yst=vmem(chunk, width, dtype=F32),
        gst=vmem(2, chunk, width, dtype=F32),
        segr=vmem(1, length, dtype=F32),
        par=vmem(2, 8, width, dtype=F32),
        sm=vmem(2, 8, width, dtype=F32),
        smr=vmem(8, width, dtype=F32),
        smt=vmem(8, width, dtype=F32),
        smz=vmem(n - 1, 8, width, dtype=F32),
        tall=vmem(4, 8, width, dtype=F32),
        lsem=dma((8,)),
        psem=dma((2,)),
        xs=dma((6,)),
        xr=dma((6,)),
        agx=dma((6,)),
        agxr=dma((6,)),
        agg=dma((6,)),
        aggr=dma((6,)),
        gs=dma((3,)),
        gr=dma((3,)),
        ws=dma((4, 3, n)),
        wr=dma((3, n)),
        fs=dma((3, n)),
        fr=dma((3, n)),
        rss=dma((4, 6)),
        rsr=dma((4, 6)),
        osend=dma((4,)),
        orecv=dma((2,)),
        ghs=dma((3,)),
        ghr=dma((3,)),
        zs=dma((2, 3, n)),
        zr=dma((3, 4)),
        za=dma((2, 3, n)),
        sms=dma((n + 3,)),
        smrs=dma((n + 3,)),
    )
    out_y, out_g, out_w, out_s = pl.pallas_call(
        functools.partial(kernel, n, heads),
        out_shape=(
            jax.ShapeDtypeStruct((2, chunk, width), F32),
            jax.ShapeDtypeStruct((2, chunk, width), F32),
            jax.ShapeDtypeStruct((3, rows_z, width), F32),
            jax.ShapeDtypeStruct((4, 8, width), F32),
        ),
        in_specs=[anywhere, anywhere, vm, vm, vm, anywhere, anywhere] + [vm] * 7,
        out_specs=(anywhere, anywhere, anywhere, vm),
        scratch_shapes=list(scratch.values()),
        compiler_params=pltpu.CompilerParams(
            collective_id=0, has_side_effects=True, vmem_limit_bytes=67043328
        ),
        name="two_layers",
    )(
        inputs.reshape(micro, chunk, width),
        cotangent.reshape(micro, chunk, width),
        segment_ids,
        qkv_weight,
        out_weight,
        up_weight,
        down_weight[0].T,
        norm_gain,
        norm_bias,
        qv_bias,
        up_bias,
        resid_bias,
        jnp.asarray(first),
        jnp.asarray(second),
    )
    shapes = (
        (2, chunk, width),
        (2, chunk, width),
        (rows_z, width),
        (rows_z, width),
        (3, rows_z, head_cols),
        (head_cols, rows_z),
        (2, width),
        (2, width),
        (2, width),
        (1, 4 * width),
        (1, width),
    )
    y, g, up_g, down_g, qkv_g, out_gr, gain_g, shift_g, qv_g, upb_g, resid_g = pl.pallas_call(
        functools.partial(write_outputs, head_cols),
        out_shape=tuple(jax.ShapeDtypeStruct(shape, F32) for shape in shapes),
        in_specs=[vm] * 4,
        out_specs=(anywhere,) * 4 + (vm,) * 7,
        scratch_shapes=[dma((4,))],
        name="outputs",
    )(out_y, out_g, out_w, out_s)
    return (
        y.reshape(1, micro, 1, chunk, width),
        g.reshape(1, micro, 1, chunk, width),
        qkv_g[None],
        out_gr[None],
        up_g[None],
        down_g.T[None],
        gain_g[None],
        shift_g[None],
        qv_g[None],
        upb_g,
        resid_g,
    )


def solution(mesh):
    return jax.shard_map(
        functools.partial(body, mesh.shape["dp"]),
        mesh=mesh,
        in_specs=(
            P(None, "dp", "tensor", None),
            P(None, "dp", None),
            P(None, "dp", "tensor", None),
            P("section", None, "dp", "tensor"),
            P("section", "tensor", "dp"),
            P("section", "dp", "tensor"),
            P("section", "tensor", "dp"),
            P("section", None, None),
            P("section", None, None),
            P("section", None, None),
            P("section", None),
            P("section", None),
        ),
        out_specs=(
            P("section", None, "dp", "tensor", None),
            P("section", None, "dp", "tensor", None),
            P("section", None, "dp", "tensor"),
            P("section", "tensor", "dp"),
            P("section", "dp", "tensor"),
            P("section", "tensor", "dp"),
            P("section", None, None),
            P("section", None, None),
            P("section", None, None),
            P("section", None),
            P("section", None),
        ),
        check_vma=False,
    )
```

```python
import functools
import math

import jax
import jax.numpy as jnp
import numpy as np
from jax import lax
from jax.experimental import pallas as pl
from jax.experimental.pallas import tpu as pltpu
from jax.sharding import PartitionSpec as P

HEAD_DIM = 64
ROT = 16
SEG_MOST = 384
EPS = 1e-05
MASKED = -1e30
ROOT_HALF = 0.7071067811865476
INV_ROOT_TAU = 0.3989422804014327

BF = jnp.bfloat16
F32 = jnp.float32
MESH = pl.DeviceIdType.MESH

NN = (((1,), (0,)), ((), ()))
NT = (((1,), (1,)), ((), ()))
TN = (((0,), (0,)), ((), ()))

BQ = 128
BK = BQ + SEG_MOST
HL = 256
QO, KO, VO, OO = 0, 192, 384, 576


def mm(a, b, dims):
    return lax.dot_general(a, b, dims, preferred_element_type=F32)


def lane_iota(rows, cols=HL):
    return lax.broadcasted_iota(jnp.int32, (rows, cols), 1)


def remote(src, dst, send, recv, dev):
    return pltpu.make_async_remote_copy(
        src_ref=src, dst_ref=dst, send_sem=send, recv_sem=recv, device_id=dev, device_id_type=MESH
    )


def kernel(
    n,
    heads,
    x_in,
    cot_in,
    seg_far,
    qkv_far,
    wo_far,
    up_in,
    down_in,
    gain_far,
    shift_far,
    qv_far,
    upb_far,
    resid_far,
    taba_far,
    tabb_far,
    out_y,
    out_g,
    out_w,
    out_s,
    seg_in,
    qkv_in,
    wo_in,
    gain_in,
    shift_in,
    qv_in,
    upb_in,
    resid_in,
    taba,
    tabb,
    w,
    x,
    an,
    mn,
    mu,
    rstd,
    qb,
    kb,
    vb,
    kt,
    vt,
    cb,
    lse,
    slope,
    hid,
    gb,
    du,
    dqkv,
    dc,
    dq,
    dk,
    dv,
    bias,
    pscr,
    dpscr,
    dscr,
    pbf,
    sendb,
    recvb,
    relayed,
    ownp,
    gw,
    gsr,
    zrecv,
    zacc,
    wacc,
    yst,
    gst,
    segr,
    par,
    sm,
    smr,
    smt,
    smz,
    tall,
    lsem,
    isem,
    psem,
    xs,
    xr,
    agx,
    agxr,
    agg,
    aggr,
    gs,
    gr,
    ws,
    wr,
    fs,
    fr,
    rss,
    rsr,
    osend,
    orecv,
    ghs,
    ghr,
    zs,
    zr,
    za,
    sms,
    smrs,
):
    s = lax.axis_index("section")
    z = lax.axis_index("dp")
    t = lax.axis_index("tensor")
    sib = (1 - s, z, t)
    width = x.shape[2]
    length = x.shape[1]
    chunk = length // 4
    rows_z = up_in.shape[1]
    half = chunk // 2
    nblk = length // BQ
    own = pl.ds(t * chunk, chunk)
    zrows = pl.ds(z * rows_z, rows_z)

    def plane(k):
        return (s, z, t ^ k)

    def other_z(j):
        return lax.rem(z + j, n)

    lx = pltpu.make_async_copy(x_in.at[s], x.at[0, own], lsem.at[0])
    lc = pltpu.make_async_copy(cot_in.at[s], gst.at[0], lsem.at[1])
    lu = pltpu.make_async_copy(up_in.at[0], w.at[s, 1, zrows], lsem.at[3])
    ld = pltpu.make_async_copy(down_in, w.at[s, 2, zrows], lsem.at[4])
    small_loads = [
        pltpu.make_async_copy(src, dst, isem.at[i])
        for i, (src, dst) in enumerate(
            (
                (qkv_far, qkv_in),
                (wo_far, wo_in),
                (gain_far, gain_in),
                (shift_far, shift_in),
                (qv_far, qv_in),
                (upb_far, upb_in),
                (resid_far, resid_in),
                (seg_far, seg_in),
                (taba_far, taba),
                (tabb_far, tabb),
            )
        )
    ]
    lx.start()
    for load in small_loads:
        load.start()
    lu.start()
    ld.start()
    lc.start()

    barrier = pltpu.get_barrier_semaphore()
    pl.semaphore_signal(barrier, inc=1, device_id=sib, device_id_type=MESH)
    for k in range(1, 4):
        pl.semaphore_signal(barrier, inc=1, device_id=plane(k), device_id_type=MESH)
    for j in range(1, n):
        pl.semaphore_signal(barrier, inc=1, device_id=(s, other_z(j), t), device_id_type=MESH)
    pl.semaphore_wait(barrier, 4 + n - 1)

    head_cols = heads * HEAD_DIM

    def picks(first):
        rows = lax.broadcasted_iota(jnp.int32, (head_cols, width), 0)
        cols = lax.broadcasted_iota(jnp.int32, (head_cols, width), 1)
        return (rows + first == cols).astype(F32).astype(BF)

    def pack_share():
        packed = mm(qkv_in[0, 0], picks(QO), NN) + mm(qkv_in[0, 1], picks(KO), NN)
        packed = packed + mm(qkv_in[0, 2], picks(VO), NN) + mm(wo_in[0], picks(OO), TN)
        w[s, 0, zrows, :] = packed.astype(BF)

    def pack_params():
        par[s, 0:2, :] = gain_in[0]
        par[s, 2:4, :] = shift_in[0]
        par[s, 4:6, :] = qv_in[0]
        par[s, 6:7, :] = upb_in[0:1, pl.ds(pl.multiple_of(t * width, 128), width)]
        par[s, 7:8, :] = resid_in[...]
        rows8 = par[s]
        turned = rows8
        for i in range(1, 4):
            turned = jnp.where(t == i, pltpu.roll(rows8, width - i * head_cols, 1), turned)
        row = lax.broadcasted_iota(jnp.int32, (8, width), 0)
        par[s] = jnp.where((row == 4) | (row == 5), turned, rows8)

    def w_rows(origin):
        return pl.ds(origin * rows_z, rows_z)

    def w_step(p, origin, far, src=None):
        rows = w_rows(origin)
        i = {1: 0, 2: 1, -1: 2, -2: 3}[far]
        return remote(
            w.at[s, p, rows] if src is None else src,
            w.at[s, p, rows],
            ws.at[i, p, origin],
            wr.at[p, origin],
            (s, lax.rem(z + far + n, n), t),
        )

    def inside(far):
        return (z + far < n) if far > 0 else (z + far >= 0)

    def w_send(p, src=None):
        for far in (2, -2, 1, -1):

            @pl.when(inside(far))
            def _():
                w_step(p, z, far, src).start()

    def w_arrive(p, passed, then):
        for e in range(2, n, 2) if passed else range(1, n):
            for sign in (1, -1):
                here = inside(-sign * e)
                if passed:
                    here = here & inside(sign)
                elif e % 2 == 0:
                    here = here & jnp.logical_not(inside(sign))

                @pl.when(here)
                def _():
                    origin = lax.rem(z - sign * e + n, n)
                    w_step(p, origin, sign).wait_recv()
                    if passed:
                        for far in (sign, 2 * sign):

                            @pl.when(inside(far))
                            def _():
                                w_step(p, origin, far).start()

                    if then is not None:
                        then(p, origin)

    def w_sent(p):
        for far in (1, -1, 2, -2):

            @pl.when(inside(far))
            def _():
                w_step(p, z, far).wait_send()

            sign = 1 if far > 0 else -1
            for e in range(2, n, 2):

                @pl.when(inside(-sign * e) & inside(far))
                def _():
                    w_step(p, lax.rem(z - sign * e + n, n), far).wait_send()

    def across(p, origin, layer=0):
        part = w.at[layer, p, w_rows(origin)]
        return remote(part, part, fs.at[p, origin], fr.at[p, origin], sib)

    def g_copy(k):
        return remote(gb.at[1, own], gb.at[1, own], gs.at[k - 1], gr.at[k - 1], plane(k))

    def g_arrival(k):
        rows = pl.ds((t ^ k) * chunk, chunk)
        return remote(gb.at[1, rows], gb.at[1, rows], gs.at[k - 1], gr.at[k - 1], plane(k))

    hops = ((0, 0, 1), (0, 1, 2), (0, 1, 1), (0, 0, 2), (1, 0, 2), (2, 1, 1))

    def gather_copy(buf, send, recv, i):
        k, h, to = hops[i]
        rows = pl.ds((t ^ k) * chunk + h * half, half)
        return remote(buf.at[rows], buf.at[rows], send.at[i], recv.at[i], plane(to))

    def gather_arrival(buf, send, recv, i):
        k, h, to = hops[i]
        rows = pl.ds((t ^ k ^ to) * chunk + h * half, half)
        return remote(buf.at[rows], buf.at[rows], send.at[i], recv.at[i], plane(to))

    def gather_start(buf, send, recv):
        for i in range(4):
            gather_copy(buf, send, recv, i).start()

    def gather_pass(buf, send, recv):
        gather_arrival(buf, send, recv, 0).wait_recv()
        gather_copy(buf, send, recv, 4).start()
        gather_arrival(buf, send, recv, 1).wait_recv()
        gather_copy(buf, send, recv, 5).start()

    def gather_wait(buf, send, recv, k):
        for i in {1: (2,), 2: (3,), 3: (4, 5)}[k]:
            gather_arrival(buf, send, recv, i).wait_recv()

    def arrive(buf, send, recv, k):
        for i in range(1, 4):

            @pl.when(k == i)
            def _():
                gather_wait(buf, send, recv, i)

    def part_copy(phase, i):
        low, high = pl.ds(0, half), pl.ds(half, half)
        bank = phase % 2
        src, dst, to = (
            (sendb.at[2, low], relayed.at[bank, 0], 1),
            (sendb.at[2, high], relayed.at[bank, 1], 2),
            (sendb.at[0, low], recvb.at[bank, 0, low], 1),
            (sendb.at[1, high], recvb.at[bank, 1, high], 2),
            (sendb.at[1, low], recvb.at[bank, 1, low], 2),
            (sendb.at[0, high], recvb.at[bank, 0, high], 1),
        )[i]
        return remote(src, dst, rss.at[phase, i], rsr.at[phase, i], plane(to))

    def parts_start(phase, k):
        for i in {3: (0, 1), 1: (2,), 2: (3,)}[k]:
            part_copy(phase, i).start()

    def parts_pass(phase):
        for i in range(2):
            part_copy(phase, i).wait_recv()
            rows = slice(i * half, (i + 1) * half)
            mine = sendb[1 - i, rows, :].astype(F32)
            sendb[1 - i, rows, :] = (mine + relayed[phase % 2, i].astype(F32)).astype(BF)
            part_copy(phase, 4 + i).start()

    def parts_sent(phase):
        for i in range(6):
            part_copy(phase, i).wait_send()

    def parts_wait(phase):
        for i in range(2, 6):
            part_copy(phase, i).wait_recv()

    ag_i = (x.at[0], xs, xr)
    ag_x = (x.at[1], agx, agxr)
    ag_g = (gb.at[0], agg, aggr)

    @pl.when(s == 0)
    def _():
        w_send(1, up_in.at[0])

    lx.wait()
    gather_start(*ag_i)
    for load in small_loads:
        load.wait()
    pack_share()

    @pl.when(s == 0)
    def _():
        w_send(0)
        w_send(2, down_in)

    pack_params()
    par_copy = remote(par.at[s], par.at[s], psem.at[0], psem.at[1], sib)
    par_copy.start()
    lu.wait()
    ld.wait()

    @pl.when(s == 0)
    def _():
        for p in (1, 0, 2):
            across(p, z).start()

    for i in range(length // BQ):
        cols = slice(i * BQ, (i + 1) * BQ)
        ids = jnp.where(s == 0, seg_in[0, :, cols], seg_in[1, :, cols]).astype(F32)
        segr[:, cols] = ids
        dq[cols, 0:BQ] = jnp.broadcast_to(ids, (BQ, BQ)).T

    @pl.loop(0, nblk)
    def _(b):
        q0 = pl.multiple_of(b * BQ, BQ)
        k0 = pl.multiple_of(jnp.maximum(b * BQ - SEG_MOST, 0), BQ)
        seg_k = dq[pl.ds(k0, BK), 0:BQ]
        seg_q = segr[:, pl.ds(q0, BQ)]
        kpos = lax.broadcasted_iota(jnp.int32, (BK, BQ), 0) + k0
        qpos = lax.broadcasted_iota(jnp.int32, (BK, BQ), 1) + q0
        allowed = (seg_k == seg_q) & (kpos <= qpos)
        bias[b] = jnp.where(allowed, 0.0, MASKED).astype(BF)

    par_wait = remote(par.at[1 - s], par.at[1 - s], psem.at[0], psem.at[1], sib)
    par_copy.wait_send()
    par_wait.wait_recv()

    @pl.loop(0, 2)
    def _(i):
        sm[i] = jnp.zeros((8, width), F32)

    def first_w_pass(p):
        @pl.when(s == 0)
        def _():
            w_arrive(p, True, lambda p, origin: across(p, origin).start())

    def first_w(p):
        @pl.when(s == 0)
        def _():
            w_arrive(p, False, lambda p, origin: across(p, origin).start())

        @pl.when(s == 1)
        def _():
            for origin in range(n):
                across(p, origin).wait_recv()

    def first_w_sent():
        @pl.when(s == 0)
        def _():
            for p in range(3):
                w_sent(p)
                for origin in range(n):
                    across(p, origin).wait_send()

    def second_w_send():
        @pl.when(s == 1)
        def _():
            w_send(1, up_in.at[0])
            w_send(0)
            w_send(2, down_in)
            for p in (1, 0, 2):
                across(p, z, 1).start()

    def second_w_pass(p):
        @pl.when(s == 1)
        def _():
            w_arrive(p, True, lambda p, origin: across(p, origin, 1).start())

    def second_w_give(p):
        @pl.when(s == 1)
        def _():
            w_arrive(p, False, lambda p, origin: across(p, origin, 1).start())

    def second_w(p):
        @pl.when(s == 0)
        def _():
            for origin in range(n):
                across(p, origin, 1).wait_recv()

    def second_w_sent():
        @pl.when(s == 1)
        def _():
            for p in range(3):
                w_sent(p)
                for origin in range(n):
                    across(p, origin, 1).wait_send()

    def prow(layer, r, cols=None):
        if cols is None:
            return par[layer, r : r + 1, :]
        return par[layer, r : r + 1, cols]

    def rope_tables(b, sign):
        ca = taba[0, b]
        sa = taba[1, b]
        c0 = tabb[0]
        s0 = tabb[1]
        cos = ca * c0 - sa * s0
        sin = sa * c0 + ca * s0
        lane = lane_iota(BQ) & (HEAD_DIM - 1)
        return cos, jnp.where(lane < ROT // 2, -sign, sign) * sin

    def rope(u, b, sign):
        halves = []
        lane = lane_iota(BQ) & (HEAD_DIM - 1)
        for i in range(u.shape[0] // BQ):
            part = u[i * BQ : (i + 1) * BQ]
            cos, sin = rope_tables(b + i, sign)
            partner = jnp.where(
                lane < ROT // 2,
                pltpu.roll(part, HL - ROT // 2, 1),
                pltpu.roll(part, ROT // 2, 1),
            )
            halves.append(part * cos + partner * sin)
        return jnp.concatenate(halves, axis=0)

    def stack_heads(block):
        lane = lane_iota(BQ) >> 6
        return jnp.concatenate(
            [jnp.where(lane == h, block, jnp.zeros_like(block)) for h in range(heads)], axis=0
        )

    sub = 64

    def norm_chunk(layer, c):
        @pl.loop(0, chunk // sub)
        def _(i):
            rows = pl.ds(pl.multiple_of(c * chunk + i * sub, sub), sub)
            v = x[layer, rows, :].astype(F32)
            m = jnp.mean(v, axis=-1, keepdims=True)
            v = v - m
            r = lax.rsqrt(jnp.mean(v * v, axis=-1, keepdims=True) + EPS)
            mu[layer, rows, :] = m
            rstd[layer, rows, :] = r
            v = v * r
            an[rows, :] = (v * prow(layer, 0) + prow(layer, 2)).astype(BF)
            mn[rows, :] = (v * prow(layer, 1) + prow(layer, 3)).astype(BF)

    def renorm_all(layer):
        @pl.loop(0, length // sub)
        def _(i):
            rows = pl.ds(pl.multiple_of(i * sub, sub), sub)
            v = (x[layer, rows, :].astype(F32) - mu[layer, rows, :]) * rstd[layer, rows, :]
            an[rows, :] = (v * prow(layer, 0) + prow(layer, 2)).astype(BF)
            mn[rows, :] = (v * prow(layer, 1) + prow(layer, 3)).astype(BF)

    def project_in(layer, c):
        rows = pl.ds(pl.multiple_of(c * chunk, chunk), chunk)
        a = an[rows, :]
        b0 = c * (chunk // BQ)
        lane = lane_iota(chunk)
        u = mm(a, w[layer, 0, :, QO : QO + HL], NN) + prow(layer, 4, slice(0, HL))
        qb[layer, rows, :] = (rope(u, b0, 1.0) * 0.125).astype(BF)
        u = mm(a, w[layer, 0, :, KO - 64 : KO - 64 + HL], NN)
        u = rope(pltpu.roll(u, HL - 64, 1), b0, 1.0)
        kb[layer, rows, :] = u.astype(BF)
        kt[layer, :, rows] = u.T[: heads * HEAD_DIM].astype(BF)
        u = mm(a, w[layer, 0, :, VO : VO + HL], NN) + prow(layer, 5, slice(0, HL))
        u = jnp.where(lane < heads * HEAD_DIM, u, 0.0)
        vb[layer, rows, :] = u.astype(BF)
        vt[layer, :, rows] = u.T[: heads * HEAD_DIM].astype(BF)

    def attend(layer, within=None):
        @pl.loop(0, nblk)
        def _(b):
            if within is not None:
                pl.when(b == nblk // 2)(within)

            q0 = pl.multiple_of(b * BQ, BQ)
            k0 = pl.multiple_of(jnp.maximum(b * BQ - SEG_MOST, 0), BQ)
            qm = stack_heads(qb[layer, pl.ds(q0, BQ), :])
            pscr[...] = mm(kb[layer, pl.ds(k0, BK), :], qm, NT)
            top = None
            for i in range(BK // BQ):
                irows = slice(i * BQ, (i + 1) * BQ)
                blk = bias[b, irows, :].astype(F32)
                sc = pscr[irows, :] + jnp.concatenate([blk] * heads, axis=1)
                pscr[irows, :] = sc
                peak = jnp.max(sc, axis=0, keepdims=True)
                top = peak if top is None else jnp.maximum(top, peak)
            total = None
            for i in range(BK // BQ):
                e = jnp.exp(pscr[i * BQ : (i + 1) * BQ, :] - top)
                pscr[i * BQ : (i + 1) * BQ, :] = e
                part = jnp.sum(e, axis=0, keepdims=True)
                total = part if total is None else total + part
            lse[layer, b] = top + jnp.log(total)
            inv = 1.0 / total
            ctx = [jnp.zeros((HL - heads * HEAD_DIM, BQ), F32)]
            for h in range(heads):
                cols = slice(h * BQ, (h + 1) * BQ)
                ph = (pscr[:, cols] * inv[:, cols]).astype(BF)
                vals = vt[layer, h * HEAD_DIM : (h + 1) * HEAD_DIM, pl.ds(k0, BK)]
                ctx.append(mm(vals, ph, NN))
            cb[layer, pl.ds(q0, BQ), :] = jnp.concatenate(ctx, axis=0).T.astype(BF)

    def hidden(layer, c):
        rows = pl.ds(pl.multiple_of(c * chunk, chunk), chunk)
        a = mn[rows, :]
        for j in range(width // 256):
            cols = slice(j * 256, (j + 1) * 256)
            u = mm(a, w[layer, 1, :, cols], NN) + prow(layer, 6, cols)
            phi = 0.5 * (1.0 + lax.erf(u * ROOT_HALF))
            hid[layer, rows, cols] = (u * phi).astype(BF)
            slope[layer, rows, cols] = (phi + u * INV_ROOT_TAU * jnp.exp(-0.5 * u * u)).astype(BF)

    def project_out(layer):
        phase = layer
        if layer == 1:
            parts_sent(0)
        for k in (3, 1, 2, 0):
            rows = pl.ds(pl.multiple_of((t ^ k) * chunk, chunk), chunk)
            c = cb[layer, rows, :]
            h = hid[layer, rows, :]
            for j in range(width // 256):
                cols = slice(j * 256, (j + 1) * 256)
                y = mm(c, w[layer, 0, cols, 512:768], NT) + mm(h, w[layer, 2, cols, :], NT)
                if k:
                    sendb[k - 1, :, cols] = y.astype(BF)
                else:
                    ownp[phase % 2, :, cols] = y
            if k:
                parts_start(phase, k)

    def place(layer, stage, out, idx):
        @pl.when(s == layer)
        def _():
            pltpu.make_async_copy(stage, out.at[s], osend.at[idx]).start()

        @pl.when(s != layer)
        def _():
            remote(stage, out.at[s], osend.at[idx], orecv.at[idx // 2], sib).start()

    def placed(layer, stage, out, idx):
        @pl.when(s == layer)
        def _():
            pltpu.make_async_copy(stage, out.at[s], osend.at[idx]).wait()

        @pl.when(s != layer)
        def _():
            remote(stage, out.at[s], osend.at[idx], orecv.at[idx // 2], sib).wait_send()

    def finish_y(layer):
        phase = layer
        parts_wait(phase)
        if layer == 1:
            placed(0, yst, out_y, 0)

        @pl.loop(0, chunk // sub)
        def _(i):
            r = pl.ds(pl.multiple_of(i * sub, sub), sub)
            rows = pl.ds(pl.multiple_of(t * chunk + i * sub, sub), sub)
            y = x[layer, rows, :].astype(F32) + ownp[phase % 2, r, :] + prow(layer, 7)
            for k in range(2):
                y = y + recvb[phase % 2, k, r, :].astype(F32)
            yst[r, :] = y
            if layer == 0:
                x[1, rows, :] = y.astype(BF)

        if layer == 0:
            gather_start(*ag_x)
        place(layer, yst, out_y, layer)

    def reduce_start(layer, p, j, buf):
        rows = pl.ds(j * 256, 256)


        @pl.when(s != layer)
        def _():
            remote(buf.at[p, rows], gsr.at[p, rows], ghs.at[p, j], ghr.at[p, j], sib).start()

    def z_item(p, e, sign, buf):
        dest = lax.rem(z + sign * e + n, n)
        way = 0 if sign > 0 else 1
        if e <= 2:
            slot = 2 * way + e - 1
            dst, recv, far = zrecv.at[p, slot], zr.at[p, slot], e
        else:
            place_no = e - 3 if sign > 0 else n - z + e - 4
            dst, recv, far = zacc.at[p, place_no], za.at[way, p, e - 3], 1
        return remote(
            buf.at[p, w_rows(dest)],
            dst,
            zs.at[way, p, e - 1],
            recv,
            (s, lax.rem(z + sign * far + n, n), t),
        )

    def first_of(sign):
        return (z == 0) if sign > 0 else (z == n - 1)

    def z_send(p, buf):
        for e in range(n - 1, 0, -1):
            for sign in (1, -1):
                go = inside(sign * e)
                if e > 1:
                    go = go & first_of(sign)

                @pl.when(go)
                def _():
                    z_item(p, e, sign, buf).start()

    def z_pass(layer, p, buf):
        @pl.when(s == layer)
        def _():
            for e in range(n - 2, 1, -1):
                for sign in (1, -1):

                    @pl.when(inside(sign * e) & inside(-sign))
                    def _():
                        way = 0 if sign > 0 else 1
                        place_no = e - 2 if sign > 0 else n - z + e - 4
                        got = zacc.at[p, place_no]
                        remote(got, got, zs.at[way, p, e - 1], za.at[way, p, e - 2], sib).wait_recv()
                        base = lax.rem(z + sign * e + n, n) * rows_z

                        @pl.loop(0, rows_z // step)
                        def _(i):
                            r = pl.ds(pl.multiple_of(i * step, 16), step)
                            q = pl.ds(pl.multiple_of(base + i * step, 16), step)
                            more = zacc[p, place_no, r, :].astype(F32)
                            buf[p, q, :] = (buf[p, q, :].astype(F32) + more).astype(BF)

                        z_item(p, e, sign, buf).start()

    def z_end(p, buf):
        for slot in range(4):
            sign = 1 if slot < 2 else -1
            e = slot % 2 + 1

            @pl.when(inside(-sign * e))
            def _():
                got = zrecv.at[p, slot]
                remote(got, got, zs.at[0, p, 0], zr.at[p, slot], sib).wait_recv()

                @pl.loop(0, rows_z // step)
                def _(i):
                    r = pl.ds(pl.multiple_of(i * step, 16), step)
                    wacc[p, r, :] = wacc[p, r, :] + zrecv[p, slot, r, :].astype(F32)

    def z_sent(p, buf):
        for e in range(1, n):
            for sign in (1, -1):

                @pl.when(inside(sign * e))
                def _():
                    z_item(p, e, sign, buf).wait_send()

    step = 48

    def reduce_cores(layer, p, buf):
        @pl.when(s == layer)
        def _():
            for j in range(width // 256):
                rows = pl.ds(j * 256, 256)
                remote(buf.at[p, rows], gsr.at[p, rows], ghs.at[p, j], ghr.at[p, j], sib).wait_recv()

            @pl.loop(0, rows_z // step)
            def _(i):
                r = pl.ds(pl.multiple_of(i * step, 16), step)
                q = pl.ds(pl.multiple_of(z * rows_z + i * step, 16), step)
                wacc[p, r, :] = buf[p, q, :].astype(F32) + gsr[p, q, :].astype(F32)

            for j in range(1, n):
                base = other_z(j) * rows_z

                @pl.loop(0, rows_z // step)
                def _(i):
                    q = pl.ds(pl.multiple_of(base + i * step, 16), step)
                    buf[p, q, :] = (buf[p, q, :].astype(F32) + gsr[p, q, :].astype(F32)).astype(BF)

            z_send(p, buf)

        @pl.when(s != layer)
        def _():
            for j in range(width // 256):
                rows = pl.ds(j * 256, 256)
                remote(buf.at[p, rows], gsr.at[p, rows], ghs.at[p, j], ghr.at[p, j], sib).wait_send()

    def add_down_grad(k, buf):
        rows = pl.ds(pl.multiple_of((t ^ k) * chunk, chunk), chunk)
        h = hid[0, rows, :]
        for j in range(width // 256):
            cols = slice(j * 256, (j + 1) * 256)
            more = mm(gb[0, rows, cols], h, TN)
            before = jnp.where(k == 0, 0.0, buf[2, cols, :].astype(F32))
            buf[2, cols, :] = (before + more).astype(BF)

            @pl.when(k == 3)
            def _():
                reduce_start(0, 2, j, buf)

    def grad_part(layer, p, buf):
        for j in range(width // 256):
            cols = slice(j * 256, (j + 1) * 256)
            if p == 2:
                buf[p, cols, :] = mm(gb[layer, :, cols], hid[layer], TN).astype(BF)
            elif p == 1:
                buf[p, cols, :] = mm(mn[:, cols], du[...], TN).astype(BF)
            else:
                buf[p, cols, 0:512] = mm(an[:, cols], dqkv[:, 0:512], TN).astype(BF)
                buf[p, cols, 512:768] = (
                    mm(an[:, cols], dqkv[:, 512:768], TN) + mm(gb[layer, :, cols], cb[layer], TN)
                ).astype(BF)
            reduce_start(layer, p, j, buf)

    def hidden_back(layer, c):
        rows = pl.ds(pl.multiple_of(c * chunk, chunk), chunk)
        g = gb[layer, rows, :]
        for j in range(width // 256):
            cols = slice(j * 256, (j + 1) * 256)
            d = mm(g, w[layer, 2, :, cols], NN) * slope[layer, rows, cols].astype(F32)
            sm[layer, 6:7, cols] = sm[layer, 6:7, cols] + jnp.sum(d, axis=0, keepdims=True)
            du[rows, cols] = d.astype(BF)
        d = pltpu.roll(mm(g, w[layer, 0, :, 512:768], NN), HL - 64, 1)
        lane = lane_iota(chunk)
        dc[rows, :] = jnp.where(lane < heads * HEAD_DIM, d, 0.0).astype(BF)

    def zero_sums():
        @pl.loop(0, length // sub)
        def _(i):
            rows = pl.ds(pl.multiple_of(i * sub, sub), sub)
            dk[rows, :] = jnp.zeros((sub, HL), F32)
            dv[rows, :] = jnp.zeros((sub, HL), F32)

    def attend_back(layer, first, last, within=None):
        @pl.loop(first, last)
        def _(b):
            if within is not None:
                pl.when(b == first + 2)(within)

            q0 = pl.multiple_of(b * BQ, BQ)
            k0 = pl.multiple_of(jnp.maximum(b * BQ - SEG_MOST, 0), BQ)
            qm = stack_heads(qb[layer, pl.ds(q0, BQ), :])
            dm = stack_heads(dc[pl.ds(q0, BQ), :])
            ls = lse[layer, b]
            win = pl.ds(k0, BK)
            pscr[...] = mm(kb[layer, win, :], qm, NT)
            dpscr[...] = mm(vb[layer, win, :], dm, NT)
            total = None
            for i in range(BK // BQ):
                irows = slice(i * BQ, (i + 1) * BQ)
                blk = bias[b, irows, :].astype(F32)
                pr = jnp.exp(pscr[irows, :] + jnp.concatenate([blk] * heads, axis=1) - ls)
                pscr[irows, :] = pr
                pbf[irows, :] = pr.astype(BF)
                part = jnp.sum(pr * dpscr[irows, :], axis=0, keepdims=True)
                total = part if total is None else total + part
            dv[win, :] = dv[win, :] + mm(pbf[...], dm, NN)
            for i in range(BK // BQ):
                irows = slice(i * BQ, (i + 1) * BQ)
                dscr[irows, :] = (pscr[irows, :] * (dpscr[irows, :] - total)).astype(BF)
            dk[win, :] = dk[win, :] + mm(dscr[...], qm, NN)
            out = []
            for h in range(heads):
                keys = kt[layer, h * HEAD_DIM : (h + 1) * HEAD_DIM, pl.ds(k0, BK)]
                out.append(mm(keys, dscr[:, h * BQ : (h + 1) * BQ], NN))
            out.append(jnp.zeros((HL - heads * HEAD_DIM, BQ), F32))
            dq[pl.ds(q0, BQ), :] = jnp.concatenate(out, axis=0).T

    def pack_qkv(layer, c):
        rows = pl.ds(pl.multiple_of(c * chunk, chunk), chunk)
        b0 = c * (chunk // BQ)
        lane = lane_iota(chunk)
        gq = rope(dq[rows, :], b0, -1.0) * 0.125
        gk = rope(dk[rows, :], b0, -1.0)
        gv = dv[rows, :]
        sm[layer, 4:5, 0:HL] = sm[layer, 4:5, 0:HL] + jnp.sum(gq, axis=0, keepdims=True)
        sm[layer, 5:6, 0:HL] = sm[layer, 5:6, 0:HL] + jnp.sum(gv, axis=0, keepdims=True)
        rk = pltpu.roll(gk, 192, 1)
        rv = pltpu.roll(gv, 128, 1)
        dqkv[rows, 0:256] = jnp.where(lane < 192, gq, rk).astype(BF)
        dqkv[rows, 256:512] = jnp.where(lane < 128, rk, rv).astype(BF)
        dqkv[rows, 512:768] = jnp.where(lane < 64, rv, 0.0).astype(BF)

    def project_back(layer):
        phase = 3 - layer
        parts_sent(1 if layer == 1 else 2)
        for k in (3, 1, 2, 0):
            rows = pl.ds(pl.multiple_of((t ^ k) * chunk, chunk), chunk)
            pack_qkv(layer, t ^ k)
            da_in = dqkv[rows, :]
            du_in = du[rows, :]
            m = mu[layer, rows, :]
            r = rstd[layer, rows, :]
            for j in range(width // 256):
                cols = slice(j * 256, (j + 1) * 256)
                da = mm(da_in, w[layer, 0, cols, :], NT)
                dm = mm(du_in, w[layer, 1, cols, :], NT)
                unit = (x[layer, rows, cols].astype(F32) - m) * r
                sums = [da * unit, dm * unit, da, dm]
                for i in range(4):
                    sm[layer, i : i + 1, cols] = sm[layer, i : i + 1, cols] + jnp.sum(
                        sums[i], axis=0, keepdims=True
                    )
                e = da * prow(layer, 0, cols) + dm * prow(layer, 1, cols)
                if k:
                    sendb[k - 1, :, cols] = e.astype(BF)
                else:
                    ownp[phase % 2, :, cols] = e
            if k:
                parts_start(phase, k)

    def finish_e(layer):
        phase = 3 - layer
        parts_wait(phase)
        stage = gst.at[1 - layer]
        given = gst.at[0]

        @pl.loop(0, chunk // sub)
        def _(i):
            r = pl.ds(pl.multiple_of(i * sub, sub), sub)
            rows = pl.ds(pl.multiple_of(t * chunk + i * sub, sub), sub)
            e = ownp[phase % 2, r, :]
            for k in range(2):
                e = e + recvb[phase % 2, k, r, :].astype(F32)
            rs = rstd[layer, rows, :]
            unit = (x[layer, rows, :].astype(F32) - mu[layer, rows, :]) * rs
            g = given[r, :]
            if layer == 1:
                sm[1, 7:8, :] = sm[1, 7:8, :] + jnp.sum(g, axis=0, keepdims=True)
            d = rs * (
                e
                - jnp.mean(e, axis=-1, keepdims=True)
                - unit * jnp.mean(e * unit, axis=-1, keepdims=True)
            )
            g = g + d
            stage[r, :] = g
            if layer == 1:
                sm[0, 7:8, :] = sm[0, 7:8, :] + jnp.sum(g, axis=0, keepdims=True)
                gb[0, rows, :] = g.astype(BF)

        if layer == 1:
            gather_start(*ag_g)
        place(layer, stage, out_g, 2 + layer)

    norm_chunk(0, t)
    zero_sums()
    gather_pass(*ag_i)
    lc.wait()
    gb[1, own, :] = gst[0].astype(BF)
    for k in range(1, 4):
        g_copy(k).start()
    first_w_pass(1)

    @pl.loop(1, 4)
    def _(k):
        arrive(*ag_i, k)
        norm_chunk(0, t ^ k)

    first_w(1)

    @pl.loop(0, 4)
    def _(c):
        hidden(0, c)

    first_w_pass(0)
    first_w(0)

    @pl.loop(0, 4)
    def _(c):
        project_in(0, c)

    first_w_pass(2)
    attend(0)
    second_w_send()
    first_w(2)
    project_out(0)
    parts_pass(0)
    second_w_pass(1)
    finish_y(0)

    @pl.loop(0, 4)
    def _(k):
        @pl.when(k == 2)
        def _():
            second_w_pass(2)
            second_w_give(0)

        @pl.when(k == 3)
        def _():
            second_w(0)

            @pl.loop(0, 3)
            def _(m):
                project_in(1, t ^ m)

        arrive(*ag_x, k)
        norm_chunk(1, t ^ k)

        @pl.when(k == 0)
        def _():
            second_w_give(1)
            gather_pass(*ag_x)
            second_w_pass(0)
            second_w(1)

        hidden(1, t ^ k)

    project_in(1, t ^ 3)
    second_w_give(2)
    attend(1)
    second_w(2)
    project_out(1)

    for k in range(1, 4):
        g_arrival(k).wait_recv()
    @pl.loop(0, 4)
    def _(c):
        hidden_back(1, c)

    attend_back(1, 0, nblk, lambda: parts_pass(1))
    project_back(1)
    grad_part(1, 2, gw)
    grad_part(1, 1, gw)
    reduce_cores(1, 2, gw)
    parts_pass(2)
    reduce_cores(1, 1, gw)
    grad_part(1, 0, gw)
    finish_y(1)
    z_pass(1, 2, gw)
    finish_e(1)

    late = w.at[1]
    per = chunk // BQ
    first_w_sent()
    second_w_sent()
    zero_sums()
    reduce_cores(1, 0, gw)

    @pl.loop(0, 8)
    def _(step_no):
        k = jnp.where(step_no < 2, 0, jnp.where(step_no < 5, step_no - 1, step_no - 4))

        @pl.when((step_no == 0) | ((step_no >= 2) & (step_no < 5)))
        def _():
            arrive(*ag_g, k)
            add_down_grad(k, late)
            hidden_back(0, t ^ k)

        @pl.when(step_no == 2)
        def _():
            z_pass(1, 1, gw)

        @pl.when(step_no == 4)
        def _():
            z_pass(1, 0, gw)

        @pl.when(step_no == 6)
        def _():
            reduce_cores(0, 2, late)
            grad_part(0, 1, late)

        @pl.when(step_no == 7)
        def _():
            reduce_cores(0, 1, late)

        @pl.when((step_no == 1) | (step_no >= 5))
        def _():
            attend_back(0, (t ^ k) * per, ((t ^ k) + 1) * per)

        @pl.when(step_no == 1)
        def _():
            gather_pass(*ag_g)
            renorm_all(0)

    z_pass(0, 2, late)
    project_back(0)

    to_sib = remote(sm.at[1 - s], smr, sms.at[0], smrs.at[0], sib)
    to_sib.start()
    grad_part(0, 0, late)
    to_sib.wait()
    smt[...] = sm[s] + smr[...]

    def small_z(j):
        return remote(smt, smz.at[j - 1], sms.at[j], smrs.at[j], (s, other_z(j), t))

    def small_copy(k):
        return remote(tall.at[t], tall.at[t], sms.at[n + k - 1], smrs.at[n + k - 1], plane(k))

    for j in range(1, n):
        small_z(j).start()
    parts_pass(3)
    z_pass(0, 1, late)
    reduce_cores(0, 0, late)

    def matrix_end(p):
        z_end(p, late)
        pltpu.make_async_copy(wacc.at[p], out_w.at[p], lsem.at[p]).start()

    matrix_end(2)
    for j in range(1, n):
        small_z(j).wait()
    total = smt[...]
    for j in range(1, n):
        total = total + smz[j - 1]
    tall[t] = total
    for k in range(1, 4):
        small_copy(k).start()
    z_pass(0, 0, late)
    finish_e(0)
    matrix_end(1)
    for k in range(1, 4):
        small_copy(k).wait_send()
        remote(
            tall.at[t ^ k], tall.at[t ^ k], sms.at[n + k - 1], smrs.at[n + k - 1], plane(k)
        ).wait_recv()
    small_out = pltpu.make_async_copy(tall, out_s, lsem.at[5])
    small_out.start()
    matrix_end(0)
    small_out.wait()

    for p in range(3):
        pltpu.make_async_copy(wacc.at[p], out_w.at[p], lsem.at[p]).wait()
        z_sent(p, late)

    for k in range(1, 4):
        g_copy(k).wait_send()
    for i in range(6):
        gather_copy(*ag_i, i).wait_send()
        gather_copy(*ag_x, i).wait_send()
        gather_copy(*ag_g, i).wait_send()
    parts_sent(3)
    placed(1, yst, out_y, 1)
    placed(1, gst.at[0], out_g, 3)
    placed(0, gst.at[1], out_g, 2)
    remote(yst, out_y.at[1 - s], osend.at[0], orecv.at[0], sib).wait_recv()
    remote(gst.at[0], out_g.at[1 - s], osend.at[0], orecv.at[1], sib).wait_recv()


def write_outputs(
    head_cols, y, g, wg, small, y_out, g_out, up, down, qkv, out, gain, shift, qv, upb, resid,
    buf_a, buf_b, buf_c, sem
):
    halves = [(y.at[i], y_out.at[i]) for i in range(2)] + [(g.at[i], g_out.at[i]) for i in range(2)]
    pairs = halves + [(wg.at[1], up), (wg.at[2], down)]
    held = [buf_a.at[i] for i in range(4)] + [buf_b.at[i] for i in range(2)]
    loads = [pltpu.make_async_copy(p[0], v, sem.at[0, i]) for i, (p, v) in enumerate(zip(pairs, held))]
    copies = [pltpu.make_async_copy(v, p[1], sem.at[1, i]) for i, (p, v) in enumerate(zip(pairs, held))]
    head = pltpu.make_async_copy(wg.at[0], buf_c, sem.at[0, 6])
    head.start()
    for load in loads:
        load.start()
    head.wait()
    first = buf_c[...]
    width = first.shape[1]
    for i in range(3):
        turned = pltpu.roll(first, width - i * head_cols, 1) if i else first
        qkv[i] = turned[:, :head_cols]
    last = pltpu.roll(first, width - 3 * head_cols, 1)[:, :256]
    out[...] = last.T[:head_cols, :]
    for load, copy in zip(loads, copies):
        load.wait()
        copy.start()
    total = small[0] + small[1] + small[2] + small[3]
    gain[...] = total[0:2]
    shift[...] = total[2:4]
    resid[...] = total[7:8]
    spread = small[0]
    upb[:, 0:width] = small[0, 6:7, :]
    for i in range(1, 4):
        spread = spread + pltpu.roll(small[i], i * head_cols, 1)
        upb[:, i * width : (i + 1) * width] = small[i, 6:7, :]
    qv[...] = spread[4:6]
    for copy in copies:
        copy.wait()


def rotary_rows(length, heads):
    rate = np.zeros((HL,), np.float64)
    for h in range(heads):
        for j in range(ROT // 2):
            value = math.exp(j * (-2.0 * math.log(10000.0) / ROT))
            rate[h * HEAD_DIM + j] = value
            rate[h * HEAD_DIM + j + ROT // 2] = value
    live = (np.arange(HL) < heads * HEAD_DIM).astype(np.float64)
    starts = np.arange(length // BQ)[:, None] * BQ * rate[None]
    offsets = np.arange(BQ)[:, None] * rate[None]
    first = np.stack([np.cos(starts), np.sin(starts)])[:, :, None].astype(np.float32)
    second = np.stack([np.cos(offsets) * live, np.sin(offsets) * live]).astype(np.float32)
    return first, second


def body(
    n,
    inputs,
    segment_ids,
    cotangent,
    qkv_weight,
    out_weight,
    up_weight,
    down_weight,
    norm_gain,
    norm_bias,
    qv_bias,
    up_bias,
    resid_bias,
):
    micro, _, chunk, width = inputs.shape
    length = segment_ids.shape[2]
    head_cols = qkv_weight.shape[3]
    rows_z = qkv_weight.shape[2]
    ff_local = up_weight.shape[2]
    heads = head_cols // HEAD_DIM
    assert micro == 2 and length == 4 * chunk and ff_local == width
    assert head_cols == 192 and width == 768

    first, second = rotary_rows(length, heads)

    vm = pl.BlockSpec(memory_space=pltpu.VMEM)
    anywhere = pl.BlockSpec(memory_space=pl.ANY)
    blk = heads * BQ
    nblk = length // BQ
    dma = pltpu.SemaphoreType.DMA

    def vmem(*shape, dtype=BF):
        return pltpu.VMEM(shape, dtype)

    scratch = dict(
        seg_in=vmem(*segment_ids.shape, dtype=jnp.int32),
        qkv_in=vmem(*qkv_weight.shape),
        wo_in=vmem(*out_weight.shape),
        gain_in=vmem(*norm_gain.shape, dtype=F32),
        shift_in=vmem(*norm_bias.shape, dtype=F32),
        qv_in=vmem(*qv_bias.shape, dtype=F32),
        upb_in=vmem(*up_bias.shape, dtype=F32),
        resid_in=vmem(*resid_bias.shape, dtype=F32),
        taba=vmem(*first.shape, dtype=F32),
        tabb=vmem(*second.shape, dtype=F32),
        w=vmem(2, 3, width, width),
        x=vmem(2, length, width),
        an=vmem(length, width),
        mn=vmem(length, width),
        mu=vmem(2, length, 1, dtype=F32),
        rstd=vmem(2, length, 1, dtype=F32),
        qb=vmem(2, length, HL),
        kb=vmem(2, length, HL),
        vb=vmem(2, length, HL),
        kt=vmem(2, heads * HEAD_DIM, length),
        vt=vmem(2, heads * HEAD_DIM, length),
        cb=vmem(2, length, HL),
        lse=vmem(2, nblk, 1, blk, dtype=F32),
        slope=vmem(2, length, width),
        hid=vmem(2, length, width),
        gb=vmem(2, length, width),
        du=vmem(length, width),
        dqkv=vmem(length, width),
        dc=vmem(length, HL),
        dq=vmem(length, HL, dtype=F32),
        dk=vmem(length, HL, dtype=F32),
        dv=vmem(length, HL, dtype=F32),
        bias=vmem(nblk, BK, BQ),
        pscr=vmem(BK, blk, dtype=F32),
        dpscr=vmem(BK, blk, dtype=F32),
        dscr=vmem(BK, blk),
        pbf=vmem(BK, blk),
        sendb=vmem(3, chunk, width),
        recvb=vmem(2, 2, chunk, width),
        relayed=vmem(2, 2, chunk // 2, width),
        ownp=vmem(2, chunk, width, dtype=F32),
        gw=vmem(3, width, width),
        gsr=vmem(3, width, width),
        zrecv=vmem(3, 4, rows_z, width),
        zacc=vmem(3, max(n - 3, 1), rows_z, width),
        wacc=vmem(3, rows_z, width, dtype=F32),
        yst=vmem(chunk, width, dtype=F32),
        gst=vmem(2, chunk, width, dtype=F32),
        segr=vmem(1, length, dtype=F32),
        par=vmem(2, 8, width, dtype=F32),
        sm=vmem(2, 8, width, dtype=F32),
        smr=vmem(8, width, dtype=F32),
        smt=vmem(8, width, dtype=F32),
        smz=vmem(n - 1, 8, width, dtype=F32),
        tall=vmem(4, 8, width, dtype=F32),
        lsem=dma((8,)),
        isem=dma((10,)),
        psem=dma((2,)),
        xs=dma((6,)),
        xr=dma((6,)),
        agx=dma((6,)),
        agxr=dma((6,)),
        agg=dma((6,)),
        aggr=dma((6,)),
        gs=dma((3,)),
        gr=dma((3,)),
        ws=dma((4, 3, n)),
        wr=dma((3, n)),
        fs=dma((3, n)),
        fr=dma((3, n)),
        rss=dma((4, 6)),
        rsr=dma((4, 6)),
        osend=dma((4,)),
        orecv=dma((2,)),
        ghs=dma((3, 3)),
        ghr=dma((3, 3)),
        zs=dma((2, 3, n)),
        zr=dma((3, 4)),
        za=dma((2, 3, n)),
        sms=dma((n + 3,)),
        smrs=dma((n + 3,)),
    )
    out_y, out_g, out_w, out_s = pl.pallas_call(
        functools.partial(kernel, n, heads),
        out_shape=(
            jax.ShapeDtypeStruct((2, chunk, width), F32),
            jax.ShapeDtypeStruct((2, chunk, width), F32),
            jax.ShapeDtypeStruct((3, rows_z, width), F32),
            jax.ShapeDtypeStruct((4, 8, width), F32),
        ),
        in_specs=[anywhere] * 14,
        out_specs=(anywhere,) * 4,
        scratch_shapes=list(scratch.values()),
        compiler_params=pltpu.CompilerParams(
            collective_id=0, has_side_effects=True, vmem_limit_bytes=67043328
        ),
        name="two_layers",
    )(
        inputs.reshape(micro, chunk, width),
        cotangent.reshape(micro, chunk, width),
        segment_ids,
        qkv_weight,
        out_weight,
        up_weight,
        down_weight[0].T,
        norm_gain,
        norm_bias,
        qv_bias,
        up_bias,
        resid_bias,
        jnp.asarray(first),
        jnp.asarray(second),
    )
    shapes = (
        (2, chunk, width),
        (2, chunk, width),
        (rows_z, width),
        (rows_z, width),
        (3, rows_z, head_cols),
        (head_cols, rows_z),
        (2, width),
        (2, width),
        (2, width),
        (1, 4 * width),
        (1, width),
    )
    y, g, up_g, down_g, qkv_g, out_gr, gain_g, shift_g, qv_g, upb_g, resid_g = pl.pallas_call(
        functools.partial(write_outputs, head_cols),
        out_shape=tuple(jax.ShapeDtypeStruct(shape, F32) for shape in shapes),
        in_specs=[anywhere] * 3 + [vm],
        out_specs=(anywhere,) * 4 + (vm,) * 7,
        scratch_shapes=[
            vmem(4, chunk, width, dtype=F32),
            vmem(2, rows_z, width, dtype=F32),
            vmem(rows_z, width, dtype=F32),
            dma((2, 7)),
        ],
        name="outputs",
    )(out_y, out_g, out_w, out_s)
    return (
        y.reshape(1, micro, 1, chunk, width),
        g.reshape(1, micro, 1, chunk, width),
        qkv_g[None],
        out_gr[None],
        up_g[None],
        down_g.T[None],
        gain_g[None],
        shift_g[None],
        qv_g[None],
        upb_g,
        resid_g,
    )


def solution(mesh):
    return jax.shard_map(
        functools.partial(body, mesh.shape["dp"]),
        mesh=mesh,
        in_specs=(
            P(None, "dp", "tensor", None),
            P(None, "dp", None),
            P(None, "dp", "tensor", None),
            P("section", None, "dp", "tensor"),
            P("section", "tensor", "dp"),
            P("section", "dp", "tensor"),
            P("section", "tensor", "dp"),
            P("section", None, None),
            P("section", None, None),
            P("section", None, None),
            P("section", None),
            P("section", None),
        ),
        out_specs=(
            P("section", None, "dp", "tensor", None),
            P("section", None, "dp", "tensor", None),
            P("section", None, "dp", "tensor"),
            P("section", "tensor", "dp"),
            P("section", "dp", "tensor"),
            P("section", "tensor", "dp"),
            P("section", None, None),
            P("section", None, None),
            P("section", None, None),
            P("section", None),
            P("section", None),
        ),
        check_vma=False,
    )
```

```python
import functools
import math

import jax
import jax.numpy as jnp
import numpy as np
from jax import lax
from jax.experimental import pallas as pl
from jax.experimental.pallas import tpu as pltpu
from jax.sharding import PartitionSpec as P

HEAD_DIM = 64
ROT = 16
SEG_MOST = 384
EPS = 1e-05
MASKED = -1e30
ROOT_HALF = 0.7071067811865476
INV_ROOT_TAU = 0.3989422804014327

BF = jnp.bfloat16
F32 = jnp.float32
MESH = pl.DeviceIdType.MESH

NN = (((1,), (0,)), ((), ()))
NT = (((1,), (1,)), ((), ()))
TN = (((0,), (0,)), ((), ()))

BQ = 128
BK = BQ + SEG_MOST
HL = 256
QO, KO, VO, OO = 0, 192, 384, 576


def mm(a, b, dims):
    return lax.dot_general(a, b, dims, preferred_element_type=F32)


def lane_iota(rows, cols=HL):
    return lax.broadcasted_iota(jnp.int32, (rows, cols), 1)


def remote(src, dst, send, recv, dev):
    return pltpu.make_async_remote_copy(
        src_ref=src, dst_ref=dst, send_sem=send, recv_sem=recv, device_id=dev, device_id_type=MESH
    )


def kernel(
    n,
    heads,
    x_in,
    cot_in,
    seg_far,
    qkv_far,
    wo_far,
    up_in,
    down_in,
    gain_far,
    shift_far,
    qv_far,
    upb_far,
    resid_far,
    taba_far,
    tabb_far,
    out_y,
    out_g,
    out_w,
    out_s,
    seg_in,
    qkv_in,
    wo_in,
    gain_in,
    shift_in,
    qv_in,
    upb_in,
    resid_in,
    taba,
    tabb,
    w,
    x,
    an,
    mn,
    mu,
    rstd,
    qb,
    kb,
    vb,
    kt,
    vt,
    cb,
    lse,
    slope,
    hid,
    gb,
    du,
    dqkv,
    dc,
    dq,
    dk,
    dv,
    bias,
    pscr,
    dpscr,
    dscr,
    pbf,
    sendb,
    recvb,
    relayed,
    ownp,
    gw,
    gsr,
    zrecv,
    zacc,
    wacc,
    yst,
    gst,
    segr,
    par,
    sm,
    smr,
    smt,
    smz,
    tall,
    lsem,
    isem,
    psem,
    xs,
    xr,
    agx,
    agxr,
    agg,
    aggr,
    gs,
    gr,
    ws,
    wr,
    fs,
    fr,
    rss,
    rsr,
    osend,
    orecv,
    ghs,
    ghr,
    zs,
    zr,
    za,
    sms,
    smrs,
):
    s = lax.axis_index("section")
    z = lax.axis_index("dp")
    t = lax.axis_index("tensor")
    sib = (1 - s, z, t)
    width = x.shape[2]
    length = x.shape[1]
    chunk = length // 4
    rows_z = up_in.shape[1]
    half = chunk // 2
    nblk = length // BQ
    own = pl.ds(t * chunk, chunk)
    zrows = pl.ds(z * rows_z, rows_z)

    def plane(k):
        return (s, z, t ^ k)

    def other_z(j):
        return lax.rem(z + j, n)

    lx = pltpu.make_async_copy(x_in.at[s], x.at[0, own], lsem.at[0])
    lc = pltpu.make_async_copy(cot_in.at[s], gst.at[0], lsem.at[1])
    lu = pltpu.make_async_copy(up_in.at[0], w.at[s, 1, zrows], lsem.at[3])
    ld = pltpu.make_async_copy(down_in, w.at[s, 2, zrows], lsem.at[4])
    small_loads = [
        pltpu.make_async_copy(src, dst, isem.at[i])
        for i, (src, dst) in enumerate(
            (
                (qkv_far, qkv_in),
                (wo_far, wo_in),
                (gain_far, gain_in),
                (shift_far, shift_in),
                (qv_far, qv_in),
                (upb_far, upb_in),
                (resid_far, resid_in),
                (seg_far, seg_in),
                (taba_far, taba),
                (tabb_far, tabb),
            )
        )
    ]
    lx.start()
    for load in small_loads:
        load.start()
    lu.start()
    ld.start()
    lc.start()

    barrier = pltpu.get_barrier_semaphore()
    pl.semaphore_signal(barrier, inc=1, device_id=sib, device_id_type=MESH)
    for k in range(1, 4):
        pl.semaphore_signal(barrier, inc=1, device_id=plane(k), device_id_type=MESH)
    for j in range(1, n):
        pl.semaphore_signal(barrier, inc=1, device_id=(s, other_z(j), t), device_id_type=MESH)
    pl.semaphore_wait(barrier, 4 + n - 1)

    head_cols = heads * HEAD_DIM

    def picks(first):
        rows = lax.broadcasted_iota(jnp.int32, (head_cols, width), 0)
        cols = lax.broadcasted_iota(jnp.int32, (head_cols, width), 1)
        return (rows + first == cols).astype(F32).astype(BF)

    def pack_share():
        packed = mm(qkv_in[0, 0], picks(QO), NN) + mm(qkv_in[0, 1], picks(KO), NN)
        packed = packed + mm(qkv_in[0, 2], picks(VO), NN) + mm(wo_in[0], picks(OO), TN)
        w[s, 0, zrows, :] = packed.astype(BF)

    def pack_params():
        par[s, 0:2, :] = gain_in[0]
        par[s, 2:4, :] = shift_in[0]
        par[s, 4:6, :] = qv_in[0]
        par[s, 6:7, :] = upb_in[0:1, pl.ds(pl.multiple_of(t * width, 128), width)]
        par[s, 7:8, :] = resid_in[...]
        rows8 = par[s]
        turned = rows8
        for i in range(1, 4):
            turned = jnp.where(t == i, pltpu.roll(rows8, width - i * head_cols, 1), turned)
        row = lax.broadcasted_iota(jnp.int32, (8, width), 0)
        par[s] = jnp.where((row == 4) | (row == 5), turned, rows8)

    def w_rows(origin):
        return pl.ds(origin * rows_z, rows_z)

    def w_step(p, origin, far, src=None):
        rows = w_rows(origin)
        i = {1: 0, 2: 1, -1: 2, -2: 3}[far]
        return remote(
            w.at[s, p, rows] if src is None else src,
            w.at[s, p, rows],
            ws.at[i, p, origin],
            wr.at[p, origin],
            (s, lax.rem(z + far + n, n), t),
        )

    def inside(far):
        return (z + far < n) if far > 0 else (z + far >= 0)

    def w_send(p, src=None):
        for far in (2, -2, 1, -1):

            @pl.when(inside(far))
            def _():
                w_step(p, z, far, src).start()

    def w_arrive(p, passed, then):
        for e in range(2, n, 2) if passed else range(1, n):
            for sign in (1, -1):
                here = inside(-sign * e)
                if passed:
                    here = here & inside(sign)
                elif e % 2 == 0:
                    here = here & jnp.logical_not(inside(sign))

                @pl.when(here)
                def _():
                    origin = lax.rem(z - sign * e + n, n)
                    w_step(p, origin, sign).wait_recv()
                    if passed:
                        for far in (sign, 2 * sign):

                            @pl.when(inside(far))
                            def _():
                                w_step(p, origin, far).start()

                    if then is not None:
                        then(p, origin)

    def w_sent(p):
        for far in (1, -1, 2, -2):

            @pl.when(inside(far))
            def _():
                w_step(p, z, far).wait_send()

            sign = 1 if far > 0 else -1
            for e in range(2, n, 2):

                @pl.when(inside(-sign * e) & inside(far))
                def _():
                    w_step(p, lax.rem(z - sign * e + n, n), far).wait_send()

    def across(p, origin, layer=0):
        part = w.at[layer, p, w_rows(origin)]
        return remote(part, part, fs.at[p, origin], fr.at[p, origin], sib)

    def g_copy(k):
        return remote(gb.at[1, own], gb.at[1, own], gs.at[k - 1], gr.at[k - 1], plane(k))

    def g_arrival(k):
        rows = pl.ds((t ^ k) * chunk, chunk)
        return remote(gb.at[1, rows], gb.at[1, rows], gs.at[k - 1], gr.at[k - 1], plane(k))

    hops = ((0, 0, 1), (0, 1, 2), (0, 1, 1), (0, 0, 2), (1, 0, 2), (2, 1, 1))

    def gather_copy(buf, send, recv, i):
        k, h, to = hops[i]
        rows = pl.ds((t ^ k) * chunk + h * half, half)
        return remote(buf.at[rows], buf.at[rows], send.at[i], recv.at[i], plane(to))

    def gather_arrival(buf, send, recv, i):
        k, h, to = hops[i]
        rows = pl.ds((t ^ k ^ to) * chunk + h * half, half)
        return remote(buf.at[rows], buf.at[rows], send.at[i], recv.at[i], plane(to))

    def gather_start(buf, send, recv):
        for i in range(4):
            gather_copy(buf, send, recv, i).start()

    def gather_pass(buf, send, recv):
        gather_arrival(buf, send, recv, 0).wait_recv()
        gather_copy(buf, send, recv, 4).start()
        gather_arrival(buf, send, recv, 1).wait_recv()
        gather_copy(buf, send, recv, 5).start()

    def gather_wait(buf, send, recv, k):
        for i in {1: (2,), 2: (3,), 3: (4, 5)}[k]:
            gather_arrival(buf, send, recv, i).wait_recv()

    def arrive(buf, send, recv, k):
        for i in range(1, 4):

            @pl.when(k == i)
            def _():
                gather_wait(buf, send, recv, i)

    def part_copy(phase, i):
        low, high = pl.ds(0, half), pl.ds(half, half)
        bank = phase % 2
        src, dst, to = (
            (sendb.at[2, low], relayed.at[bank, 0], 1),
            (sendb.at[2, high], relayed.at[bank, 1], 2),
            (sendb.at[0, low], recvb.at[bank, 0, low], 1),
            (sendb.at[1, high], recvb.at[bank, 1, high], 2),
            (sendb.at[1, low], recvb.at[bank, 1, low], 2),
            (sendb.at[0, high], recvb.at[bank, 0, high], 1),
        )[i]
        return remote(src, dst, rss.at[phase, i], rsr.at[phase, i], plane(to))

    def parts_start(phase, k):
        for i in {3: (0, 1), 1: (2,), 2: (3,)}[k]:
            part_copy(phase, i).start()

    def parts_pass(phase):
        for i in range(2):
            part_copy(phase, i).wait_recv()
            rows = slice(i * half, (i + 1) * half)
            mine = sendb[1 - i, rows, :].astype(F32)
            sendb[1 - i, rows, :] = (mine + relayed[phase % 2, i].astype(F32)).astype(BF)
            part_copy(phase, 4 + i).start()

    def parts_sent(phase):
        for i in range(6):
            part_copy(phase, i).wait_send()

    def parts_wait(phase):
        for i in range(2, 6):
            part_copy(phase, i).wait_recv()

    ag_i = (x.at[0], xs, xr)
    ag_x = (x.at[1], agx, agxr)
    ag_g = (gb.at[0], agg, aggr)

    @pl.when(s == 0)
    def _():
        w_send(1, up_in.at[0])

    lx.wait()
    gather_start(*ag_i)
    for load in small_loads:
        load.wait()
    pack_share()

    @pl.when(s == 0)
    def _():
        w_send(0)
        w_send(2, down_in)

    pack_params()
    par_copy = remote(par.at[s], par.at[s], psem.at[0], psem.at[1], sib)
    par_copy.start()
    lu.wait()
    ld.wait()

    @pl.when(s == 0)
    def _():
        for p in (1, 0, 2):
            across(p, z).start()

    for i in range(length // BQ):
        cols = slice(i * BQ, (i + 1) * BQ)
        ids = jnp.where(s == 0, seg_in[0, :, cols], seg_in[1, :, cols]).astype(F32)
        segr[:, cols] = ids
        dq[cols, 0:BQ] = jnp.broadcast_to(ids, (BQ, BQ)).T

    @pl.loop(0, nblk)
    def _(b):
        q0 = pl.multiple_of(b * BQ, BQ)
        k0 = pl.multiple_of(jnp.maximum(b * BQ - SEG_MOST, 0), BQ)
        seg_k = dq[pl.ds(k0, BK), 0:BQ]
        seg_q = segr[:, pl.ds(q0, BQ)]
        kpos = lax.broadcasted_iota(jnp.int32, (BK, BQ), 0) + k0
        qpos = lax.broadcasted_iota(jnp.int32, (BK, BQ), 1) + q0
        allowed = (seg_k == seg_q) & (kpos <= qpos)
        bias[b] = jnp.where(allowed, 0.0, MASKED).astype(BF)

    par_wait = remote(par.at[1 - s], par.at[1 - s], psem.at[0], psem.at[1], sib)
    par_copy.wait_send()
    par_wait.wait_recv()

    @pl.loop(0, 2)
    def _(i):
        sm[i] = jnp.zeros((8, width), F32)

    def first_w_pass(p):
        @pl.when(s == 0)
        def _():
            w_arrive(p, True, lambda p, origin: across(p, origin).start())

    def first_w(p):
        @pl.when(s == 0)
        def _():
            w_arrive(p, False, lambda p, origin: across(p, origin).start())

        @pl.when(s == 1)
        def _():
            for origin in range(n):
                across(p, origin).wait_recv()

    def first_w_sent():
        @pl.when(s == 0)
        def _():
            for p in range(3):
                w_sent(p)
                for origin in range(n):
                    across(p, origin).wait_send()

    def second_w_send():
        @pl.when(s == 1)
        def _():
            w_send(1, up_in.at[0])
            w_send(0)
            w_send(2, down_in)
            for p in (1, 0, 2):
                across(p, z, 1).start()

    def second_w_pass(p):
        @pl.when(s == 1)
        def _():
            w_arrive(p, True, lambda p, origin: across(p, origin, 1).start())

    def second_w_give(p):
        @pl.when(s == 1)
        def _():
            w_arrive(p, False, lambda p, origin: across(p, origin, 1).start())

    def second_w(p):
        @pl.when(s == 0)
        def _():
            for origin in range(n):
                across(p, origin, 1).wait_recv()

    def second_w_sent():
        @pl.when(s == 1)
        def _():
            for p in range(3):
                w_sent(p)
                for origin in range(n):
                    across(p, origin, 1).wait_send()

    def prow(layer, r, cols=None):
        if cols is None:
            return par[layer, r : r + 1, :]
        return par[layer, r : r + 1, cols]

    def rope_tables(b, sign):
        ca = taba[0, b]
        sa = taba[1, b]
        c0 = tabb[0]
        s0 = tabb[1]
        cos = ca * c0 - sa * s0
        sin = sa * c0 + ca * s0
        lane = lane_iota(BQ) & (HEAD_DIM - 1)
        return cos, jnp.where(lane < ROT // 2, -sign, sign) * sin

    def rope(u, b, sign):
        halves = []
        lane = lane_iota(BQ) & (HEAD_DIM - 1)
        for i in range(u.shape[0] // BQ):
            part = u[i * BQ : (i + 1) * BQ]
            cos, sin = rope_tables(b + i, sign)
            partner = jnp.where(
                lane < ROT // 2,
                pltpu.roll(part, HL - ROT // 2, 1),
                pltpu.roll(part, ROT // 2, 1),
            )
            halves.append(part * cos + partner * sin)
        return jnp.concatenate(halves, axis=0)

    def stack_heads(block):
        lane = lane_iota(BQ) >> 6
        return jnp.concatenate(
            [jnp.where(lane == h, block, jnp.zeros_like(block)) for h in range(heads)], axis=0
        )

    sub = 64

    def norm_chunk(layer, c):
        @pl.loop(0, chunk // sub)
        def _(i):
            rows = pl.ds(pl.multiple_of(c * chunk + i * sub, sub), sub)
            v = x[layer, rows, :].astype(F32)
            m = jnp.mean(v, axis=-1, keepdims=True)
            v = v - m
            r = lax.rsqrt(jnp.mean(v * v, axis=-1, keepdims=True) + EPS)
            mu[layer, rows, :] = m
            rstd[layer, rows, :] = r
            v = v * r
            an[rows, :] = (v * prow(layer, 0) + prow(layer, 2)).astype(BF)
            mn[rows, :] = (v * prow(layer, 1) + prow(layer, 3)).astype(BF)

    def renorm_all(layer):
        @pl.loop(0, length // sub)
        def _(i):
            rows = pl.ds(pl.multiple_of(i * sub, sub), sub)
            v = (x[layer, rows, :].astype(F32) - mu[layer, rows, :]) * rstd[layer, rows, :]
            an[rows, :] = (v * prow(layer, 0) + prow(layer, 2)).astype(BF)
            mn[rows, :] = (v * prow(layer, 1) + prow(layer, 3)).astype(BF)

    def project_in(layer, c):
        rows = pl.ds(pl.multiple_of(c * chunk, chunk), chunk)
        a = an[rows, :]
        b0 = c * (chunk // BQ)
        lane = lane_iota(chunk)
        u = mm(a, w[layer, 0, :, QO : QO + HL], NN) + prow(layer, 4, slice(0, HL))
        qb[layer, rows, :] = (rope(u, b0, 1.0) * 0.125).astype(BF)
        u = mm(a, w[layer, 0, :, KO - 64 : KO - 64 + HL], NN)
        u = rope(pltpu.roll(u, HL - 64, 1), b0, 1.0)
        kb[layer, rows, :] = u.astype(BF)
        kt[layer, :, rows] = u.T[: heads * HEAD_DIM].astype(BF)
        u = mm(a, w[layer, 0, :, VO : VO + HL], NN) + prow(layer, 5, slice(0, HL))
        u = jnp.where(lane < heads * HEAD_DIM, u, 0.0)
        vb[layer, rows, :] = u.astype(BF)
        vt[layer, :, rows] = u.T[: heads * HEAD_DIM].astype(BF)

    def attend(layer, within=None):
        @pl.loop(0, nblk)
        def _(b):
            if within is not None:
                pl.when(b == nblk // 2)(within)

            q0 = pl.multiple_of(b * BQ, BQ)
            k0 = pl.multiple_of(jnp.maximum(b * BQ - SEG_MOST, 0), BQ)
            qm = stack_heads(qb[layer, pl.ds(q0, BQ), :])
            pscr[...] = mm(kb[layer, pl.ds(k0, BK), :], qm, NT)
            top = None
            for i in range(BK // BQ):
                irows = slice(i * BQ, (i + 1) * BQ)
                blk = bias[b, irows, :].astype(F32)
                sc = pscr[irows, :] + jnp.concatenate([blk] * heads, axis=1)
                pscr[irows, :] = sc
                peak = jnp.max(sc, axis=0, keepdims=True)
                top = peak if top is None else jnp.maximum(top, peak)
            total = None
            for i in range(BK // BQ):
                e = jnp.exp(pscr[i * BQ : (i + 1) * BQ, :] - top)
                pscr[i * BQ : (i + 1) * BQ, :] = e
                part = jnp.sum(e, axis=0, keepdims=True)
                total = part if total is None else total + part
            lse[layer, b] = top + jnp.log(total)
            inv = 1.0 / total
            ctx = [jnp.zeros((HL - heads * HEAD_DIM, BQ), F32)]
            for h in range(heads):
                cols = slice(h * BQ, (h + 1) * BQ)
                ph = (pscr[:, cols] * inv[:, cols]).astype(BF)
                vals = vt[layer, h * HEAD_DIM : (h + 1) * HEAD_DIM, pl.ds(k0, BK)]
                ctx.append(mm(vals, ph, NN))
            cb[layer, pl.ds(q0, BQ), :] = jnp.concatenate(ctx, axis=0).T.astype(BF)

    def hidden(layer, c):
        rows = pl.ds(pl.multiple_of(c * chunk, chunk), chunk)
        a = mn[rows, :]
        for j in range(width // 256):
            cols = slice(j * 256, (j + 1) * 256)
            u = mm(a, w[layer, 1, :, cols], NN) + prow(layer, 6, cols)
            phi = 0.5 * (1.0 + lax.erf(u * ROOT_HALF))
            hid[layer, rows, cols] = (u * phi).astype(BF)
            slope[layer, rows, cols] = (phi + u * INV_ROOT_TAU * jnp.exp(-0.5 * u * u)).astype(BF)

    def project_out(layer):
        phase = layer
        if layer == 1:
            parts_sent(0)
        for k in (3, 1, 2, 0):
            rows = pl.ds(pl.multiple_of((t ^ k) * chunk, chunk), chunk)
            c = cb[layer, rows, :]
            h = hid[layer, rows, :]
            for j in range(width // 256):
                cols = slice(j * 256, (j + 1) * 256)
                y = mm(c, w[layer, 0, cols, 512:768], NT) + mm(h, w[layer, 2, cols, :], NT)
                if k:
                    sendb[k - 1, :, cols] = y.astype(BF)
                else:
                    ownp[phase % 2, :, cols] = y
            if k:
                parts_start(phase, k)

    def place(layer, stage, out, idx):
        @pl.when(s == layer)
        def _():
            pltpu.make_async_copy(stage, out.at[s], osend.at[idx]).start()

        @pl.when(s != layer)
        def _():
            remote(stage, out.at[s], osend.at[idx], orecv.at[idx // 2], sib).start()

    def placed(layer, stage, out, idx):
        @pl.when(s == layer)
        def _():
            pltpu.make_async_copy(stage, out.at[s], osend.at[idx]).wait()

        @pl.when(s != layer)
        def _():
            remote(stage, out.at[s], osend.at[idx], orecv.at[idx // 2], sib).wait_send()

    def finish_y(layer):
        phase = layer
        parts_wait(phase)
        if layer == 1:
            placed(0, yst, out_y, 0)

        @pl.loop(0, chunk // sub)
        def _(i):
            r = pl.ds(pl.multiple_of(i * sub, sub), sub)
            rows = pl.ds(pl.multiple_of(t * chunk + i * sub, sub), sub)
            y = x[layer, rows, :].astype(F32) + ownp[phase % 2, r, :] + prow(layer, 7)
            for k in range(2):
                y = y + recvb[phase % 2, k, r, :].astype(F32)
            yst[r, :] = y
            if layer == 0:
                x[1, rows, :] = y.astype(BF)

        if layer == 0:
            gather_start(*ag_x)
        place(layer, yst, out_y, layer)

    def reduce_start(layer, p, j, buf):
        rows = pl.ds(j * 256, 256)


        @pl.when(s != layer)
        def _():
            remote(buf.at[p, rows], gsr.at[p, rows], ghs.at[p, j], ghr.at[p, j], sib).start()

    def z_item(p, e, sign, buf):
        dest = lax.rem(z + sign * e + n, n)
        way = 0 if sign > 0 else 1
        if e <= 2:
            slot = 2 * way + e - 1
            dst, recv, far = zrecv.at[p, slot], zr.at[p, slot], e
        else:
            place_no = e - 3 if sign > 0 else n - z + e - 4
            dst, recv, far = zacc.at[p, place_no], za.at[way, p, e - 3], 1
        return remote(
            buf.at[p, w_rows(dest)],
            dst,
            zs.at[way, p, e - 1],
            recv,
            (s, lax.rem(z + sign * far + n, n), t),
        )

    def first_of(sign):
        return (z == 0) if sign > 0 else (z == n - 1)

    def z_send(p, buf):
        for e in range(n - 1, 0, -1):
            for sign in (1, -1):
                go = inside(sign * e)
                if e > 1:
                    go = go & first_of(sign)

                @pl.when(go)
                def _():
                    z_item(p, e, sign, buf).start()

    def z_pass(layer, p, buf):
        @pl.when(s == layer)
        def _():
            for e in range(n - 2, 1, -1):
                for sign in (1, -1):

                    @pl.when(inside(sign * e) & inside(-sign))
                    def _():
                        way = 0 if sign > 0 else 1
                        place_no = e - 2 if sign > 0 else n - z + e - 4
                        got = zacc.at[p, place_no]
                        remote(got, got, zs.at[way, p, e - 1], za.at[way, p, e - 2], sib).wait_recv()
                        base = lax.rem(z + sign * e + n, n) * rows_z

                        @pl.loop(0, rows_z // step)
                        def _(i):
                            r = pl.ds(pl.multiple_of(i * step, 16), step)
                            q = pl.ds(pl.multiple_of(base + i * step, 16), step)
                            more = zacc[p, place_no, r, :].astype(F32)
                            buf[p, q, :] = (buf[p, q, :].astype(F32) + more).astype(BF)

                        z_item(p, e, sign, buf).start()

    def z_end(p, buf):
        for slot in range(4):
            sign = 1 if slot < 2 else -1
            e = slot % 2 + 1

            @pl.when(inside(-sign * e))
            def _():
                got = zrecv.at[p, slot]
                remote(got, got, zs.at[0, p, 0], zr.at[p, slot], sib).wait_recv()

                @pl.loop(0, rows_z // step)
                def _(i):
                    r = pl.ds(pl.multiple_of(i * step, 16), step)
                    wacc[p, r, :] = wacc[p, r, :] + zrecv[p, slot, r, :].astype(F32)

    def z_sent(p, buf):
        for e in range(1, n):
            for sign in (1, -1):

                @pl.when(inside(sign * e))
                def _():
                    z_item(p, e, sign, buf).wait_send()

    step = 48

    def reduce_cores(layer, p, buf):
        @pl.when(s == layer)
        def _():
            for j in range(width // 256):
                rows = pl.ds(j * 256, 256)
                remote(buf.at[p, rows], gsr.at[p, rows], ghs.at[p, j], ghr.at[p, j], sib).wait_recv()

            @pl.loop(0, rows_z // step)
            def _(i):
                r = pl.ds(pl.multiple_of(i * step, 16), step)
                q = pl.ds(pl.multiple_of(z * rows_z + i * step, 16), step)
                wacc[p, r, :] = buf[p, q, :].astype(F32) + gsr[p, q, :].astype(F32)

            for j in range(1, n):
                base = other_z(j) * rows_z

                @pl.loop(0, rows_z // step)
                def _(i):
                    q = pl.ds(pl.multiple_of(base + i * step, 16), step)
                    buf[p, q, :] = (buf[p, q, :].astype(F32) + gsr[p, q, :].astype(F32)).astype(BF)

            z_send(p, buf)

        @pl.when(s != layer)
        def _():
            for j in range(width // 256):
                rows = pl.ds(j * 256, 256)
                remote(buf.at[p, rows], gsr.at[p, rows], ghs.at[p, j], ghr.at[p, j], sib).wait_send()

    def add_down_grad(k, buf):
        rows = pl.ds(pl.multiple_of((t ^ k) * chunk, chunk), chunk)
        h = hid[0, rows, :]
        for j in range(width // 256):
            cols = slice(j * 256, (j + 1) * 256)
            more = mm(gb[0, rows, cols], h, TN)
            before = jnp.where(k == 0, 0.0, buf[2, cols, :].astype(F32))
            buf[2, cols, :] = (before + more).astype(BF)

            @pl.when(k == 3)
            def _():
                reduce_start(0, 2, j, buf)

    def grad_part(layer, p, buf):
        for j in range(width // 256):
            cols = slice(j * 256, (j + 1) * 256)
            if p == 2:
                buf[p, cols, :] = mm(gb[layer, :, cols], hid[layer], TN).astype(BF)
            elif p == 1:
                buf[p, cols, :] = mm(mn[:, cols], du[...], TN).astype(BF)
            else:
                buf[p, cols, 0:512] = mm(an[:, cols], dqkv[:, 0:512], TN).astype(BF)
                buf[p, cols, 512:768] = (
                    mm(an[:, cols], dqkv[:, 512:768], TN) + mm(gb[layer, :, cols], cb[layer], TN)
                ).astype(BF)
            reduce_start(layer, p, j, buf)

    def hidden_back(layer, c):
        rows = pl.ds(pl.multiple_of(c * chunk, chunk), chunk)
        g = gb[layer, rows, :]
        for j in range(width // 256):
            cols = slice(j * 256, (j + 1) * 256)
            d = mm(g, w[layer, 2, :, cols], NN) * slope[layer, rows, cols].astype(F32)
            sm[layer, 6:7, cols] = sm[layer, 6:7, cols] + jnp.sum(d, axis=0, keepdims=True)
            du[rows, cols] = d.astype(BF)
        d = pltpu.roll(mm(g, w[layer, 0, :, 512:768], NN), HL - 64, 1)
        lane = lane_iota(chunk)
        dc[rows, :] = jnp.where(lane < heads * HEAD_DIM, d, 0.0).astype(BF)

    def zero_sums():
        @pl.loop(0, length // sub)
        def _(i):
            rows = pl.ds(pl.multiple_of(i * sub, sub), sub)
            dk[rows, :] = jnp.zeros((sub, HL), F32)
            dv[rows, :] = jnp.zeros((sub, HL), F32)

    def attend_back(layer, first, last, within=None):
        @pl.loop(first, last)
        def _(b):
            if within is not None:
                pl.when(b == first + 2)(within)

            q0 = pl.multiple_of(b * BQ, BQ)
            k0 = pl.multiple_of(jnp.maximum(b * BQ - SEG_MOST, 0), BQ)
            qm = stack_heads(qb[layer, pl.ds(q0, BQ), :])
            dm = stack_heads(dc[pl.ds(q0, BQ), :])
            ls = lse[layer, b]
            win = pl.ds(k0, BK)
            pscr[...] = mm(kb[layer, win, :], qm, NT)
            dpscr[...] = mm(vb[layer, win, :], dm, NT)
            total = None
            for i in range(BK // BQ):
                irows = slice(i * BQ, (i + 1) * BQ)
                blk = bias[b, irows, :].astype(F32)
                pr = jnp.exp(pscr[irows, :] + jnp.concatenate([blk] * heads, axis=1) - ls)
                pscr[irows, :] = pr
                pbf[irows, :] = pr.astype(BF)
                part = jnp.sum(pr * dpscr[irows, :], axis=0, keepdims=True)
                total = part if total is None else total + part
            dv[win, :] = dv[win, :] + mm(pbf[...], dm, NN)
            for i in range(BK // BQ):
                irows = slice(i * BQ, (i + 1) * BQ)
                dscr[irows, :] = (pscr[irows, :] * (dpscr[irows, :] - total)).astype(BF)
            dk[win, :] = dk[win, :] + mm(dscr[...], qm, NN)
            out = []
            for h in range(heads):
                keys = kt[layer, h * HEAD_DIM : (h + 1) * HEAD_DIM, pl.ds(k0, BK)]
                out.append(mm(keys, dscr[:, h * BQ : (h + 1) * BQ], NN))
            out.append(jnp.zeros((HL - heads * HEAD_DIM, BQ), F32))
            dq[pl.ds(q0, BQ), :] = jnp.concatenate(out, axis=0).T

    def pack_qkv(layer, c):
        rows = pl.ds(pl.multiple_of(c * chunk, chunk), chunk)
        b0 = c * (chunk // BQ)
        lane = lane_iota(chunk)
        gq = rope(dq[rows, :], b0, -1.0) * 0.125
        gk = rope(dk[rows, :], b0, -1.0)
        gv = dv[rows, :]
        sm[layer, 4:5, 0:HL] = sm[layer, 4:5, 0:HL] + jnp.sum(gq, axis=0, keepdims=True)
        sm[layer, 5:6, 0:HL] = sm[layer, 5:6, 0:HL] + jnp.sum(gv, axis=0, keepdims=True)
        rk = pltpu.roll(gk, 192, 1)
        rv = pltpu.roll(gv, 128, 1)
        dqkv[rows, 0:256] = jnp.where(lane < 192, gq, rk).astype(BF)
        dqkv[rows, 256:512] = jnp.where(lane < 128, rk, rv).astype(BF)
        dqkv[rows, 512:768] = jnp.where(lane < 64, rv, 0.0).astype(BF)

    def project_back(layer):
        phase = 3 - layer
        parts_sent(1 if layer == 1 else 2)
        for k in (3, 1, 2, 0):
            rows = pl.ds(pl.multiple_of((t ^ k) * chunk, chunk), chunk)
            pack_qkv(layer, t ^ k)
            da_in = dqkv[rows, :]
            du_in = du[rows, :]
            m = mu[layer, rows, :]
            r = rstd[layer, rows, :]
            for j in range(width // 256):
                cols = slice(j * 256, (j + 1) * 256)
                da = mm(da_in, w[layer, 0, cols, :], NT)
                dm = mm(du_in, w[layer, 1, cols, :], NT)
                unit = (x[layer, rows, cols].astype(F32) - m) * r
                sums = [da * unit, dm * unit, da, dm]
                for i in range(4):
                    sm[layer, i : i + 1, cols] = sm[layer, i : i + 1, cols] + jnp.sum(
                        sums[i], axis=0, keepdims=True
                    )
                e = da * prow(layer, 0, cols) + dm * prow(layer, 1, cols)
                if k:
                    sendb[k - 1, :, cols] = e.astype(BF)
                else:
                    ownp[phase % 2, :, cols] = e
            if k:
                parts_start(phase, k)

    def finish_e(layer):
        phase = 3 - layer
        parts_wait(phase)
        stage = gst.at[1 - layer]
        given = gst.at[0]

        @pl.loop(0, chunk // sub)
        def _(i):
            r = pl.ds(pl.multiple_of(i * sub, sub), sub)
            rows = pl.ds(pl.multiple_of(t * chunk + i * sub, sub), sub)
            e = ownp[phase % 2, r, :]
            for k in range(2):
                e = e + recvb[phase % 2, k, r, :].astype(F32)
            rs = rstd[layer, rows, :]
            unit = (x[layer, rows, :].astype(F32) - mu[layer, rows, :]) * rs
            g = given[r, :]
            if layer == 1:
                sm[1, 7:8, :] = sm[1, 7:8, :] + jnp.sum(g, axis=0, keepdims=True)
            d = rs * (
                e
                - jnp.mean(e, axis=-1, keepdims=True)
                - unit * jnp.mean(e * unit, axis=-1, keepdims=True)
            )
            g = g + d
            stage[r, :] = g
            if layer == 1:
                sm[0, 7:8, :] = sm[0, 7:8, :] + jnp.sum(g, axis=0, keepdims=True)
                gb[0, rows, :] = g.astype(BF)

        if layer == 1:
            gather_start(*ag_g)
        place(layer, stage, out_g, 2 + layer)

    norm_chunk(0, t)
    zero_sums()
    gather_pass(*ag_i)
    lc.wait()
    gb[1, own, :] = gst[0].astype(BF)
    for k in range(1, 4):
        g_copy(k).start()
    first_w_pass(1)

    @pl.loop(1, 4)
    def _(k):
        arrive(*ag_i, k)
        norm_chunk(0, t ^ k)

    first_w(1)

    @pl.loop(0, 4)
    def _(c):
        hidden(0, c)

    first_w_pass(0)
    first_w(0)

    @pl.loop(0, 4)
    def _(c):
        project_in(0, c)

    first_w_pass(2)
    attend(0)
    second_w_send()
    first_w(2)
    project_out(0)
    parts_pass(0)
    second_w_pass(1)
    second_w_pass(0)
    finish_y(0)

    @pl.loop(0, 4)
    def _(k):
        @pl.when(k == 2)
        def _():
            second_w_give(0)

        @pl.when(k == 3)
        def _():
            second_w(0)

            @pl.loop(0, 3)
            def _(m):
                project_in(1, t ^ m)

        arrive(*ag_x, k)
        norm_chunk(1, t ^ k)

        @pl.when(k == 0)
        def _():
            second_w_give(1)
            gather_pass(*ag_x)
            second_w_pass(2)
            second_w(1)

        hidden(1, t ^ k)

    project_in(1, t ^ 3)
    second_w_give(2)
    attend(1)
    second_w(2)
    project_out(1)

    for k in range(1, 4):
        g_arrival(k).wait_recv()
    @pl.loop(0, 4)
    def _(c):
        hidden_back(1, c)

    attend_back(1, 0, nblk, lambda: parts_pass(1))
    project_back(1)
    grad_part(1, 2, gw)
    grad_part(1, 1, gw)
    reduce_cores(1, 2, gw)
    parts_pass(2)
    reduce_cores(1, 1, gw)
    grad_part(1, 0, gw)
    finish_y(1)
    z_pass(1, 2, gw)
    finish_e(1)

    late = w.at[1]
    per = chunk // BQ
    first_w_sent()
    second_w_sent()
    zero_sums()
    reduce_cores(1, 0, gw)

    @pl.loop(0, 8)
    def _(step_no):
        k = jnp.where(step_no < 2, 0, jnp.where(step_no < 5, step_no - 1, step_no - 4))

        @pl.when((step_no == 0) | ((step_no >= 2) & (step_no < 5)))
        def _():
            arrive(*ag_g, k)
            add_down_grad(k, late)
            hidden_back(0, t ^ k)

        @pl.when(step_no == 2)
        def _():
            z_pass(1, 1, gw)

        @pl.when(step_no == 4)
        def _():
            z_pass(1, 0, gw)

        @pl.when(step_no == 6)
        def _():
            reduce_cores(0, 2, late)
            grad_part(0, 1, late)

        @pl.when(step_no == 7)
        def _():
            reduce_cores(0, 1, late)

        @pl.when((step_no == 1) | (step_no >= 5))
        def _():
            attend_back(0, (t ^ k) * per, ((t ^ k) + 1) * per)

        @pl.when(step_no == 1)
        def _():
            gather_pass(*ag_g)
            renorm_all(0)

    z_pass(0, 2, late)
    project_back(0)

    to_sib = remote(sm.at[1 - s], smr, sms.at[0], smrs.at[0], sib)
    to_sib.start()
    grad_part(0, 0, late)
    to_sib.wait()
    smt[...] = sm[s] + smr[...]

    def small_z(j):
        return remote(smt, smz.at[j - 1], sms.at[j], smrs.at[j], (s, other_z(j), t))

    def small_copy(k):
        return remote(tall.at[t], tall.at[t], sms.at[n + k - 1], smrs.at[n + k - 1], plane(k))

    for j in range(1, n):
        small_z(j).start()
    parts_pass(3)
    z_pass(0, 1, late)
    reduce_cores(0, 0, late)

    def matrix_end(p):
        z_end(p, late)
        pltpu.make_async_copy(wacc.at[p], out_w.at[p], lsem.at[p]).start()

    matrix_end(2)
    for j in range(1, n):
        small_z(j).wait()
    total = smt[...]
    for j in range(1, n):
        total = total + smz[j - 1]
    tall[t] = total
    for k in range(1, 4):
        small_copy(k).start()
    z_pass(0, 0, late)
    finish_e(0)
    matrix_end(1)
    for k in range(1, 4):
        small_copy(k).wait_send()
        remote(
            tall.at[t ^ k], tall.at[t ^ k], sms.at[n + k - 1], smrs.at[n + k - 1], plane(k)
        ).wait_recv()
    small_out = pltpu.make_async_copy(tall, out_s, lsem.at[5])
    small_out.start()
    matrix_end(0)
    small_out.wait()

    for p in range(3):
        pltpu.make_async_copy(wacc.at[p], out_w.at[p], lsem.at[p]).wait()
        z_sent(p, late)

    for k in range(1, 4):
        g_copy(k).wait_send()
    for i in range(6):
        gather_copy(*ag_i, i).wait_send()
        gather_copy(*ag_x, i).wait_send()
        gather_copy(*ag_g, i).wait_send()
    parts_sent(3)
    placed(1, yst, out_y, 1)
    placed(1, gst.at[0], out_g, 3)
    placed(0, gst.at[1], out_g, 2)
    remote(yst, out_y.at[1 - s], osend.at[0], orecv.at[0], sib).wait_recv()
    remote(gst.at[0], out_g.at[1 - s], osend.at[0], orecv.at[1], sib).wait_recv()


def write_outputs(
    head_cols, y, g, wg, small, y_out, g_out, up, down, qkv, out, gain, shift, qv, upb, resid,
    buf_a, buf_b, buf_c, sem
):
    halves = [(y.at[i], y_out.at[i]) for i in range(2)] + [(g.at[i], g_out.at[i]) for i in range(2)]
    pairs = halves + [(wg.at[1], up), (wg.at[2], down)]
    held = [buf_a.at[i] for i in range(4)] + [buf_b.at[i] for i in range(2)]
    loads = [pltpu.make_async_copy(p[0], v, sem.at[0, i]) for i, (p, v) in enumerate(zip(pairs, held))]
    copies = [pltpu.make_async_copy(v, p[1], sem.at[1, i]) for i, (p, v) in enumerate(zip(pairs, held))]
    head = pltpu.make_async_copy(wg.at[0], buf_c, sem.at[0, 6])
    head.start()
    for load in loads:
        load.start()
    head.wait()
    first = buf_c[...]
    width = first.shape[1]
    for i in range(3):
        turned = pltpu.roll(first, width - i * head_cols, 1) if i else first
        qkv[i] = turned[:, :head_cols]
    last = pltpu.roll(first, width - 3 * head_cols, 1)[:, :256]
    out[...] = last.T[:head_cols, :]
    for load, copy in zip(loads, copies):
        load.wait()
        copy.start()
    total = small[0] + small[1] + small[2] + small[3]
    gain[...] = total[0:2]
    shift[...] = total[2:4]
    resid[...] = total[7:8]
    spread = small[0]
    upb[:, 0:width] = small[0, 6:7, :]
    for i in range(1, 4):
        spread = spread + pltpu.roll(small[i], i * head_cols, 1)
        upb[:, i * width : (i + 1) * width] = small[i, 6:7, :]
    qv[...] = spread[4:6]
    for copy in copies:
        copy.wait()


def rotary_rows(length, heads):
    rate = np.zeros((HL,), np.float64)
    for h in range(heads):
        for j in range(ROT // 2):
            value = math.exp(j * (-2.0 * math.log(10000.0) / ROT))
            rate[h * HEAD_DIM + j] = value
            rate[h * HEAD_DIM + j + ROT // 2] = value
    live = (np.arange(HL) < heads * HEAD_DIM).astype(np.float64)
    starts = np.arange(length // BQ)[:, None] * BQ * rate[None]
    offsets = np.arange(BQ)[:, None] * rate[None]
    first = np.stack([np.cos(starts), np.sin(starts)])[:, :, None].astype(np.float32)
    second = np.stack([np.cos(offsets) * live, np.sin(offsets) * live]).astype(np.float32)
    return first, second


def body(
    n,
    inputs,
    segment_ids,
    cotangent,
    qkv_weight,
    out_weight,
    up_weight,
    down_weight,
    norm_gain,
    norm_bias,
    qv_bias,
    up_bias,
    resid_bias,
):
    micro, _, chunk, width = inputs.shape
    length = segment_ids.shape[2]
    head_cols = qkv_weight.shape[3]
    rows_z = qkv_weight.shape[2]
    ff_local = up_weight.shape[2]
    heads = head_cols // HEAD_DIM
    assert micro == 2 and length == 4 * chunk and ff_local == width
    assert head_cols == 192 and width == 768

    first, second = rotary_rows(length, heads)

    vm = pl.BlockSpec(memory_space=pltpu.VMEM)
    anywhere = pl.BlockSpec(memory_space=pl.ANY)
    blk = heads * BQ
    nblk = length // BQ
    dma = pltpu.SemaphoreType.DMA

    def vmem(*shape, dtype=BF):
        return pltpu.VMEM(shape, dtype)

    scratch = dict(
        seg_in=vmem(*segment_ids.shape, dtype=jnp.int32),
        qkv_in=vmem(*qkv_weight.shape),
        wo_in=vmem(*out_weight.shape),
        gain_in=vmem(*norm_gain.shape, dtype=F32),
        shift_in=vmem(*norm_bias.shape, dtype=F32),
        qv_in=vmem(*qv_bias.shape, dtype=F32),
        upb_in=vmem(*up_bias.shape, dtype=F32),
        resid_in=vmem(*resid_bias.shape, dtype=F32),
        taba=vmem(*first.shape, dtype=F32),
        tabb=vmem(*second.shape, dtype=F32),
        w=vmem(2, 3, width, width),
        x=vmem(2, length, width),
        an=vmem(length, width),
        mn=vmem(length, width),
        mu=vmem(2, length, 1, dtype=F32),
        rstd=vmem(2, length, 1, dtype=F32),
        qb=vmem(2, length, HL),
        kb=vmem(2, length, HL),
        vb=vmem(2, length, HL),
        kt=vmem(2, heads * HEAD_DIM, length),
        vt=vmem(2, heads * HEAD_DIM, length),
        cb=vmem(2, length, HL),
        lse=vmem(2, nblk, 1, blk, dtype=F32),
        slope=vmem(2, length, width),
        hid=vmem(2, length, width),
        gb=vmem(2, length, width),
        du=vmem(length, width),
        dqkv=vmem(length, width),
        dc=vmem(length, HL),
        dq=vmem(length, HL, dtype=F32),
        dk=vmem(length, HL, dtype=F32),
        dv=vmem(length, HL, dtype=F32),
        bias=vmem(nblk, BK, BQ),
        pscr=vmem(BK, blk, dtype=F32),
        dpscr=vmem(BK, blk, dtype=F32),
        dscr=vmem(BK, blk),
        pbf=vmem(BK, blk),
        sendb=vmem(3, chunk, width),
        recvb=vmem(2, 2, chunk, width),
        relayed=vmem(2, 2, chunk // 2, width),
        ownp=vmem(2, chunk, width, dtype=F32),
        gw=vmem(3, width, width),
        gsr=vmem(3, width, width),
        zrecv=vmem(3, 4, rows_z, width),
        zacc=vmem(3, max(n - 3, 1), rows_z, width),
        wacc=vmem(3, rows_z, width, dtype=F32),
        yst=vmem(chunk, width, dtype=F32),
        gst=vmem(2, chunk, width, dtype=F32),
        segr=vmem(1, length, dtype=F32),
        par=vmem(2, 8, width, dtype=F32),
        sm=vmem(2, 8, width, dtype=F32),
        smr=vmem(8, width, dtype=F32),
        smt=vmem(8, width, dtype=F32),
        smz=vmem(n - 1, 8, width, dtype=F32),
        tall=vmem(4, 8, width, dtype=F32),
        lsem=dma((8,)),
        isem=dma((10,)),
        psem=dma((2,)),
        xs=dma((6,)),
        xr=dma((6,)),
        agx=dma((6,)),
        agxr=dma((6,)),
        agg=dma((6,)),
        aggr=dma((6,)),
        gs=dma((3,)),
        gr=dma((3,)),
        ws=dma((4, 3, n)),
        wr=dma((3, n)),
        fs=dma((3, n)),
        fr=dma((3, n)),
        rss=dma((4, 6)),
        rsr=dma((4, 6)),
        osend=dma((4,)),
        orecv=dma((2,)),
        ghs=dma((3, 3)),
        ghr=dma((3, 3)),
        zs=dma((2, 3, n)),
        zr=dma((3, 4)),
        za=dma((2, 3, n)),
        sms=dma((n + 3,)),
        smrs=dma((n + 3,)),
    )
    out_y, out_g, out_w, out_s = pl.pallas_call(
        functools.partial(kernel, n, heads),
        out_shape=(
            jax.ShapeDtypeStruct((2, chunk, width), F32),
            jax.ShapeDtypeStruct((2, chunk, width), F32),
            jax.ShapeDtypeStruct((3, rows_z, width), F32),
            jax.ShapeDtypeStruct((4, 8, width), F32),
        ),
        in_specs=[anywhere] * 14,
        out_specs=(anywhere,) * 4,
        scratch_shapes=list(scratch.values()),
        compiler_params=pltpu.CompilerParams(
            collective_id=0, has_side_effects=True, vmem_limit_bytes=67043328
        ),
        name="two_layers",
    )(
        inputs.reshape(micro, chunk, width),
        cotangent.reshape(micro, chunk, width),
        segment_ids,
        qkv_weight,
        out_weight,
        up_weight,
        down_weight[0].T,
        norm_gain,
        norm_bias,
        qv_bias,
        up_bias,
        resid_bias,
        jnp.asarray(first),
        jnp.asarray(second),
    )
    shapes = (
        (2, chunk, width),
        (2, chunk, width),
        (rows_z, width),
        (rows_z, width),
        (3, rows_z, head_cols),
        (head_cols, rows_z),
        (2, width),
        (2, width),
        (2, width),
        (1, 4 * width),
        (1, width),
    )
    y, g, up_g, down_g, qkv_g, out_gr, gain_g, shift_g, qv_g, upb_g, resid_g = pl.pallas_call(
        functools.partial(write_outputs, head_cols),
        out_shape=tuple(jax.ShapeDtypeStruct(shape, F32) for shape in shapes),
        in_specs=[anywhere] * 3 + [vm],
        out_specs=(anywhere,) * 4 + (vm,) * 7,
        scratch_shapes=[
            vmem(4, chunk, width, dtype=F32),
            vmem(2, rows_z, width, dtype=F32),
            vmem(rows_z, width, dtype=F32),
            dma((2, 7)),
        ],
        name="outputs",
    )(out_y, out_g, out_w, out_s)
    return (
        y.reshape(1, micro, 1, chunk, width),
        g.reshape(1, micro, 1, chunk, width),
        qkv_g[None],
        out_gr[None],
        up_g[None],
        down_g.T[None],
        gain_g[None],
        shift_g[None],
        qv_g[None],
        upb_g,
        resid_g,
    )


def solution(mesh):
    return jax.shard_map(
        functools.partial(body, mesh.shape["dp"]),
        mesh=mesh,
        in_specs=(
            P(None, "dp", "tensor", None),
            P(None, "dp", None),
            P(None, "dp", "tensor", None),
            P("section", None, "dp", "tensor"),
            P("section", "tensor", "dp"),
            P("section", "dp", "tensor"),
            P("section", "tensor", "dp"),
            P("section", None, None),
            P("section", None, None),
            P("section", None, None),
            P("section", None),
            P("section", None),
        ),
        out_specs=(
            P("section", None, "dp", "tensor", None),
            P("section", None, "dp", "tensor", None),
            P("section", None, "dp", "tensor"),
            P("section", "tensor", "dp"),
            P("section", "dp", "tensor"),
            P("section", "tensor", "dp"),
            P("section", None, None),
            P("section", None, None),
            P("section", None, None),
            P("section", None),
            P("section", None),
        ),
        check_vma=False,
    )
```

```python
import functools
import math

import jax
import jax.numpy as jnp
import numpy as np
from jax import lax
from jax.experimental import pallas as pl
from jax.experimental.pallas import tpu as pltpu
from jax.sharding import PartitionSpec as P

HEAD_DIM = 64
ROT = 16
SEG_MOST = 384
EPS = 1e-05
MASKED = -1e30
ROOT_HALF = 0.7071067811865476
INV_ROOT_TAU = 0.3989422804014327

BF = jnp.bfloat16
F32 = jnp.float32
MESH = pl.DeviceIdType.MESH

NN = (((1,), (0,)), ((), ()))
NT = (((1,), (1,)), ((), ()))
TN = (((0,), (0,)), ((), ()))

BQ = 128
BK = BQ + SEG_MOST
HL = 256
QO, KO, VO, OO = 0, 192, 384, 576


def mm(a, b, dims):
    return lax.dot_general(a, b, dims, preferred_element_type=F32)


def lane_iota(rows, cols=HL):
    return lax.broadcasted_iota(jnp.int32, (rows, cols), 1)


def remote(src, dst, send, recv, dev):
    return pltpu.make_async_remote_copy(
        src_ref=src, dst_ref=dst, send_sem=send, recv_sem=recv, device_id=dev, device_id_type=MESH
    )


def kernel(
    n,
    heads,
    x_in,
    cot_in,
    seg_far,
    qkv_far,
    wo_far,
    up_in,
    down_in,
    gain_far,
    shift_far,
    qv_far,
    upb_far,
    resid_far,
    taba_far,
    tabb_far,
    out_y,
    out_g,
    out_w,
    out_s,
    seg_in,
    qkv_in,
    wo_in,
    gain_in,
    shift_in,
    qv_in,
    upb_in,
    resid_in,
    taba,
    tabb,
    w,
    x,
    an,
    mn,
    mu,
    rstd,
    qb,
    kb,
    vb,
    kt,
    vt,
    cb,
    lse,
    slope,
    hid,
    gb,
    du,
    dqkv,
    dc,
    dq,
    dk,
    dv,
    bias,
    pscr,
    dpscr,
    dscr,
    pbf,
    sendb,
    recvb,
    relayed,
    ownp,
    gw,
    gsr,
    zrecv,
    zacc,
    wacc,
    yst,
    gst,
    segr,
    par,
    sm,
    smr,
    smt,
    smz,
    tall,
    lsem,
    isem,
    psem,
    xs,
    xr,
    agx,
    agxr,
    agg,
    aggr,
    gs,
    gr,
    ws,
    wr,
    fs,
    fr,
    rss,
    rsr,
    osend,
    orecv,
    ghs,
    ghr,
    zs,
    zr,
    za,
    sms,
    smrs,
):
    s = lax.axis_index("section")
    z = lax.axis_index("dp")
    t = lax.axis_index("tensor")
    sib = (1 - s, z, t)
    width = x.shape[2]
    length = x.shape[1]
    chunk = length // 4
    rows_z = up_in.shape[1]
    half = chunk // 2
    nblk = length // BQ
    own = pl.ds(t * chunk, chunk)
    zrows = pl.ds(z * rows_z, rows_z)

    def plane(k):
        return (s, z, t ^ k)

    def other_z(j):
        return lax.rem(z + j, n)

    lx = pltpu.make_async_copy(x_in.at[s], x.at[0, own], lsem.at[0])
    lc = pltpu.make_async_copy(cot_in.at[s], gst.at[0], lsem.at[1])
    lu = pltpu.make_async_copy(up_in.at[0], w.at[s, 1, zrows], lsem.at[3])
    ld = pltpu.make_async_copy(down_in, w.at[s, 2, zrows], lsem.at[4])
    small_loads = [
        pltpu.make_async_copy(src, dst, isem.at[i])
        for i, (src, dst) in enumerate(
            (
                (qkv_far, qkv_in),
                (wo_far, wo_in),
                (gain_far, gain_in),
                (shift_far, shift_in),
                (qv_far, qv_in),
                (upb_far, upb_in),
                (resid_far, resid_in),
                (seg_far, seg_in),
                (taba_far, taba),
                (tabb_far, tabb),
            )
        )
    ]
    lx.start()
    for load in small_loads:
        load.start()
    lu.start()
    ld.start()
    lc.start()

    barrier = pltpu.get_barrier_semaphore()
    pl.semaphore_signal(barrier, inc=1, device_id=sib, device_id_type=MESH)
    for k in range(1, 4):
        pl.semaphore_signal(barrier, inc=1, device_id=plane(k), device_id_type=MESH)
    for j in range(1, n):
        pl.semaphore_signal(barrier, inc=1, device_id=(s, other_z(j), t), device_id_type=MESH)
    pl.semaphore_wait(barrier, 4 + n - 1)

    head_cols = heads * HEAD_DIM

    def picks(first):
        rows = lax.broadcasted_iota(jnp.int32, (head_cols, width), 0)
        cols = lax.broadcasted_iota(jnp.int32, (head_cols, width), 1)
        return (rows + first == cols).astype(F32).astype(BF)

    def pack_share():
        packed = mm(qkv_in[0, 0], picks(QO), NN) + mm(qkv_in[0, 1], picks(KO), NN)
        packed = packed + mm(qkv_in[0, 2], picks(VO), NN) + mm(wo_in[0], picks(OO), TN)
        w[s, 0, zrows, :] = packed.astype(BF)

    def pack_params():
        par[s, 0:2, :] = gain_in[0]
        par[s, 2:4, :] = shift_in[0]
        par[s, 4:6, :] = qv_in[0]
        par[s, 6:7, :] = upb_in[0:1, pl.ds(pl.multiple_of(t * width, 128), width)]
        par[s, 7:8, :] = resid_in[...]
        rows8 = par[s]
        turned = rows8
        for i in range(1, 4):
            turned = jnp.where(t == i, pltpu.roll(rows8, width - i * head_cols, 1), turned)
        row = lax.broadcasted_iota(jnp.int32, (8, width), 0)
        par[s] = jnp.where((row == 4) | (row == 5), turned, rows8)

    def w_rows(origin):
        return pl.ds(origin * rows_z, rows_z)

    def w_step(p, origin, far, src=None):
        rows = w_rows(origin)
        i = {1: 0, 2: 1, -1: 2, -2: 3}[far]
        return remote(
            w.at[s, p, rows] if src is None else src,
            w.at[s, p, rows],
            ws.at[i, p, origin],
            wr.at[p, origin],
            (s, lax.rem(z + far + n, n), t),
        )

    def inside(far):
        return (z + far < n) if far > 0 else (z + far >= 0)

    def w_send(p, src=None):
        for far in (2, -2, 1, -1):

            @pl.when(inside(far))
            def _():
                w_step(p, z, far, src).start()

    def w_arrive(p, passed, then):
        for e in range(2, n, 2) if passed else range(1, n):
            for sign in (1, -1):
                here = inside(-sign * e)
                if passed:
                    here = here & inside(sign)
                elif e % 2 == 0:
                    here = here & jnp.logical_not(inside(sign))

                @pl.when(here)
                def _():
                    origin = lax.rem(z - sign * e + n, n)
                    w_step(p, origin, sign).wait_recv()
                    if passed:
                        for far in (sign, 2 * sign):

                            @pl.when(inside(far))
                            def _():
                                w_step(p, origin, far).start()

                    if then is not None:
                        then(p, origin)

    def w_sent(p):
        for far in (1, -1, 2, -2):

            @pl.when(inside(far))
            def _():
                w_step(p, z, far).wait_send()

            sign = 1 if far > 0 else -1
            for e in range(2, n, 2):

                @pl.when(inside(-sign * e) & inside(far))
                def _():
                    w_step(p, lax.rem(z - sign * e + n, n), far).wait_send()

    def across(p, origin, layer=0):
        part = w.at[layer, p, w_rows(origin)]
        return remote(part, part, fs.at[p, origin], fr.at[p, origin], sib)

    def g_copy(k):
        return remote(gb.at[1, own], gb.at[1, own], gs.at[k - 1], gr.at[k - 1], plane(k))

    def g_arrival(k):
        rows = pl.ds((t ^ k) * chunk, chunk)
        return remote(gb.at[1, rows], gb.at[1, rows], gs.at[k - 1], gr.at[k - 1], plane(k))

    hops = ((0, 0, 1), (0, 1, 2), (0, 1, 1), (0, 0, 2), (1, 0, 2), (2, 1, 1))

    def gather_copy(buf, send, recv, i):
        k, h, to = hops[i]
        rows = pl.ds((t ^ k) * chunk + h * half, half)
        return remote(buf.at[rows], buf.at[rows], send.at[i], recv.at[i], plane(to))

    def gather_arrival(buf, send, recv, i):
        k, h, to = hops[i]
        rows = pl.ds((t ^ k ^ to) * chunk + h * half, half)
        return remote(buf.at[rows], buf.at[rows], send.at[i], recv.at[i], plane(to))

    def gather_start(buf, send, recv):
        for i in range(4):
            gather_copy(buf, send, recv, i).start()

    def gather_pass(buf, send, recv):
        gather_arrival(buf, send, recv, 0).wait_recv()
        gather_copy(buf, send, recv, 4).start()
        gather_arrival(buf, send, recv, 1).wait_recv()
        gather_copy(buf, send, recv, 5).start()

    def gather_wait(buf, send, recv, k):
        for i in {1: (2,), 2: (3,), 3: (4, 5)}[k]:
            gather_arrival(buf, send, recv, i).wait_recv()

    def arrive(buf, send, recv, k):
        for i in range(1, 4):

            @pl.when(k == i)
            def _():
                gather_wait(buf, send, recv, i)

    def part_copy(phase, i):
        low, high = pl.ds(0, half), pl.ds(half, half)
        bank = phase % 2
        src, dst, to = (
            (sendb.at[2, low], relayed.at[bank, 0], 1),
            (sendb.at[2, high], relayed.at[bank, 1], 2),
            (sendb.at[0, low], recvb.at[bank, 0, low], 1),
            (sendb.at[1, high], recvb.at[bank, 1, high], 2),
            (sendb.at[1, low], recvb.at[bank, 1, low], 2),
            (sendb.at[0, high], recvb.at[bank, 0, high], 1),
        )[i]
        return remote(src, dst, rss.at[phase, i], rsr.at[phase, i], plane(to))

    def parts_start(phase, k):
        for i in {3: (0, 1), 1: (2,), 2: (3,)}[k]:
            part_copy(phase, i).start()

    def parts_pass(phase):
        for i in range(2):
            part_copy(phase, i).wait_recv()
            rows = slice(i * half, (i + 1) * half)
            mine = sendb[1 - i, rows, :].astype(F32)
            sendb[1 - i, rows, :] = (mine + relayed[phase % 2, i].astype(F32)).astype(BF)
            part_copy(phase, 4 + i).start()

    def parts_sent(phase):
        for i in range(6):
            part_copy(phase, i).wait_send()

    def parts_wait(phase):
        for i in range(2, 6):
            part_copy(phase, i).wait_recv()

    ag_i = (x.at[0], xs, xr)
    ag_x = (x.at[1], agx, agxr)
    ag_g = (gb.at[0], agg, aggr)

    @pl.when(s == 0)
    def _():
        w_send(1, up_in.at[0])

    lx.wait()
    gather_start(*ag_i)
    for load in small_loads:
        load.wait()
    pack_share()

    @pl.when(s == 0)
    def _():
        w_send(0)
        w_send(2, down_in)

    pack_params()
    par_copy = remote(par.at[s], par.at[s], psem.at[0], psem.at[1], sib)
    par_copy.start()
    lu.wait()
    ld.wait()

    @pl.when(s == 0)
    def _():
        for p in (1, 0, 2):
            across(p, z).start()

    for i in range(length // BQ):
        cols = slice(i * BQ, (i + 1) * BQ)
        ids = jnp.where(s == 0, seg_in[0, :, cols], seg_in[1, :, cols]).astype(F32)
        segr[:, cols] = ids
        dq[cols, 0:BQ] = jnp.broadcast_to(ids, (BQ, BQ)).T

    @pl.loop(0, nblk)
    def _(b):
        q0 = pl.multiple_of(b * BQ, BQ)
        k0 = pl.multiple_of(jnp.maximum(b * BQ - SEG_MOST, 0), BQ)
        seg_k = dq[pl.ds(k0, BK), 0:BQ]
        seg_q = segr[:, pl.ds(q0, BQ)]
        kpos = lax.broadcasted_iota(jnp.int32, (BK, BQ), 0) + k0
        qpos = lax.broadcasted_iota(jnp.int32, (BK, BQ), 1) + q0
        allowed = (seg_k == seg_q) & (kpos <= qpos)
        bias[b] = jnp.where(allowed, 0.0, MASKED).astype(BF)

    par_wait = remote(par.at[1 - s], par.at[1 - s], psem.at[0], psem.at[1], sib)
    par_copy.wait_send()
    par_wait.wait_recv()

    @pl.loop(0, 2)
    def _(i):
        sm[i] = jnp.zeros((8, width), F32)

    def first_w_pass(p):
        @pl.when(s == 0)
        def _():
            w_arrive(p, True, lambda p, origin: across(p, origin).start())

    def first_w(p):
        @pl.when(s == 0)
        def _():
            w_arrive(p, False, lambda p, origin: across(p, origin).start())

        @pl.when(s == 1)
        def _():
            for origin in range(n):
                across(p, origin).wait_recv()

    def first_w_sent():
        @pl.when(s == 0)
        def _():
            for p in range(3):
                w_sent(p)
                for origin in range(n):
                    across(p, origin).wait_send()

    def second_w_send():
        @pl.when(s == 1)
        def _():
            w_send(1, up_in.at[0])
            w_send(0)
            w_send(2, down_in)
            for p in (1, 0, 2):
                across(p, z, 1).start()

    def second_w_pass(p):
        @pl.when(s == 1)
        def _():
            w_arrive(p, True, lambda p, origin: across(p, origin, 1).start())

    def second_w_give(p):
        @pl.when(s == 1)
        def _():
            w_arrive(p, False, lambda p, origin: across(p, origin, 1).start())

    def second_w(p):
        @pl.when(s == 0)
        def _():
            for origin in range(n):
                across(p, origin, 1).wait_recv()

    def second_w_sent():
        @pl.when(s == 1)
        def _():
            for p in range(3):
                w_sent(p)
                for origin in range(n):
                    across(p, origin, 1).wait_send()

    def prow(layer, r, cols=None):
        if cols is None:
            return par[layer, r : r + 1, :]
        return par[layer, r : r + 1, cols]

    def rope_tables(b, sign):
        ca = taba[0, b]
        sa = taba[1, b]
        c0 = tabb[0]
        s0 = tabb[1]
        cos = ca * c0 - sa * s0
        sin = sa * c0 + ca * s0
        lane = lane_iota(BQ) & (HEAD_DIM - 1)
        return cos, jnp.where(lane < ROT // 2, -sign, sign) * sin

    def rope(u, b, sign):
        halves = []
        lane = lane_iota(BQ) & (HEAD_DIM - 1)
        for i in range(u.shape[0] // BQ):
            part = u[i * BQ : (i + 1) * BQ]
            cos, sin = rope_tables(b + i, sign)
            partner = jnp.where(
                lane < ROT // 2,
                pltpu.roll(part, HL - ROT // 2, 1),
                pltpu.roll(part, ROT // 2, 1),
            )
            halves.append(part * cos + partner * sin)
        return jnp.concatenate(halves, axis=0)

    def stack_heads(block):
        lane = lane_iota(BQ) >> 6
        return jnp.concatenate(
            [jnp.where(lane == h, block, jnp.zeros_like(block)) for h in range(heads)], axis=0
        )

    sub = 128

    def norm_chunk(layer, c):
        @pl.loop(0, chunk // sub)
        def _(i):
            rows = pl.ds(pl.multiple_of(c * chunk + i * sub, sub), sub)
            v = x[layer, rows, :].astype(F32)
            m = jnp.mean(v, axis=-1, keepdims=True)
            v = v - m
            r = lax.rsqrt(jnp.mean(v * v, axis=-1, keepdims=True) + EPS)
            mu[layer, rows, :] = m
            rstd[layer, rows, :] = r
            v = v * r
            an[rows, :] = (v * prow(layer, 0) + prow(layer, 2)).astype(BF)
            mn[rows, :] = (v * prow(layer, 1) + prow(layer, 3)).astype(BF)

    def renorm_all(layer):
        @pl.loop(0, length // sub)
        def _(i):
            rows = pl.ds(pl.multiple_of(i * sub, sub), sub)
            v = (x[layer, rows, :].astype(F32) - mu[layer, rows, :]) * rstd[layer, rows, :]
            an[rows, :] = (v * prow(layer, 0) + prow(layer, 2)).astype(BF)
            mn[rows, :] = (v * prow(layer, 1) + prow(layer, 3)).astype(BF)

    def project_in(layer, c):
        rows = pl.ds(pl.multiple_of(c * chunk, chunk), chunk)
        a = an[rows, :]
        b0 = c * (chunk // BQ)
        lane = lane_iota(chunk)
        u = mm(a, w[layer, 0, :, QO : QO + HL], NN) + prow(layer, 4, slice(0, HL))
        qb[layer, rows, :] = (rope(u, b0, 1.0) * 0.125).astype(BF)
        u = mm(a, w[layer, 0, :, KO - 64 : KO - 64 + HL], NN)
        u = rope(pltpu.roll(u, HL - 64, 1), b0, 1.0)
        kb[layer, rows, :] = u.astype(BF)
        kt[layer, :, rows] = u.T[: heads * HEAD_DIM].astype(BF)
        u = mm(a, w[layer, 0, :, VO : VO + HL], NN) + prow(layer, 5, slice(0, HL))
        u = jnp.where(lane < heads * HEAD_DIM, u, 0.0)
        vb[layer, rows, :] = u.astype(BF)
        vt[layer, :, rows] = u.T[: heads * HEAD_DIM].astype(BF)

    def attend(layer, within=None):
        @pl.loop(0, nblk)
        def _(b):
            if within is not None:
                pl.when(b == nblk // 2)(within)

            q0 = pl.multiple_of(b * BQ, BQ)
            k0 = pl.multiple_of(jnp.maximum(b * BQ - SEG_MOST, 0), BQ)
            qm = stack_heads(qb[layer, pl.ds(q0, BQ), :])
            pscr[...] = mm(kb[layer, pl.ds(k0, BK), :], qm, NT)
            top = None
            for i in range(BK // BQ):
                irows = slice(i * BQ, (i + 1) * BQ)
                blk = bias[b, irows, :].astype(F32)
                sc = pscr[irows, :] + jnp.concatenate([blk] * heads, axis=1)
                pscr[irows, :] = sc
                peak = jnp.max(sc, axis=0, keepdims=True)
                top = peak if top is None else jnp.maximum(top, peak)
            total = None
            for i in range(BK // BQ):
                e = jnp.exp(pscr[i * BQ : (i + 1) * BQ, :] - top)
                pscr[i * BQ : (i + 1) * BQ, :] = e
                part = jnp.sum(e, axis=0, keepdims=True)
                total = part if total is None else total + part
            lse[layer, b] = top + jnp.log(total)
            inv = 1.0 / total
            ctx = [jnp.zeros((HL - heads * HEAD_DIM, BQ), F32)]
            for h in range(heads):
                cols = slice(h * BQ, (h + 1) * BQ)
                ph = (pscr[:, cols] * inv[:, cols]).astype(BF)
                vals = vt[layer, h * HEAD_DIM : (h + 1) * HEAD_DIM, pl.ds(k0, BK)]
                ctx.append(mm(vals, ph, NN))
            cb[layer, pl.ds(q0, BQ), :] = jnp.concatenate(ctx, axis=0).T.astype(BF)

    def hidden(layer, c):
        rows = pl.ds(pl.multiple_of(c * chunk, chunk), chunk)
        a = mn[rows, :]
        for j in range(width // 256):
            cols = slice(j * 256, (j + 1) * 256)
            u = mm(a, w[layer, 1, :, cols], NN) + prow(layer, 6, cols)
            phi = 0.5 * (1.0 + lax.erf(u * ROOT_HALF))
            hid[layer, rows, cols] = (u * phi).astype(BF)
            slope[layer, rows, cols] = (phi + u * INV_ROOT_TAU * jnp.exp(-0.5 * u * u)).astype(BF)

    def project_out(layer):
        phase = layer
        if layer == 1:
            parts_sent(0)
        for k in (3, 1, 2, 0):
            rows = pl.ds(pl.multiple_of((t ^ k) * chunk, chunk), chunk)
            c = cb[layer, rows, :]
            h = hid[layer, rows, :]
            for j in range(width // 256):
                cols = slice(j * 256, (j + 1) * 256)
                y = mm(c, w[layer, 0, cols, 512:768], NT) + mm(h, w[layer, 2, cols, :], NT)
                if k:
                    sendb[k - 1, :, cols] = y.astype(BF)
                else:
                    ownp[phase % 2, :, cols] = y
            if k:
                parts_start(phase, k)

    def place(layer, stage, out, idx):
        @pl.when(s == layer)
        def _():
            pltpu.make_async_copy(stage, out.at[s], osend.at[idx]).start()

        @pl.when(s != layer)
        def _():
            remote(stage, out.at[s], osend.at[idx], orecv.at[idx // 2], sib).start()

    def placed(layer, stage, out, idx):
        @pl.when(s == layer)
        def _():
            pltpu.make_async_copy(stage, out.at[s], osend.at[idx]).wait()

        @pl.when(s != layer)
        def _():
            remote(stage, out.at[s], osend.at[idx], orecv.at[idx // 2], sib).wait_send()

    def finish_y(layer):
        phase = layer
        parts_wait(phase)
        if layer == 1:
            placed(0, yst, out_y, 0)

        @pl.loop(0, chunk // sub)
        def _(i):
            r = pl.ds(pl.multiple_of(i * sub, sub), sub)
            rows = pl.ds(pl.multiple_of(t * chunk + i * sub, sub), sub)
            y = x[layer, rows, :].astype(F32) + ownp[phase % 2, r, :] + prow(layer, 7)
            for k in range(2):
                y = y + recvb[phase % 2, k, r, :].astype(F32)
            yst[r, :] = y
            if layer == 0:
                x[1, rows, :] = y.astype(BF)

        if layer == 0:
            gather_start(*ag_x)
        place(layer, yst, out_y, layer)

    def reduce_start(layer, p, j, buf):
        rows = pl.ds(j * 256, 256)


        @pl.when(s != layer)
        def _():
            remote(buf.at[p, rows], gsr.at[p, rows], ghs.at[p, j], ghr.at[p, j], sib).start()

    def z_item(p, e, sign, buf):
        dest = lax.rem(z + sign * e + n, n)
        way = 0 if sign > 0 else 1
        if e <= 2:
            slot = 2 * way + e - 1
            dst, recv, far = zrecv.at[p, slot], zr.at[p, slot], e
        else:
            place_no = e - 3 if sign > 0 else n - z + e - 4
            dst, recv, far = zacc.at[p, place_no], za.at[way, p, e - 3], 1
        return remote(
            buf.at[p, w_rows(dest)],
            dst,
            zs.at[way, p, e - 1],
            recv,
            (s, lax.rem(z + sign * far + n, n), t),
        )

    def first_of(sign):
        return (z == 0) if sign > 0 else (z == n - 1)

    def z_send(p, buf):
        for e in range(n - 1, 0, -1):
            for sign in (1, -1):
                go = inside(sign * e)
                if e > 1:
                    go = go & first_of(sign)

                @pl.when(go)
                def _():
                    z_item(p, e, sign, buf).start()

    def z_pass(layer, p, buf):
        @pl.when(s == layer)
        def _():
            for e in range(n - 2, 1, -1):
                for sign in (1, -1):

                    @pl.when(inside(sign * e) & inside(-sign))
                    def _():
                        way = 0 if sign > 0 else 1
                        place_no = e - 2 if sign > 0 else n - z + e - 4
                        got = zacc.at[p, place_no]
                        remote(got, got, zs.at[way, p, e - 1], za.at[way, p, e - 2], sib).wait_recv()
                        base = lax.rem(z + sign * e + n, n) * rows_z

                        @pl.loop(0, rows_z // step)
                        def _(i):
                            r = pl.ds(pl.multiple_of(i * step, 16), step)
                            q = pl.ds(pl.multiple_of(base + i * step, 16), step)
                            more = zacc[p, place_no, r, :].astype(F32)
                            buf[p, q, :] = (buf[p, q, :].astype(F32) + more).astype(BF)

                        z_item(p, e, sign, buf).start()

    def z_end(p, buf):
        for slot in range(4):
            sign = 1 if slot < 2 else -1
            e = slot % 2 + 1

            @pl.when(inside(-sign * e))
            def _():
                got = zrecv.at[p, slot]
                remote(got, got, zs.at[0, p, 0], zr.at[p, slot], sib).wait_recv()

                @pl.loop(0, rows_z // step)
                def _(i):
                    r = pl.ds(pl.multiple_of(i * step, 16), step)
                    wacc[p, r, :] = wacc[p, r, :] + zrecv[p, slot, r, :].astype(F32)

    def z_sent(p, buf):
        for e in range(1, n):
            for sign in (1, -1):

                @pl.when(inside(sign * e))
                def _():
                    z_item(p, e, sign, buf).wait_send()

    step = 48

    def reduce_cores(layer, p, buf):
        @pl.when(s == layer)
        def _():
            for j in range(width // 256):
                rows = pl.ds(j * 256, 256)
                remote(buf.at[p, rows], gsr.at[p, rows], ghs.at[p, j], ghr.at[p, j], sib).wait_recv()

            @pl.loop(0, rows_z // step)
            def _(i):
                r = pl.ds(pl.multiple_of(i * step, 16), step)
                q = pl.ds(pl.multiple_of(z * rows_z + i * step, 16), step)
                wacc[p, r, :] = buf[p, q, :].astype(F32) + gsr[p, q, :].astype(F32)

            for j in range(1, n):
                base = other_z(j) * rows_z

                @pl.loop(0, rows_z // step)
                def _(i):
                    q = pl.ds(pl.multiple_of(base + i * step, 16), step)
                    buf[p, q, :] = (buf[p, q, :].astype(F32) + gsr[p, q, :].astype(F32)).astype(BF)

            z_send(p, buf)

        @pl.when(s != layer)
        def _():
            for j in range(width // 256):
                rows = pl.ds(j * 256, 256)
                remote(buf.at[p, rows], gsr.at[p, rows], ghs.at[p, j], ghr.at[p, j], sib).wait_send()

    def add_down_grad(k, buf):
        rows = pl.ds(pl.multiple_of((t ^ k) * chunk, chunk), chunk)
        h = hid[0, rows, :]
        for j in range(width // 256):
            cols = slice(j * 256, (j + 1) * 256)
            more = mm(gb[0, rows, cols], h, TN)
            before = jnp.where(k == 0, 0.0, buf[2, cols, :].astype(F32))
            buf[2, cols, :] = (before + more).astype(BF)

            @pl.when(k == 3)
            def _():
                reduce_start(0, 2, j, buf)

    def grad_part(layer, p, buf):
        for j in range(width // 256):
            cols = slice(j * 256, (j + 1) * 256)
            if p == 2:
                buf[p, cols, :] = mm(gb[layer, :, cols], hid[layer], TN).astype(BF)
            elif p == 1:
                buf[p, cols, :] = mm(mn[:, cols], du[...], TN).astype(BF)
            else:
                buf[p, cols, 0:512] = mm(an[:, cols], dqkv[:, 0:512], TN).astype(BF)
                buf[p, cols, 512:768] = (
                    mm(an[:, cols], dqkv[:, 512:768], TN) + mm(gb[layer, :, cols], cb[layer], TN)
                ).astype(BF)
            reduce_start(layer, p, j, buf)

    def hidden_back(layer, c):
        rows = pl.ds(pl.multiple_of(c * chunk, chunk), chunk)
        g = gb[layer, rows, :]
        for j in range(width // 256):
            cols = slice(j * 256, (j + 1) * 256)
            d = mm(g, w[layer, 2, :, cols], NN) * slope[layer, rows, cols].astype(F32)
            sm[layer, 6:7, cols] = sm[layer, 6:7, cols] + jnp.sum(d, axis=0, keepdims=True)
            du[rows, cols] = d.astype(BF)
        d = pltpu.roll(mm(g, w[layer, 0, :, 512:768], NN), HL - 64, 1)
        lane = lane_iota(chunk)
        dc[rows, :] = jnp.where(lane < heads * HEAD_DIM, d, 0.0).astype(BF)

    def zero_sums():
        @pl.loop(0, length // sub)
        def _(i):
            rows = pl.ds(pl.multiple_of(i * sub, sub), sub)
            dk[rows, :] = jnp.zeros((sub, HL), F32)
            dv[rows, :] = jnp.zeros((sub, HL), F32)

    def attend_back(layer, first, last, within=None):
        @pl.loop(first, last)
        def _(b):
            if within is not None:
                pl.when(b == first + 2)(within)

            q0 = pl.multiple_of(b * BQ, BQ)
            k0 = pl.multiple_of(jnp.maximum(b * BQ - SEG_MOST, 0), BQ)
            qm = stack_heads(qb[layer, pl.ds(q0, BQ), :])
            dm = stack_heads(dc[pl.ds(q0, BQ), :])
            ls = lse[layer, b]
            win = pl.ds(k0, BK)
            pscr[...] = mm(kb[layer, win, :], qm, NT)
            dpscr[...] = mm(vb[layer, win, :], dm, NT)
            total = None
            for i in range(BK // BQ):
                irows = slice(i * BQ, (i + 1) * BQ)
                blk = bias[b, irows, :].astype(F32)
                pr = jnp.exp(pscr[irows, :] + jnp.concatenate([blk] * heads, axis=1) - ls)
                pscr[irows, :] = pr
                pbf[irows, :] = pr.astype(BF)
                part = jnp.sum(pr * dpscr[irows, :], axis=0, keepdims=True)
                total = part if total is None else total + part
            dv[win, :] = dv[win, :] + mm(pbf[...], dm, NN)
            for i in range(BK // BQ):
                irows = slice(i * BQ, (i + 1) * BQ)
                dscr[irows, :] = (pscr[irows, :] * (dpscr[irows, :] - total)).astype(BF)
            dk[win, :] = dk[win, :] + mm(dscr[...], qm, NN)
            out = []
            for h in range(heads):
                keys = kt[layer, h * HEAD_DIM : (h + 1) * HEAD_DIM, pl.ds(k0, BK)]
                out.append(mm(keys, dscr[:, h * BQ : (h + 1) * BQ], NN))
            out.append(jnp.zeros((HL - heads * HEAD_DIM, BQ), F32))
            dq[pl.ds(q0, BQ), :] = jnp.concatenate(out, axis=0).T

    def pack_qkv(layer, c):
        rows = pl.ds(pl.multiple_of(c * chunk, chunk), chunk)
        b0 = c * (chunk // BQ)
        lane = lane_iota(chunk)
        gq = rope(dq[rows, :], b0, -1.0) * 0.125
        gk = rope(dk[rows, :], b0, -1.0)
        gv = dv[rows, :]
        sm[layer, 4:5, 0:HL] = sm[layer, 4:5, 0:HL] + jnp.sum(gq, axis=0, keepdims=True)
        sm[layer, 5:6, 0:HL] = sm[layer, 5:6, 0:HL] + jnp.sum(gv, axis=0, keepdims=True)
        rk = pltpu.roll(gk, 192, 1)
        rv = pltpu.roll(gv, 128, 1)
        dqkv[rows, 0:256] = jnp.where(lane < 192, gq, rk).astype(BF)
        dqkv[rows, 256:512] = jnp.where(lane < 128, rk, rv).astype(BF)
        dqkv[rows, 512:768] = jnp.where(lane < 64, rv, 0.0).astype(BF)

    def project_back(layer):
        phase = 3 - layer
        parts_sent(1 if layer == 1 else 2)
        for k in (3, 1, 2, 0):
            rows = pl.ds(pl.multiple_of((t ^ k) * chunk, chunk), chunk)
            pack_qkv(layer, t ^ k)
            da_in = dqkv[rows, :]
            du_in = du[rows, :]
            m = mu[layer, rows, :]
            r = rstd[layer, rows, :]
            for j in range(width // 256):
                cols = slice(j * 256, (j + 1) * 256)
                da = mm(da_in, w[layer, 0, cols, :], NT)
                dm = mm(du_in, w[layer, 1, cols, :], NT)
                unit = (x[layer, rows, cols].astype(F32) - m) * r
                sums = [da * unit, dm * unit, da, dm]
                for i in range(4):
                    sm[layer, i : i + 1, cols] = sm[layer, i : i + 1, cols] + jnp.sum(
                        sums[i], axis=0, keepdims=True
                    )
                e = da * prow(layer, 0, cols) + dm * prow(layer, 1, cols)
                if k:
                    sendb[k - 1, :, cols] = e.astype(BF)
                else:
                    ownp[phase % 2, :, cols] = e
            if k:
                parts_start(phase, k)

    def finish_e(layer):
        phase = 3 - layer
        parts_wait(phase)
        stage = gst.at[1 - layer]
        given = gst.at[0]

        @pl.loop(0, chunk // sub)
        def _(i):
            r = pl.ds(pl.multiple_of(i * sub, sub), sub)
            rows = pl.ds(pl.multiple_of(t * chunk + i * sub, sub), sub)
            e = ownp[phase % 2, r, :]
            for k in range(2):
                e = e + recvb[phase % 2, k, r, :].astype(F32)
            rs = rstd[layer, rows, :]
            unit = (x[layer, rows, :].astype(F32) - mu[layer, rows, :]) * rs
            g = given[r, :]
            if layer == 1:
                sm[1, 7:8, :] = sm[1, 7:8, :] + jnp.sum(g, axis=0, keepdims=True)
            d = rs * (
                e
                - jnp.mean(e, axis=-1, keepdims=True)
                - unit * jnp.mean(e * unit, axis=-1, keepdims=True)
            )
            g = g + d
            stage[r, :] = g
            if layer == 1:
                sm[0, 7:8, :] = sm[0, 7:8, :] + jnp.sum(g, axis=0, keepdims=True)
                gb[0, rows, :] = g.astype(BF)

        if layer == 1:
            gather_start(*ag_g)
        place(layer, stage, out_g, 2 + layer)

    norm_chunk(0, t)
    zero_sums()
    gather_pass(*ag_i)
    lc.wait()
    gb[1, own, :] = gst[0].astype(BF)
    for k in range(1, 4):
        g_copy(k).start()
    first_w_pass(1)

    @pl.loop(1, 4)
    def _(k):
        arrive(*ag_i, k)
        norm_chunk(0, t ^ k)

    first_w(1)

    @pl.loop(0, 4)
    def _(c):
        hidden(0, c)

    first_w_pass(0)
    first_w(0)

    @pl.loop(0, 4)
    def _(c):
        project_in(0, c)

    first_w_pass(2)
    attend(0)
    second_w_send()
    first_w(2)
    project_out(0)
    parts_pass(0)
    second_w_pass(1)
    second_w_pass(0)
    finish_y(0)

    @pl.loop(0, 4)
    def _(k):
        @pl.when(k == 2)
        def _():
            second_w_give(0)

        @pl.when(k == 3)
        def _():
            second_w(0)

            @pl.loop(0, 3)
            def _(m):
                project_in(1, t ^ m)

        arrive(*ag_x, k)
        norm_chunk(1, t ^ k)

        @pl.when(k == 0)
        def _():
            second_w_give(1)
            gather_pass(*ag_x)
            second_w_pass(2)
            second_w(1)

        hidden(1, t ^ k)

    project_in(1, t ^ 3)
    second_w_give(2)
    attend(1)
    second_w(2)
    project_out(1)

    for k in range(1, 4):
        g_arrival(k).wait_recv()
    @pl.loop(0, 4)
    def _(c):
        hidden_back(1, c)

    attend_back(1, 0, nblk, lambda: parts_pass(1))
    project_back(1)
    grad_part(1, 2, gw)
    grad_part(1, 1, gw)
    reduce_cores(1, 2, gw)
    parts_pass(2)
    reduce_cores(1, 1, gw)
    grad_part(1, 0, gw)
    finish_y(1)
    z_pass(1, 2, gw)
    finish_e(1)

    late = w.at[1]
    per = chunk // BQ
    first_w_sent()
    second_w_sent()
    zero_sums()
    reduce_cores(1, 0, gw)

    @pl.loop(0, 8)
    def _(step_no):
        k = jnp.where(step_no < 2, 0, jnp.where(step_no < 5, step_no - 1, step_no - 4))

        @pl.when((step_no == 0) | ((step_no >= 2) & (step_no < 5)))
        def _():
            arrive(*ag_g, k)
            add_down_grad(k, late)
            hidden_back(0, t ^ k)

        @pl.when(step_no == 2)
        def _():
            z_pass(1, 1, gw)

        @pl.when(step_no == 4)
        def _():
            z_pass(1, 0, gw)

        @pl.when(step_no == 6)
        def _():
            reduce_cores(0, 2, late)
            grad_part(0, 1, late)

        @pl.when(step_no == 7)
        def _():
            reduce_cores(0, 1, late)

        @pl.when((step_no == 1) | (step_no >= 5))
        def _():
            attend_back(0, (t ^ k) * per, ((t ^ k) + 1) * per)

        @pl.when(step_no == 1)
        def _():
            gather_pass(*ag_g)
            renorm_all(0)

    z_pass(0, 2, late)
    project_back(0)

    to_sib = remote(sm.at[1 - s], smr, sms.at[0], smrs.at[0], sib)
    to_sib.start()
    grad_part(0, 0, late)
    to_sib.wait()
    smt[...] = sm[s] + smr[...]

    def small_z(j):
        return remote(smt, smz.at[j - 1], sms.at[j], smrs.at[j], (s, other_z(j), t))

    def small_copy(k):
        return remote(tall.at[t], tall.at[t], sms.at[n + k - 1], smrs.at[n + k - 1], plane(k))

    for j in range(1, n):
        small_z(j).start()
    parts_pass(3)
    z_pass(0, 1, late)
    reduce_cores(0, 0, late)

    def matrix_end(p):
        z_end(p, late)
        pltpu.make_async_copy(wacc.at[p], out_w.at[p], lsem.at[p]).start()

    matrix_end(2)
    for j in range(1, n):
        small_z(j).wait()
    total = smt[...]
    for j in range(1, n):
        total = total + smz[j - 1]
    tall[t] = total
    for k in range(1, 4):
        small_copy(k).start()
    z_pass(0, 0, late)
    finish_e(0)
    matrix_end(1)
    for k in range(1, 4):
        small_copy(k).wait_send()
        remote(
            tall.at[t ^ k], tall.at[t ^ k], sms.at[n + k - 1], smrs.at[n + k - 1], plane(k)
        ).wait_recv()
    small_out = pltpu.make_async_copy(tall, out_s, lsem.at[5])
    small_out.start()
    matrix_end(0)
    small_out.wait()

    for p in range(3):
        pltpu.make_async_copy(wacc.at[p], out_w.at[p], lsem.at[p]).wait()
        z_sent(p, late)

    for k in range(1, 4):
        g_copy(k).wait_send()
    for i in range(6):
        gather_copy(*ag_i, i).wait_send()
        gather_copy(*ag_x, i).wait_send()
        gather_copy(*ag_g, i).wait_send()
    parts_sent(3)
    placed(1, yst, out_y, 1)
    placed(1, gst.at[0], out_g, 3)
    placed(0, gst.at[1], out_g, 2)
    remote(yst, out_y.at[1 - s], osend.at[0], orecv.at[0], sib).wait_recv()
    remote(gst.at[0], out_g.at[1 - s], osend.at[0], orecv.at[1], sib).wait_recv()


def write_outputs(
    head_cols, y, g, wg, small, y_out, g_out, up, down, qkv, out, gain, shift, qv, upb, resid,
    buf_a, buf_b, buf_c, sem
):
    halves = [(y.at[i], y_out.at[i]) for i in range(2)] + [(g.at[i], g_out.at[i]) for i in range(2)]
    pairs = halves + [(wg.at[1], up), (wg.at[2], down)]
    held = [buf_a.at[i] for i in range(4)] + [buf_b.at[i] for i in range(2)]
    loads = [pltpu.make_async_copy(p[0], v, sem.at[0, i]) for i, (p, v) in enumerate(zip(pairs, held))]
    copies = [pltpu.make_async_copy(v, p[1], sem.at[1, i]) for i, (p, v) in enumerate(zip(pairs, held))]
    head = pltpu.make_async_copy(wg.at[0], buf_c, sem.at[0, 6])
    head.start()
    for load in loads:
        load.start()
    head.wait()
    first = buf_c[...]
    width = first.shape[1]
    for i in range(3):
        turned = pltpu.roll(first, width - i * head_cols, 1) if i else first
        qkv[i] = turned[:, :head_cols]
    last = pltpu.roll(first, width - 3 * head_cols, 1)[:, :256]
    out[...] = last.T[:head_cols, :]
    for load, copy in zip(loads, copies):
        load.wait()
        copy.start()
    total = small[0] + small[1] + small[2] + small[3]
    gain[...] = total[0:2]
    shift[...] = total[2:4]
    resid[...] = total[7:8]
    spread = small[0]
    upb[:, 0:width] = small[0, 6:7, :]
    for i in range(1, 4):
        spread = spread + pltpu.roll(small[i], i * head_cols, 1)
        upb[:, i * width : (i + 1) * width] = small[i, 6:7, :]
    qv[...] = spread[4:6]
    for copy in copies:
        copy.wait()


def rotary_rows(length, heads):
    rate = np.zeros((HL,), np.float64)
    for h in range(heads):
        for j in range(ROT // 2):
            value = math.exp(j * (-2.0 * math.log(10000.0) / ROT))
            rate[h * HEAD_DIM + j] = value
            rate[h * HEAD_DIM + j + ROT // 2] = value
    live = (np.arange(HL) < heads * HEAD_DIM).astype(np.float64)
    starts = np.arange(length // BQ)[:, None] * BQ * rate[None]
    offsets = np.arange(BQ)[:, None] * rate[None]
    first = np.stack([np.cos(starts), np.sin(starts)])[:, :, None].astype(np.float32)
    second = np.stack([np.cos(offsets) * live, np.sin(offsets) * live]).astype(np.float32)
    return first, second


def body(
    n,
    inputs,
    segment_ids,
    cotangent,
    qkv_weight,
    out_weight,
    up_weight,
    down_weight,
    norm_gain,
    norm_bias,
    qv_bias,
    up_bias,
    resid_bias,
):
    micro, _, chunk, width = inputs.shape
    length = segment_ids.shape[2]
    head_cols = qkv_weight.shape[3]
    rows_z = qkv_weight.shape[2]
    ff_local = up_weight.shape[2]
    heads = head_cols // HEAD_DIM
    assert micro == 2 and length == 4 * chunk and ff_local == width
    assert head_cols == 192 and width == 768

    first, second = rotary_rows(length, heads)

    vm = pl.BlockSpec(memory_space=pltpu.VMEM)
    anywhere = pl.BlockSpec(memory_space=pl.ANY)
    blk = heads * BQ
    nblk = length // BQ
    dma = pltpu.SemaphoreType.DMA

    def vmem(*shape, dtype=BF):
        return pltpu.VMEM(shape, dtype)

    scratch = dict(
        seg_in=vmem(*segment_ids.shape, dtype=jnp.int32),
        qkv_in=vmem(*qkv_weight.shape),
        wo_in=vmem(*out_weight.shape),
        gain_in=vmem(*norm_gain.shape, dtype=F32),
        shift_in=vmem(*norm_bias.shape, dtype=F32),
        qv_in=vmem(*qv_bias.shape, dtype=F32),
        upb_in=vmem(*up_bias.shape, dtype=F32),
        resid_in=vmem(*resid_bias.shape, dtype=F32),
        taba=vmem(*first.shape, dtype=F32),
        tabb=vmem(*second.shape, dtype=F32),
        w=vmem(2, 3, width, width),
        x=vmem(2, length, width),
        an=vmem(length, width),
        mn=vmem(length, width),
        mu=vmem(2, length, 1, dtype=F32),
        rstd=vmem(2, length, 1, dtype=F32),
        qb=vmem(2, length, HL),
        kb=vmem(2, length, HL),
        vb=vmem(2, length, HL),
        kt=vmem(2, heads * HEAD_DIM, length),
        vt=vmem(2, heads * HEAD_DIM, length),
        cb=vmem(2, length, HL),
        lse=vmem(2, nblk, 1, blk, dtype=F32),
        slope=vmem(2, length, width),
        hid=vmem(2, length, width),
        gb=vmem(2, length, width),
        du=vmem(length, width),
        dqkv=vmem(length, width),
        dc=vmem(length, HL),
        dq=vmem(length, HL, dtype=F32),
        dk=vmem(length, HL, dtype=F32),
        dv=vmem(length, HL, dtype=F32),
        bias=vmem(nblk, BK, BQ),
        pscr=vmem(BK, blk, dtype=F32),
        dpscr=vmem(BK, blk, dtype=F32),
        dscr=vmem(BK, blk),
        pbf=vmem(BK, blk),
        sendb=vmem(3, chunk, width),
        recvb=vmem(2, 2, chunk, width),
        relayed=vmem(2, 2, chunk // 2, width),
        ownp=vmem(2, chunk, width, dtype=F32),
        gw=vmem(3, width, width),
        gsr=vmem(3, width, width),
        zrecv=vmem(3, 4, rows_z, width),
        zacc=vmem(3, max(n - 3, 1), rows_z, width),
        wacc=vmem(3, rows_z, width, dtype=F32),
        yst=vmem(chunk, width, dtype=F32),
        gst=vmem(2, chunk, width, dtype=F32),
        segr=vmem(1, length, dtype=F32),
        par=vmem(2, 8, width, dtype=F32),
        sm=vmem(2, 8, width, dtype=F32),
        smr=vmem(8, width, dtype=F32),
        smt=vmem(8, width, dtype=F32),
        smz=vmem(n - 1, 8, width, dtype=F32),
        tall=vmem(4, 8, width, dtype=F32),
        lsem=dma((8,)),
        isem=dma((10,)),
        psem=dma((2,)),
        xs=dma((6,)),
        xr=dma((6,)),
        agx=dma((6,)),
        agxr=dma((6,)),
        agg=dma((6,)),
        aggr=dma((6,)),
        gs=dma((3,)),
        gr=dma((3,)),
        ws=dma((4, 3, n)),
        wr=dma((3, n)),
        fs=dma((3, n)),
        fr=dma((3, n)),
        rss=dma((4, 6)),
        rsr=dma((4, 6)),
        osend=dma((4,)),
        orecv=dma((2,)),
        ghs=dma((3, 3)),
        ghr=dma((3, 3)),
        zs=dma((2, 3, n)),
        zr=dma((3, 4)),
        za=dma((2, 3, n)),
        sms=dma((n + 3,)),
        smrs=dma((n + 3,)),
    )
    out_y, out_g, out_w, out_s = pl.pallas_call(
        functools.partial(kernel, n, heads),
        out_shape=(
            jax.ShapeDtypeStruct((2, chunk, width), F32),
            jax.ShapeDtypeStruct((2, chunk, width), F32),
            jax.ShapeDtypeStruct((3, rows_z, width), F32),
            jax.ShapeDtypeStruct((4, 8, width), F32),
        ),
        in_specs=[anywhere] * 14,
        out_specs=(anywhere,) * 4,
        scratch_shapes=list(scratch.values()),
        compiler_params=pltpu.CompilerParams(
            collective_id=0, has_side_effects=True, vmem_limit_bytes=67043328
        ),
        name="two_layers",
    )(
        inputs.reshape(micro, chunk, width),
        cotangent.reshape(micro, chunk, width),
        segment_ids,
        qkv_weight,
        out_weight,
        up_weight,
        down_weight[0].T,
        norm_gain,
        norm_bias,
        qv_bias,
        up_bias,
        resid_bias,
        jnp.asarray(first),
        jnp.asarray(second),
    )
    shapes = (
        (2, chunk, width),
        (2, chunk, width),
        (rows_z, width),
        (rows_z, width),
        (3, rows_z, head_cols),
        (head_cols, rows_z),
        (2, width),
        (2, width),
        (2, width),
        (1, 4 * width),
        (1, width),
    )
    y, g, up_g, down_g, qkv_g, out_gr, gain_g, shift_g, qv_g, upb_g, resid_g = pl.pallas_call(
        functools.partial(write_outputs, head_cols),
        out_shape=tuple(jax.ShapeDtypeStruct(shape, F32) for shape in shapes),
        in_specs=[anywhere] * 3 + [vm],
        out_specs=(anywhere,) * 4 + (vm,) * 7,
        scratch_shapes=[
            vmem(4, chunk, width, dtype=F32),
            vmem(2, rows_z, width, dtype=F32),
            vmem(rows_z, width, dtype=F32),
            dma((2, 7)),
        ],
        name="outputs",
    )(out_y, out_g, out_w, out_s)
    return (
        y.reshape(1, micro, 1, chunk, width),
        g.reshape(1, micro, 1, chunk, width),
        qkv_g[None],
        out_gr[None],
        up_g[None],
        down_g.T[None],
        gain_g[None],
        shift_g[None],
        qv_g[None],
        upb_g,
        resid_g,
    )


def solution(mesh):
    return jax.shard_map(
        functools.partial(body, mesh.shape["dp"]),
        mesh=mesh,
        in_specs=(
            P(None, "dp", "tensor", None),
            P(None, "dp", None),
            P(None, "dp", "tensor", None),
            P("section", None, "dp", "tensor"),
            P("section", "tensor", "dp"),
            P("section", "dp", "tensor"),
            P("section", "tensor", "dp"),
            P("section", None, None),
            P("section", None, None),
            P("section", None, None),
            P("section", None),
            P("section", None),
        ),
        out_specs=(
            P("section", None, "dp", "tensor", None),
            P("section", None, "dp", "tensor", None),
            P("section", None, "dp", "tensor"),
            P("section", "tensor", "dp"),
            P("section", "dp", "tensor"),
            P("section", "tensor", "dp"),
            P("section", None, None),
            P("section", None, None),
            P("section", None, None),
            P("section", None),
            P("section", None),
        ),
        check_vma=False,
    )
```
